32 devices in a mesh: seq: 8 (over z, core), batch: 4 (over y, x).
Axes of the slice: x: 2, y: 2, z: 4, core: 2. Of those that a mesh axis runs over, the one named last changes fastest.
Arguments:
- hidden_in: bfloat16 [4, 1024, 1024], P('batch', 'seq'), may hold values from -6 to 6
- cotangent: bfloat16 [4, 1024, 1024], P('batch', 'seq'), may hold values from -6 to 6
- lengths: int32 [4], P('batch'), may hold values from 1 to 1024, as said below
- mixer_gain: bfloat16 [1024], P(('seq', 'batch')), may hold values from 0.099609375 to 1.8984375
- query_weight: bfloat16 [1024, 1024], P(('seq', 'batch')), may hold values from -0.1875 to 0.1875
- key_weight: bfloat16 [1024, 2048], P(('seq', 'batch')), may hold values from -0.1875 to 0.1875
- value_weight: bfloat16 [1024, 2048], P(('seq', 'batch')), may hold values from -0.1875 to 0.1875
- beta_weight: bfloat16 [1024, 16], P(('seq', 'batch')), may hold values from -0.1875 to 0.1875
- alpha_weight: bfloat16 [1024, 8], P(('seq', 'batch')), may hold values from -0.1875 to 0.1875
- gate_weight: bfloat16 [1024, 1024], P(('seq', 'batch')), may hold values from -0.1875 to 0.1875
- out_weight: bfloat16 [1024, 1024], P(None, ('seq', 'batch')), may hold values from -0.375 to 0.375
- feed_gain: bfloat16 [1024], P(('seq', 'batch')), may hold values from 0.099609375 to 1.8984375
- feed_gate: bfloat16 [1024, 2816], P(('seq', 'batch')), may hold values from -0.1875 to 0.1875
- feed_up: bfloat16 [1024, 2816], P(('seq', 'batch')), may hold values from -0.1875 to 0.1875
- feed_down: bfloat16 [2816, 1024], P(None, ('seq', 'batch')), may hold values from -0.15625 to 0.15625
- conv_taps: bfloat16 [4, 5120], replicated, may hold values from -3 to 3
- decay_log: float32 [8], replicated, may hold values from -1 to 0.5
- decay_bias: float32 [8], replicated, may hold values from -8 to -2.25
- head_gain: bfloat16 [128], replicated, may hold values from 0.099609375 to 1.8984375
Outputs:
- block_out: bfloat16 [4, 1024, 1024], P('batch', 'seq')
- grad_in: bfloat16 [4, 1024, 1024], P('batch', 'seq')
- grad_mixer_gain: float32 [1024], replicated
- grad_query_weight: float32 [1024, 1024], P('seq', 'batch')
- grad_key_weight: float32 [1024, 2048], P('seq', 'batch')
- grad_value_weight: float32 [1024, 2048], P('seq', 'batch')
- grad_beta_weight: float32 [1024, 16], replicated
- grad_alpha_weight: float32 [1024, 8], replicated
- grad_gate_weight: float32 [1024, 1024], P('seq', 'batch')
- grad_out_weight: float32 [1024, 1024], P('seq', 'batch')
- grad_feed_gain: float32 [1024], replicated
- grad_feed_gate: float32 [1024, 2816], P('seq', 'batch')
- grad_feed_up: float32 [1024, 2816], P('seq', 'batch')
- grad_feed_down: float32 [2816, 1024], P('seq', 'batch')
- grad_conv_taps: float32 [4, 5120], replicated
- grad_decay_log: float32 [8], replicated
- grad_decay_bias: float32 [8], replicated
- grad_head_gain: float32 [128], replicated
The draws below stay inside these ranges and needn't reach their ends.
Inputs may be any that keep to these rules, and one draw needn't show every extreme that they name: `lengths`: A row's positions below its length are real, the rest padding; in every draw some row has all 1024 positions real.
All inputs are finite; a program needn't handle non-finite values.
Results may differ from the reference program's by a relative error of at most 0.024.
Values may be sent and summed in bfloat16 or wider, within the bound.
A program may use at most 192 MiB of HBM per device.

```python
import jax
import jax.numpy as jnp
from jax import lax

D = 1024
H = 8
DK = 128
FF = 2816
SPAN = 64
KEY = 1024
SEQ_LEN = 1024
ROWS = 4


def draw_lengths(key, part):
    draw_key, pick_key = jax.random.split(jax.random.fold_in(key, 7))
    lengths = jax.random.randint(draw_key, (ROWS,), 1, SEQ_LEN + 1, dtype=jnp.int32)
    chosen = jax.random.randint(pick_key, (), 0, ROWS, dtype=jnp.int32)
    return jnp.where(jnp.arange(ROWS, dtype=jnp.int32) == chosen, SEQ_LEN, lengths).astype(jnp.int32)


def draw_decay_bias(key, part):
    ranking_key, jitter_key = jax.random.split(jax.random.fold_in(key, 11))
    ranking = jax.random.permutation(ranking_key, H).astype(jnp.float32)
    jitter = jax.random.uniform(jitter_key, (H,), jnp.float32)
    bottom, summit = (-6.9, -2.25)
    return (bottom + (summit - bottom) * (ranking + jitter) / H).astype(jnp.float32)


def levels(rng, extent, pieces, smallest, high):
    gain, own = 1.0, jax.random.fold_in(rng, 6)
    for axis_at, parts in pieces:
        draws = jnp.exp(jax.random.uniform(jax.random.fold_in(own, axis_at), (parts,), jnp.float32, smallest / len(pieces), high / len(pieces)))
        gain = gain * jnp.repeat(draws, extent[axis_at] // parts).reshape([-1 if axis == axis_at else 1 for axis in range(len(extent))])
    return gain


def normal_values(key, extent, width, reach, cuts=(), kind=jnp.bfloat16):
    factor_of = levels(key, extent, cuts, -0.22, 0.18) if cuts else 1.0
    entries = jax.random.normal(key, extent, jnp.float32) * width * factor_of
    return jnp.minimum(jnp.maximum(entries, -reach), reach).astype(kind)


def setup_inputs(seed: int = 0) -> dict:
    key_of = jax.random.split(jax.random.key(seed), 20)
    hidden_in = normal_values(key_of[0], (ROWS, SEQ_LEN, D), 1.0, 6.0, ((0, 4), (1, 8)))
    cotangent = normal_values(key_of[1], (ROWS, SEQ_LEN, D), 1.0, 6.0, ((0, 4), (1, 8)))
    lengths = draw_lengths(jax.random.fold_in(key_of[19], 71), 0)
    mixer_gain = jnp.clip(1.0 + 0.18 * jax.random.normal(key_of[3], (D,), jnp.float32), 0.099609375, 1.8984375).astype(jnp.bfloat16)
    query_weight = normal_values(key_of[4], (D, KEY), D ** -0.5, 0.1875, ((0, 32),))
    key_weight = normal_values(key_of[5], (D, 2 * KEY), D ** -0.5, 0.1875, ((0, 32),))
    value_weight = normal_values(key_of[6], (D, 2 * KEY), D ** -0.5, 0.1875, ((0, 32),))
    beta_weight = normal_values(key_of[7], (D, 2 * H), D ** -0.5, 0.1875, ((0, 32),))
    alpha_weight = normal_values(key_of[8], (D, H), D ** -0.5, 0.1875, ((0, 32),))
    gate_weight = normal_values(key_of[9], (D, KEY), D ** -0.5, 0.1875, ((0, 32),))
    out_weight = normal_values(key_of[10], (KEY, D), (KEY // 4) ** -0.5, 0.375, ((1, 32),))
    feed_gain = jnp.clip(1.0 + 0.18 * jax.random.normal(key_of[11], (D,), jnp.float32), 0.099609375, 1.8984375).astype(jnp.bfloat16)
    feed_gate = normal_values(key_of[12], (D, FF), D ** -0.5, 0.1875, ((0, 32),))
    feed_up = normal_values(key_of[13], (D, FF), D ** -0.5, 0.1875, ((0, 32),))
    feed_down = normal_values(key_of[14], (FF, D), (FF // 2) ** -0.5, 0.15625, ((1, 32),))
    conv_taps = normal_values(key_of[15], (4, 5 * KEY), 0.5, 3.0)
    decay_log = jnp.clip(jax.random.uniform(key_of[16], (H,), jnp.float32, -1.0, 0.5), -1.0, 0.5)
    decay_bias = draw_decay_bias(jax.random.fold_in(key_of[19], 71), 0)
    head_gain = jnp.clip(1.0 + 0.18 * jax.random.normal(key_of[18], (DK,), jnp.float32), 0.099609375, 1.8984375).astype(jnp.bfloat16)
    return dict(hidden_in=hidden_in, cotangent=cotangent, lengths=lengths, mixer_gain=mixer_gain, query_weight=query_weight, key_weight=key_weight, value_weight=value_weight, beta_weight=beta_weight, alpha_weight=alpha_weight, gate_weight=gate_weight, out_weight=out_weight, feed_gain=feed_gain, feed_gate=feed_gate, feed_up=feed_up, feed_down=feed_down, conv_taps=conv_taps, decay_log=decay_log, decay_bias=decay_bias, head_gain=head_gain)


EPSILON = 1e-05
PRECISE = lax.Precision.HIGHEST

@jax.custom_vjp
def low(v):
    return lax.optimization_barrier(v.astype(jnp.bfloat16)).astype(jnp.float32)

@jax.custom_vjp
def low_back(v):
    return v

def low_keep(v):
    return (low(v), None)

def low_pass(kept, grad):
    return (grad,)

def back_keep(v):
    return (v, None)

def back_low(kept, grad):
    return (low(grad),)
low.defvjp(low_keep, low_pass)
low_back.defvjp(back_keep, back_low)

def matmul(left_side, right_hand):
    return jnp.dot(left_side.astype(jnp.float32), right_hand.astype(jnp.float32), precision=PRECISE, preferred_element_type=jnp.float32)

def root_norm(values, norm_gain):
    return values * lax.rsqrt(lax.optimization_barrier(jnp.mean(values * values, axis=-1, keepdims=True)) + EPSILON) * norm_gain

def unit_norm(values):
    return values * lax.rsqrt(lax.optimization_barrier(jnp.sum(values * values, axis=-1, keepdims=True)) + EPSILON)

def span_core(carried, queries, key_vecs, value_vecs, strength, gate_log):
    sub_steps = key_vecs.shape[0]
    cumulative = jnp.transpose(jnp.cumsum(gate_log, axis=0))
    key_heads = jnp.transpose(key_vecs, (1, 0, 2))
    value_heads = jnp.transpose(value_vecs, (1, 0, 2))
    query_heads = jnp.transpose(queries, (1, 0, 2))
    beta_heads = jnp.transpose(strength)
    places = jnp.arange(sub_steps)
    lower_mask = places[:, None] >= places[None, :]
    strict_mask = places[:, None] > places[None, :]
    spread = cumulative[:, :, None] - cumulative[:, None, :]
    decays = jnp.where(lower_mask, jnp.exp(jnp.where(lower_mask, spread, 0.0)), 0.0)
    key_gram = jnp.einsum('hid,hjd->hij', key_heads, key_heads, precision=PRECISE)
    system = jnp.where(strict_mask, key_gram * decays, 0.0) * beta_heads[:, :, None] + jnp.eye(sub_steps, dtype=jnp.float32)
    right_side = jnp.concatenate([(beta_heads * jnp.exp(cumulative))[:, :, None] * key_heads, beta_heads[:, :, None] * value_heads], axis=-1)
    solved = lax.linalg.triangular_solve(system, right_side, left_side=True, lower=True, unit_diagonal=True)
    weighted = solved[..., :DK]
    base_vals = solved[..., DK:]
    new_vals = base_vals - jnp.einsum('hnd,hde->hne', weighted, carried, precision=PRECISE)
    scores = jnp.einsum('htd,hjd->htj', query_heads, key_heads, precision=PRECISE) * decays[:, 1::2, :]
    output = jnp.exp(cumulative[:, 1::2])[:, :, None] * jnp.einsum('htd,hde->hte', query_heads, carried, precision=PRECISE)
    output = output + jnp.einsum('htj,hje->hte', scores, new_vals, precision=PRECISE)
    final_log = cumulative[:, -1:]
    carried_keys = jnp.exp(final_log - cumulative)[:, :, None] * key_heads
    new_state = jnp.exp(final_log)[:, :, None] * carried + jnp.einsum('hjd,hje->hde', carried_keys, new_vals, precision=PRECISE)
    return (new_state, jnp.transpose(output, (1, 0, 2)))

def mixer_row(queries, key_vecs, value_vecs, strength, gate_log):
    tok_count = queries.shape[0]
    blocks = tok_count // SPAN
    sub_steps = 2 * SPAN
    sub_gates = jnp.stack([gate_log, jnp.zeros_like(gate_log)], axis=1).reshape(blocks, sub_steps, H)
    span_inputs = (queries.reshape(blocks, SPAN, H, DK), key_vecs.reshape(blocks, sub_steps, H, DK), value_vecs.reshape(blocks, sub_steps, H, DK), strength.reshape(blocks, sub_steps, H), sub_gates)
    stepper = jax.checkpoint(span_core)

    def advance(carried, span_in):
        return stepper(carried, *span_in)
    _, outputs = lax.scan(advance, jnp.zeros((H, DK, DK), jnp.float32), span_inputs)
    return outputs.reshape(tok_count, H, DK)

def forward_row(stream_in, params, keep_mask):
    mixer_gain, query_weight, key_weight, value_weight, beta_weight, alpha_weight, gate_weight, out_weight, feed_gain, feed_gate, feed_up, feed_down, conv_taps, decay_log, decay_bias, head_gain = params
    tok_count = stream_in.shape[0]
    normed_in = low(root_norm(stream_in, mixer_gain))
    projected = jnp.concatenate([matmul(normed_in, query_weight), matmul(normed_in, key_weight), matmul(normed_in, value_weight)], axis=-1)
    projected = low_back(low(projected))
    extended = jnp.pad(projected, ((3, 0), (0, 0)))
    mixed_sum = conv_taps[0] * extended[0:tok_count]
    for tap_index in range(1, 4):
        mixed_sum = mixed_sum + conv_taps[tap_index] * extended[tap_index:tap_index + tok_count]
    activated = jax.nn.silu(mixed_sum)
    queries = unit_norm(activated[:, :KEY].reshape(tok_count, H, DK)) * DK ** (-0.5)
    key_vecs = unit_norm(activated[:, KEY:3 * KEY].reshape(tok_count, 2, H, DK))
    value_vecs = activated[:, 3 * KEY:].reshape(tok_count, 2, H, DK)
    beta_lin = low_back(matmul(normed_in, beta_weight))
    alpha_lin = low_back(matmul(normed_in, alpha_weight))
    strength = jax.nn.sigmoid(beta_lin).reshape(tok_count, 2, H) * keep_mask[:, None, None]
    gate_log = -jnp.exp(decay_log) * jax.nn.softplus(alpha_lin + decay_bias) * keep_mask[:, None]
    gate_lin = low_back(matmul(normed_in, gate_weight))
    raw_out = mixer_row(queries, key_vecs, value_vecs, strength, gate_log)
    normed = root_norm(raw_out, head_gain) * jax.nn.silu(gate_lin.reshape(tok_count, H, DK))
    gated = low(normed.reshape(tok_count, KEY))
    after_mixer = stream_in + low_back(matmul(gated, out_weight))
    normed_mid = low(root_norm(after_mixer, feed_gain))
    gate_act = low_back(matmul(normed_mid, feed_gate))
    up_act = low_back(matmul(normed_mid, feed_up))
    hidden = low(jax.nn.silu(gate_act) * up_act)
    return after_mixer + matmul(hidden, feed_down)

def reference(hidden_in, cotangent, lengths, mixer_gain, query_weight, key_weight, value_weight, beta_weight, alpha_weight, gate_weight, out_weight, feed_gain, feed_gate, feed_up, feed_down, conv_taps, decay_log, decay_bias, head_gain):
    params = tuple((weight.astype(jnp.float32) for weight in (mixer_gain, query_weight, key_weight, value_weight, beta_weight, alpha_weight, gate_weight, out_weight, feed_gain, feed_gate, feed_up, feed_down, conv_taps, decay_log, decay_bias, head_gain)))
    positions = jnp.arange(SEQ_LEN, dtype=jnp.int32)

    def row_step(totals, row_in):
        stream_row, grad_row, length = row_in
        keep_mask = (positions < length).astype(jnp.float32)

        def forward_fn(stream_in, weights):
            return forward_row(stream_in, weights, keep_mask)
        output, back_fn = jax.vjp(forward_fn, stream_row.astype(jnp.float32), params)
        grad_stream, grad_params = back_fn(grad_row.astype(jnp.float32))
        totals = jax.tree.map(lambda former, latter: former + latter, totals, grad_params)
        return (totals, (output.astype(jnp.bfloat16), grad_stream.astype(jnp.bfloat16)))
    zero_grads = tuple((jnp.zeros_like(weight) for weight in params))
    totals, (block_out, grad_in) = lax.scan(row_step, zero_grads, (hidden_in, cotangent, lengths))
    return (block_out, grad_in, totals[0], totals[1], totals[2], totals[3], totals[4], totals[5], totals[6], totals[7], totals[8], totals[9], totals[10], totals[11], totals[12], totals[13], totals[14], totals[15])
```

```python
import functools
import jax
import jax.numpy as jnp
from jax import lax
from jax.experimental import pallas as pl
from jax.experimental.pallas import tpu as pltpu
from jax.sharding import PartitionSpec as P

F32, BF16 = jnp.float32, jnp.bfloat16
EPS = 1e-05
DK = 128
HALF = 64
GS = 4
GB = GS * HALF
NN = (((1,), (0,)), ((), ()))
NT = (((1,), (1,)), ((), ()))
TN = (((0,), (0,)), ((), ()))


def mm(a, b, dims=NN):
    return lax.dot_general(a.astype(BF16), b.astype(BF16), dims, preferred_element_type=F32)


def split(a):
    hi = a.astype(BF16)
    return hi, (a - hi.astype(F32)).astype(BF16)


def mm3(a, b, dims=NN):
    (ah, al), (bh, bl) = (x if isinstance(x, tuple) else split(x) for x in (a, b))
    return (
        lax.dot_general(ah, bl, dims, preferred_element_type=F32)
        + lax.dot_general(al, bh, dims, preferred_element_type=F32)
    ) + lax.dot_general(ah, bh, dims, preferred_element_type=F32)


def iota(shape, axis):
    return lax.broadcasted_iota(jnp.int32, shape, axis)


def sub_masks():
    rows, cols = iota((128, 128), 0), iota((128, 128), 1)
    tr, tc = 2 * (rows & 63) + (rows >> 6), 2 * (cols & 63) + (cols >> 6)
    strict = tr > tc
    levels = []
    for bits in range(3, 7):
        same_up = (tr >> (bits + 1)) == (tc >> (bits + 1))
        levels.append(strict & same_up & ((tr >> bits) != (tc >> bits)))
    base = strict & ((tr >> 3) == (tc >> 3))
    return strict, base, levels


def unit(a):
    r = lax.rsqrt(jnp.sum(a * a, axis=-1, keepdims=True) + EPS)
    return a * r, r


def softplus(x):
    return jnp.maximum(x, 0.0) + jnp.log1p(jnp.exp(-jnp.abs(x)))


def lane(x, width=128):
    return jnp.broadcast_to(x, (x.shape[0], width))


def gates(sm, dec_log, dec_bias, keep):
    sig0, sig1 = jax.nn.sigmoid(sm[:, 0:1]), jax.nn.sigmoid(sm[:, 1:2])
    al = sm[:, 2:3] + dec_bias
    return sig0, sig1, al


def span_decay(gb, tri, masks):
    c = mm3(tri, gb)
    ct = jnp.transpose(jnp.concatenate([c, c], axis=0))[:64]
    e = jnp.exp(jnp.minimum(c - ct, 0.0))
    return c, e


def conv_mix(buf, taps):
    mix = taps[0:1] * buf[5 : 5 + GB]
    for j in range(1, 4):
        mix = mix + taps[j : j + 1] * buf[5 + j : 5 + j + GB]
    return mix


def head_taps(taps_ref, head, heads):
    parts = []
    for col in (head, heads + head, 2 * heads + head, 3 * heads + head, 4 * heads + head):
        parts.append(taps_ref[:, pl.ds(pl.multiple_of(col * 128, 128), 128)].astype(F32))
    return jnp.concatenate(parts, axis=1)


def fwd_kernel(
    rep, heads,
    len_ref, dlog_ref, dbias_ref,
    hid_ref, gain_ref, w_ref, taps_ref, hg_ref,
    part_ref, normed_ref, pre_ref, gl_ref, sm_ref, gated_ref, raw_ref,
    t_ref, wt_ref, vn_ref, n_ref, p_ref, s_ref,
    buf, state,
):
    step = pl.program_id(0)
    place = lax.axis_index("seq")
    head = place // rep

    @pl.when(step == 0)
    def _():
        state[...] = jnp.zeros_like(state)
        buf[0:8] = jnp.zeros((8, 640), F32)

    x = hid_ref[...].astype(F32)
    r = lax.rsqrt(jnp.mean(x * x, axis=-1, keepdims=True) + EPS)
    normed = (x * r * gain_ref[...]).astype(BF16)
    normed_ref[...] = normed
    proj = mm(normed, w_ref[:, 0:896])
    pre = proj[:, 0:640].astype(BF16).astype(F32)
    pre_ref[...] = pre
    gl = proj[:, 640:768]
    sm = proj[:, 768:896]
    gl_ref[...] = gl
    sm_ref[...] = sm
    buf[8 : 8 + GB] = pre
    taps = head_taps(taps_ref, head, heads)
    mix = conv_mix(buf, taps)
    buf[0:8] = pre[GB - 8 : GB]
    act = mix * jax.nn.sigmoid(mix)
    q = unit(act[:, 0:128])[0] * DK ** (-0.5)
    k0, k1 = unit(act[:, 128:256])[0], unit(act[:, 256:384])[0]
    v0, v1 = act[:, 384:512], act[:, 512:640]
    pos = step * GB + iota((GB, 1), 0)
    keep = (pos < len_ref[0]).astype(F32)
    sig0, sig1, al = gates(sm, None, dbias_ref[head], keep)
    b0, b1 = sig0 * keep, sig1 * keep
    eg = jnp.exp(jnp.full((1, 1), dlog_ref[head], F32))
    g = lane(-eg * softplus(al) * keep)
    b0, b1 = lane(b0), lane(b1)

    strict, base, levels = sub_masks()
    eye = (iota((128, 128), 0) == iota((128, 128), 1)).astype(F32)
    tri = (iota((64, 64), 0) >= iota((64, 64), 1)).astype(F32)
    causal = iota((64, 128), 0) >= (iota((64, 128), 1) & 63)

    K, Q, V, B, C, N, P, Kc = [], [], [], [], [], [], [], []
    for s in range(GS):
        sl = slice(64 * s, 64 * s + 64)
        K.append(jnp.concatenate([k0[sl], k1[sl]], axis=0))
        V.append(jnp.concatenate([v0[sl], v1[sl]], axis=0))
        B.append(jnp.concatenate([b0[sl], b1[sl]], axis=0))
        Q.append(q[sl])
        c, e = span_decay(g[sl], tri, None)
        C.append(c)
        ee = jnp.concatenate([e, e], axis=0)
        gram = mm3(jnp.concatenate([K[s], Q[s]], axis=0), K[s], NT)
        N.append(jnp.where(strict, gram[:128] * ee, 0.0) * B[s])
        P.append(jnp.where(causal, gram[128:] * e, 0.0))
        cc = jnp.concatenate([c, c], axis=0)
        Kc.append(jnp.exp(cc[63:64] - cc) * K[s])
    X = []
    n1 = [jnp.where(base, n, 0.0) for n in N]
    n1s = [split(n) for n in n1]
    n2 = [mm3(a, a) for a in n1s]
    n2s = [split(n) for n in n2]
    n3 = [mm3(a, b) for a, b in zip(n1s, n2s)]
    n4 = [mm3(a, a) for a in n2s]
    y = [eye - a + b - c for a, b, c in zip(n1, n2, n3)]
    X = [a + mm3(a, b) for a, b in zip(y, n4)]
    for lv in levels:
        xs = [split(x_) for x_ in X]
        bl = [jnp.where(lv, n, 0.0) for n in N]
        xb = [mm3(a, b) for a, b in zip(xs, bl)]
        X = [x_ - mm3(a, b) for x_, a, b in zip(X, xb, xs)]
    W, U = [], []
    for s in range(GS):
        cc = jnp.concatenate([C[s], C[s]], axis=0)
        rhs = jnp.concatenate([B[s] * jnp.exp(cc) * K[s], B[s] * V[s]], axis=1)
        wu = mm3(X[s], rhs)
        W.append(wu[:, :128])
        U.append(wu[:, 128:])
        t_ref[s] = X[s]
        wt_ref[s] = W[s]
        n_ref[s] = N[s]
        p_ref[s] = P[s]
    S = state[...]
    raw = []
    Ws = [split(a) for a in W]
    Kcs = [split(a) for a in Kc]
    for s in range(GS):
        s_ref[s] = S
        ss = split(S)
        vn = U[s] - mm3(Ws[s], ss)
        vn_ref[s] = vn
        vs = split(vn)
        o = jnp.exp(C[s]) * mm3(Q[s], ss) + mm3(P[s], vs)
        raw.append(o)
        S = jnp.exp(C[s][63:64]) * S + mm3(Kcs[s], vs, TN)
    state[...] = S
    o = jnp.concatenate(raw, axis=0)
    raw_ref[...] = o
    rr = lax.rsqrt(jnp.mean(o * o, axis=-1, keepdims=True) + EPS)
    gated = (o * rr * hg_ref[...] * (gl * jax.nn.sigmoid(gl))).astype(BF16)
    gated_ref[...] = gated
    if rep > 1:
        gated = jnp.where(lax.rem(place, rep) == 0, gated, jnp.zeros_like(gated))
    part_ref[...] = mm(gated, w_ref[:, 896:1024], NT).astype(BF16)


def bwd_kernel(
    rep, heads, steps,
    len_ref, dlog_ref, dbias_ref,
    dbr_ref, w_ref, taps_ref, hg_ref, pre_ref, prev_ref, gl_ref, sm_ref, raw_ref,
    t_ref, wt_ref, vn_ref, n_ref, p_ref, s_ref,
    dall_ref, part_ref, small_ref,
    buf, dbuf, dstate,
):
    step = pl.program_id(0)
    blk = steps - 1 - step
    place = lax.axis_index("seq")
    head = place // rep

    @pl.when(step == 0)
    def _():
        dstate[...] = jnp.zeros_like(dstate)
        dbuf[GB : GB + 8] = jnp.zeros((8, 640), F32)
        small_ref[...] = jnp.zeros_like(small_ref)

    d_gated = mm(dbr_ref[...], w_ref[:, 896:1024])
    gl, sm, o, hg = gl_ref[...], sm_ref[...], raw_ref[...], hg_ref[...]
    sg = jax.nn.sigmoid(gl)
    rr = lax.rsqrt(jnp.mean(o * o, axis=-1, keepdims=True) + EPS)
    yn = o * rr
    dn = d_gated * (gl * sg)
    d_gl = d_gated * (yn * hg) * (sg * (1.0 + gl * (1.0 - sg)))
    g_hg = jnp.sum(dn * yn, axis=0, keepdims=True)
    dy = dn * hg
    d_raw = rr * (dy - yn * jnp.mean(yn * dy, axis=-1, keepdims=True))

    pre = pre_ref[...]
    buf[8 : 8 + GB] = pre
    buf[0:8] = jnp.where(blk > 0, prev_ref[...], 0.0)
    taps = head_taps(taps_ref, head, heads)
    mix = conv_mix(buf, taps)
    sig = jax.nn.sigmoid(mix)
    act = mix * sig
    qn, rq = unit(act[:, 0:128])
    k0, r0 = unit(act[:, 128:256])
    k1, r1 = unit(act[:, 256:384])
    v0, v1 = act[:, 384:512], act[:, 512:640]
    q = qn * DK ** (-0.5)
    pos = blk * GB + iota((GB, 1), 0)
    keep = (pos < len_ref[0]).astype(F32)
    sig0, sig1, al = gates(sm, None, dbias_ref[head], keep)
    eg = jnp.exp(jnp.full((1, 1), dlog_ref[head], F32))
    g1 = -eg * softplus(al) * keep
    g = lane(g1)
    b0, b1 = lane(sig0 * keep), lane(sig1 * keep)

    strict, _, _ = sub_masks()
    tri = (iota((64, 64), 0) >= iota((64, 64), 1)).astype(F32)
    trit = (iota((64, 64), 0) <= iota((64, 64), 1)).astype(F32)
    causal = iota((64, 128), 0) >= (iota((64, 128), 1) & 63)

    K, Q, V, B, C, E, Kc, A1, A2, DO = [], [], [], [], [], [], [], [], [], []
    for s in range(GS):
        sl = slice(64 * s, 64 * s + 64)
        K.append(jnp.concatenate([k0[sl], k1[sl]], axis=0))
        V.append(jnp.concatenate([v0[sl], v1[sl]], axis=0))
        B.append(jnp.concatenate([b0[sl], b1[sl]], axis=0))
        Q.append(q[sl])
        c, e = span_decay(g[sl], tri, None)
        C.append(c)
        E.append(e)
        cc = jnp.concatenate([c, c], axis=0)
        Kc.append(jnp.exp(cc[63:64] - cc) * K[s])
        do = d_raw[sl]
        DO.append(do)
        A1.append(mm3(p_ref[s], do, TN))
        A2.append(mm3(jnp.exp(c) * Q[s], do, TN))
    dS = dstate[...]
    DV, DS = [None] * GS, [None] * GS
    for s in reversed(range(GS)):
        DS[s] = dS
        dss = split(dS)
        dvn = A1[s] + mm3(Kc[s], dss)
        DV[s] = dvn
        dS = jnp.exp(C[s][63:64]) * dS + A2[s] - mm3(wt_ref[s], dvn, TN)
    dstate[...] = dS
    dq_l, dk0_l, dk1_l, dv0_l, dv1_l, db0_l, db1_l, dg_l = [], [], [], [], [], [], [], []
    for s in range(GS):
        vn, sst, n, p = vn_ref[s], s_ref[s], n_ref[s], p_ref[s]
        vns = split(vn)
        cc = jnp.concatenate([C[s], C[s]], axis=0)
        ec = jnp.exp(cc)
        ee = jnp.concatenate([E[s], E[s]], axis=0)
        dr = mm3(t_ref[s], DV[s], TN)
        dd = mm3(jnp.concatenate([dr, DO[s]], axis=0), vns, NT)
        dN = jnp.where(strict, -dd[:128], 0.0)
        dP = jnp.where(causal, dd[128:], 0.0)
        h = mm3(jnp.concatenate([dr, DO[s]], axis=0), sst, NT)
        hk, hq = h[:128], h[128:]
        fh = dP * E[s]
        dq = ec[:64] * hq + mm3(fh, K[s])
        dgm = dN * ee * B[s]
        dkc = mm3(vns, DS[s], NT)
        ekc = jnp.exp(cc[63:64] - cc)
        dk = (
            ekc * dkc - B[s] * ec * hk + mm3(fh, Q[s], TN) + mm3(dgm + jnp.transpose(dgm), K[s])
        )
        khk = jnp.sum(K[s] * hk, axis=-1, keepdims=True)
        ecl = ec[:, 0:1]
        nb = jnp.where(strict, ee, 0.0)
        graml = mm3(K[s], K[s], NT)
        db = (
            jnp.sum(dr * V[s], axis=-1, keepdims=True)
            - ecl * khk
            + jnp.sum(dN * (graml * nb), axis=-1, keepdims=True)
        )
        e1 = dN * n
        f1 = dP * p
        z = e1[:64, :64] + e1[:64, 64:] + e1[64:, :64] + e1[64:, 64:] + f1[:, :64] + f1[:, 64:]
        dc = jnp.sum(z - jnp.transpose(z), axis=-1, keepdims=True)
        dks = -B[s][:, 0:1] * ecl * khk
        hj = jnp.sum(Kc[s] * dkc, axis=-1, keepdims=True)
        dc = dc + dks[:64] + dks[64:] - hj[:64] - hj[64:]
        dc = dc + ec[:64, 0:1] * jnp.sum(Q[s] * hq, axis=-1, keepdims=True)
        dcl = jnp.sum(hj, keepdims=True).reshape(1, 1) + ec[63:64, 0:1] * jnp.sum(
            jnp.sum(sst * DS[s], axis=-1, keepdims=True), axis=0, keepdims=True
        )
        dg = mm3(trit, lane(dc)) + dcl
        dg_l.append(dg[:, 0:1])
        dq_l.append(dq)
        dk0_l.append(dk[:64])
        dk1_l.append(dk[64:])
        dv = B[s] * dr
        dv0_l.append(dv[:64])
        dv1_l.append(dv[64:])
        db0_l.append(db[:64])
        db1_l.append(db[64:])
    cat = lambda parts: jnp.concatenate(parts, axis=0)
    dq, dk0, dk1, dv0, dv1 = cat(dq_l), cat(dk0_l), cat(dk1_l), cat(dv0_l), cat(dv1_l)
    db0, db1, dg = cat(db0_l), cat(db1_l), cat(dg_l)

    def unit_back(d, n, rn):
        return rn * (d - n * jnp.sum(d * n, axis=-1, keepdims=True))

    d_act = jnp.concatenate(
        [unit_back(dq * DK ** (-0.5), qn, rq), unit_back(dk0, k0, r0), unit_back(dk1, k1, r1), dv0, dv1],
        axis=1,
    )
    d_mix = d_act * (sig * (1.0 + mix * (1.0 - sig)))
    for j in range(4):
        small_ref[j : j + 1, 0:640] += jnp.sum(d_mix * buf[5 + j : 5 + j + GB], axis=0, keepdims=True)
    dbuf[0:GB] = d_mix
    d_pre = taps[3:4] * d_mix
    for j in range(3):
        d_pre = d_pre + taps[j : j + 1] * dbuf[3 - j : 3 - j + GB]
    dbuf[GB : GB + 8] = d_mix[0:8]

    d_al = -dg * eg * jax.nn.sigmoid(al) * keep
    d_b0 = db0 * keep * sig0 * (1.0 - sig0)
    d_b1 = db1 * keep * sig1 * (1.0 - sig1)
    lanes = iota((GB, 128), 1)
    d_sm = jnp.where(lanes == 0, d_b0, jnp.where(lanes == 1, d_b1, jnp.where(lanes == 2, d_al, 0.0)))
    small_ref[0:1, 640:768] += g_hg
    small_ref[1:2, 640:768] += jnp.broadcast_to(jnp.sum(dg * g1, axis=0, keepdims=True), (1, 128))
    small_ref[2:3, 640:768] += jnp.broadcast_to(jnp.sum(d_al, axis=0, keepdims=True), (1, 128))
    dall = jnp.concatenate([d_pre.astype(BF16), d_gl.astype(BF16), d_sm.astype(BF16)], axis=1)
    dall_ref[...] = dall
    if rep > 1:
        dall = jnp.where(lax.rem(place, rep) == 0, dall, jnp.zeros_like(dall))
    part_ref[...] = mm(dall, w_ref[:, 0:896], NT).astype(BF16)


def mixer_fwd(lengths, dlog, dbias, hid, gain, w, taps, hg, rep, heads):
    n = hid.shape[0]
    steps = n // GB
    spans = n // HALF
    sds = jax.ShapeDtypeStruct
    smem = pl.BlockSpec(memory_space=pltpu.SMEM)
    whole = lambda a: pl.BlockSpec(a.shape, lambda i: (0,) * a.ndim)
    rows = lambda width: pl.BlockSpec((GB, width), lambda i: (i, 0))
    sq = lambda r: pl.BlockSpec((GS, r, 128), lambda i: (i, 0, 0))
    outs = [
        (sds((n, 1024), BF16), rows(1024)),
        (sds((n, 1024), BF16), rows(1024)),
        (sds((n, 640), F32), rows(640)),
        (sds((n, 128), F32), rows(128)),
        (sds((n, 128), F32), rows(128)),
        (sds((n, 128), BF16), rows(128)),
        (sds((n, 128), F32), rows(128)),
        (sds((spans, 128, 128), F32), sq(128)),
        (sds((spans, 128, 128), F32), sq(128)),
        (sds((spans, 128, 128), F32), sq(128)),
        (sds((spans, 128, 128), F32), sq(128)),
        (sds((spans, 64, 128), F32), sq(64)),
        (sds((spans, 128, 128), F32), sq(128)),
    ]
    return pl.pallas_call(
        functools.partial(fwd_kernel, rep, heads),
        grid=(steps,),
        in_specs=[smem, smem, smem, rows(1024), whole(gain), whole(w), whole(taps), whole(hg)],
        out_specs=[o[1] for o in outs],
        out_shape=[o[0] for o in outs],
        scratch_shapes=[pltpu.VMEM((8 + GB, 640), F32), pltpu.VMEM((128, 128), F32)],
        compiler_params=pltpu.CompilerParams(vmem_limit_bytes=48 * 1024 * 1024),
        cost_estimate=pl.CostEstimate(flops=4 * n * 1024 * 1024, bytes_accessed=16 * n * 1024, transcendentals=n * 2000),
        name="mixer_fwd",
    )(lengths, dlog, dbias, hid, gain, w, taps, hg)


def mixer_bwd(lengths, dlog, dbias, dbr, w, taps, hg, saved, rep, heads):
    pre, gl, sm, raw, t, wt, vn, nm, p, st = saved
    n = dbr.shape[0]
    steps = n // GB
    sds = jax.ShapeDtypeStruct
    smem = pl.BlockSpec(memory_space=pltpu.SMEM)
    whole = lambda a: pl.BlockSpec(a.shape, lambda i: (0,) * a.ndim)
    rows = lambda width: pl.BlockSpec((GB, width), lambda i: (steps - 1 - i, 0))
    sq = lambda r: pl.BlockSpec((GS, r, 128), lambda i: (steps - 1 - i, 0, 0))
    prev = pl.BlockSpec((8, 640), lambda i: (jnp.maximum((steps - 1 - i) * (GB // 8) - 1, 0), 0))
    return pl.pallas_call(
        functools.partial(bwd_kernel, rep, heads, steps),
        grid=(steps,),
        in_specs=[smem, smem, smem, rows(1024), whole(w), whole(taps), whole(hg), rows(640), prev, rows(128),
                  rows(128), rows(128), sq(128), sq(128), sq(128), sq(128), sq(64), sq(128)],
        out_specs=[rows(896), rows(1024), pl.BlockSpec((8, 768), lambda i: (0, 0))],
        out_shape=[sds((n, 896), BF16), sds((n, 1024), BF16), sds((8, 768), F32)],
        scratch_shapes=[pltpu.VMEM((8 + GB, 640), F32), pltpu.VMEM((GB + 8, 640), F32), pltpu.VMEM((128, 128), F32)],
        compiler_params=pltpu.CompilerParams(vmem_limit_bytes=48 * 1024 * 1024),
        cost_estimate=pl.CostEstimate(flops=4 * n * 1024 * 1024, bytes_accessed=16 * n * 1024, transcendentals=n * 2000),
        name="mixer_bwd",
    )(lengths, dlog, dbias, dbr, w, taps, hg, pre, pre, gl, sm, raw, t, wt, vn, nm, p, st)


MESH = pl.DeviceIdType.MESH


class Place:
    def __init__(self, ns, nb):
        self.ns, self.nb, self.nz = ns, nb, ns // 2
        self.s, self.b = lax.axis_index("seq"), lax.axis_index("batch")
        self.z, self.c = self.s // 2, lax.rem(self.s, 2)
        self.sib = self.s + 1 - 2 * self.c

    def chip(self, dz):
        return lax.rem(self.z + dz, self.nz)

    def chip_before(self, dz):
        return lax.rem(self.z + self.nz - dz, self.nz)

    def seq_at(self, ds):
        return lax.rem(self.s + ds, self.ns)

    def seq_before(self, ds):
        return lax.rem(self.s + self.ns - ds, self.ns)

    def batch_at(self, db):
        return lax.rem(self.b + db, self.nb)

    def batch_before(self, db):
        return lax.rem(self.b + self.nb - db, self.nb)


def enter(at):
    barrier = pltpu.get_barrier_semaphore()
    for ds in range(1, at.ns):
        pl.semaphore_signal(barrier, inc=1, device_id={"seq": at.seq_at(ds)}, device_id_type=MESH)
    for db in range(1, at.nb):
        pl.semaphore_signal(barrier, inc=1, device_id={"batch": at.batch_at(db)}, device_id_type=MESH)
    pl.semaphore_wait(barrier, at.ns + at.nb - 2)


def send(src, dst, send_sem, recv_sem, where):
    return pltpu.make_async_remote_copy(
        src_ref=src, dst_ref=dst, send_sem=send_sem, recv_sem=recv_sem, device_id=where, device_id_type=MESH
    )


class SeqGather:
    def __init__(self, at, src, out, ssem, rsem):
        self.at, self.out, self.ssem, self.rsem = at, out, ssem, rsem
        nz = at.nz
        self.far = [
            send(src, out.at[at.s], ssem.at[dz], rsem.at[dz], {"seq": 2 * at.chip(dz) + at.c}) for dz in range(1, nz)
        ]
        self.near = send(src, out.at[at.s], ssem.at[0], rsem.at[0], {"seq": at.sib})

    def start(self):
        for copy in self.far:
            copy.start()
        self.near.start()

    def finish(self):
        at, out, nz = self.at, self.out, self.at.nz
        onward = []
        for dz in range(1, nz):
            self.far[dz - 1].wait_recv()
            block = out.at[2 * at.chip_before(dz) + at.c]
            copy = send(block, block, self.ssem.at[nz - 1 + dz], self.rsem.at[nz - 1 + dz], {"seq": at.sib})
            copy.start()
            onward.append(copy)
        self.near.wait_recv()
        for copy in onward:
            copy.wait_recv()
        for copy in self.far + [self.near] + onward:
            copy.wait_send()


class SeqSum:
    def __init__(self, at, part, got, out, far, ssem, rsem):
        self.at, self.part, self.got, self.out, self.far = at, part, got, out, far
        self.pair = []
        self.hop = []
        for i, dz in enumerate(list(range(1, at.nz)) + [0]):
            z = at.chip(dz)
            self.pair.append(
                send(part.at[2 * z + 1 - at.c], got.at[dz], ssem.at[i], rsem.at[i], {"seq": at.sib})
            )
            if dz:
                self.hop.append(
                    send(out.at[dz], far.at[dz], ssem.at[at.nz + i], rsem.at[at.nz + i], {"seq": 2 * z + at.c})
                )

    def start(self):
        for copy in self.pair:
            copy.start()

    def forward(self):
        at = self.at
        for i in range(at.nz - 1):
            dz = i + 1
            self.pair[i].wait_recv()
            mine = self.part[2 * at.chip(dz) + at.c].astype(F32)
            self.out[dz] = (mine + self.got[dz].astype(F32)).astype(BF16)
            self.hop[i].start()
        self.pair[at.nz - 1].wait_recv()

    def finish(self):
        at = self.at
        total = self.part[2 * at.z + at.c].astype(F32) + self.got[0].astype(F32)
        for copy in self.hop:
            copy.wait_recv()
        for dz in range(1, at.nz):
            total = total + self.far[dz].astype(F32)
        for copy in self.pair + self.hop:
            copy.wait_send()
        return total


def gather_kernel(ns, nb, hid, wmix, wff, hid_out, wm_out, ff_out, lsem, hs, hr, ws, wr, fs, fr):
    at = Place(ns, nb)
    enter(at)
    local = [
        pltpu.make_async_copy(hid, hid_out.at[at.s], lsem.at[0]),
        pltpu.make_async_copy(wmix.at[at.s], wm_out.at[at.s, at.b], lsem.at[1]),
        pltpu.make_async_copy(wff.at[at.b], ff_out.at[:, at.b], lsem.at[2]),
    ]
    for copy in local:
        copy.start()
    spread = [
        send(wmix.at[at.seq_at(ds)], wm_out.at[at.s, at.b], ws.at[ds], wr.at[ds], {"seq": at.seq_at(ds)})
        for ds in range(1, ns)
    ]
    for copy in spread:
        copy.start()
    rows = SeqGather(at, hid, hid_out, hs, hr)
    rows.start()
    onward = []
    for ds in range(ns):
        if ds:
            spread[ds - 1].wait_recv()
        origin = at.seq_before(ds)
        block = wm_out.at[origin, at.b]
        for db in range(1, nb):
            k = ns + ds * (nb - 1) + db - 1
            copy = send(wmix.at[at.s] if ds == 0 else block, block, ws.at[k], wr.at[k], {"batch": at.batch_at(db)})
            copy.start()
            onward.append(copy)
    cols = [
        send(wff.at[at.batch_at(db)], ff_out.at[:, at.b], fs.at[db], fr.at[db], {"batch": at.batch_at(db)})
        for db in range(1, nb)
    ]
    for copy in cols:
        copy.start()
    rows.finish()
    for copy in onward + cols:
        copy.wait_recv()
    for copy in spread + onward + cols:
        copy.wait_send()
    for copy in local:
        copy.wait()


def mid_kernel(ns, nb, part, hid, cot, gain, after, nm_out, cot_out, got, out, far, nm, lsem, qs, qr, ns_, nr, cs, cr):
    at = Place(ns, nb)
    enter(at)
    rows = SeqSum(at, part, got, out, far, qs, qr)
    rows.start()
    mine = pltpu.make_async_copy(cot, cot_out.at[at.b], lsem.at[0])
    mine.start()
    cots = [
        send(cot, cot_out.at[at.b], cs.at[db], cr.at[db], {"batch": at.batch_at(db)}) for db in range(1, nb)
    ]
    for copy in cots:
        copy.start()
    rows.forward()
    total = rows.finish() + hid[...].astype(F32)
    after[...] = total
    r = lax.rsqrt(jnp.mean(total * total, axis=-1, keepdims=True) + EPS)
    nm[...] = (total * r * gain[...]).astype(BF16)
    own = pltpu.make_async_copy(nm, nm_out.at[at.b], lsem.at[1])
    own.start()
    mids = [send(nm, nm_out.at[at.b], ns_.at[db], nr.at[db], {"batch": at.batch_at(db)}) for db in range(1, nb)]
    for copy in mids:
        copy.start()
    for copy in mids + cots:
        copy.wait_recv()
    for copy in mids + cots:
        copy.wait_send()
    mine.wait()
    own.wait()


def turn_kernel(
    ns, nb, pmid, pout, after, cot, gain,
    block_out, d_stream, dbr_out, gfeed,
    got_m, got_o, dbr, lsem, ms, mr, os_, or_, gs, gr,
):
    at = Place(ns, nb)
    enter(at)
    mids = [
        send(pmid.at[at.batch_at(db)], got_m.at[db], ms.at[db], mr.at[db], {"batch": at.batch_at(db)})
        for db in range(1, nb)
    ]
    outs = [
        send(pout.at[at.batch_at(db)], got_o.at[db], os_.at[db], or_.at[db], {"batch": at.batch_at(db)})
        for db in range(1, nb)
    ]
    for copy in mids + outs:
        copy.start()
    x = after[...]
    d_mid = pmid[at.b].astype(F32)
    for copy in mids:
        copy.wait_recv()
    for db in range(1, nb):
        d_mid = d_mid + got_m[db].astype(F32)
    r = lax.rsqrt(jnp.mean(x * x, axis=-1, keepdims=True) + EPS)
    y = x * r
    gfeed[...] = jnp.sum(d_mid * y, axis=0, keepdims=True)
    dy = d_mid * gain[...]
    ds_ = cot[...].astype(F32) + r * (dy - y * jnp.mean(dy * y, axis=-1, keepdims=True))
    d_stream[...] = ds_
    dbr[...] = ds_.astype(BF16)
    own = pltpu.make_async_copy(dbr, dbr_out.at[at.s], lsem.at[0])
    own.start()
    rows = SeqGather(at, dbr, dbr_out, gs, gr)
    rows.start()
    for copy in outs:
        copy.wait_recv()
    total = after[...] + pout[at.b].astype(F32)
    for db in range(1, nb):
        total = total + got_o[db].astype(F32)
    block_out[...] = total.astype(BF16)
    rows.finish()
    for copy in mids + outs:
        copy.wait_send()
    own.wait()


def last_kernel(
    ns, nb, rep,
    part, grads, gout, smalls, hid, gain, d_stream, gfeed,
    grad_in, slots, gout_sum, small_all, vec_sum,
    got, out, far, got_g, piece, got_o, got_s, small_sum, got_v, vec, got_w,
    ready, lsem, qs, qr, gs, gr, ps, pr, os_, or_, ss, sr, us, ur, vs, vr, xs, xr,
):
    at = Place(ns, nb)
    nk, nq = ns // nb, slots.shape[0] // 6
    enter(at)
    for ds in range(1, ns):
        pl.semaphore_signal(ready, inc=1, device_id={"seq": at.seq_at(ds)}, device_id_type=MESH)
    rows = SeqSum(at, part, got, out, far, qs, qr)
    rows.start()
    over = []
    for k in range(nk):
        for db in range(1, nb):
            to = at.batch_at(db)
            i = k * nb + db
            over.append(send(grads.at[to + nb * k], got_g.at[i], gs.at[i], gr.at[i], {"batch": to}))
    outs = [
        send(gout.at[at.batch_at(db)], got_o.at[db], os_.at[db], or_.at[db], {"batch": at.batch_at(db)})
        for db in range(1, nb)
    ]
    small = [
        send(smalls, got_s.at[db], ss.at[db], sr.at[db], {"batch": at.batch_at(db)}) for db in range(1, nb)
    ]
    for copy in small + over + outs:
        copy.start()
    rows.forward()
    total = smalls[...]
    for copy in small:
        copy.wait_recv()
    for db in range(1, nb):
        total = total + got_s[db]
    small_sum[...] = total
    own = pltpu.make_async_copy(small_sum, small_all.at[at.s], lsem.at[0])
    own.start()
    heads = [
        send(small_sum, small_all.at[at.s], us.at[ds], ur.at[ds], {"seq": at.seq_at(ds)}) for ds in range(1, ns)
    ]
    for copy in heads:
        copy.start()
    for copy in over:
        copy.wait_recv()
    pl.semaphore_wait(ready, ns - 1)
    width = slots.shape[2]
    units = (at.s // nq, at.s, ns + at.s, at.s, ns + at.s, at.s // nq)
    placed = []
    for k in range(nk):
        row = at.b + nb * k
        acc = grads[row].astype(F32)
        for db in range(1, nb):
            acc = acc + got_g[k * nb + db].astype(F32)
        for m in range(6):
            block = acc[:, 128 * m : 128 * m + 128]
            if rep > 1:
                block = jnp.where(lax.rem(at.s, rep) == 0, block[:, :width], block[:, width:])
            piece[k * 6 + m] = block.astype(BF16)
            if m in (0, 5):
                owner, slot = at.s // nq, (0 if m == 0 else 5 * nq) + lax.rem(at.s, nq)
            else:
                unit_at = ((m - 1) % 2) * ns + at.s
                owner, slot = unit_at // (2 * nq), (nq if m < 3 else 3 * nq) + lax.rem(unit_at, 2 * nq)
            placed.append((piece.at[k * 6 + m], row, owner, slot, k * 6 + m))
    for src, row, owner, slot, i in placed:
        here = jnp.logical_and(row == at.s, owner == at.b)

        @pl.when(here)
        def _():
            pltpu.make_async_copy(src, slots.at[slot], pr.at[slot]).start()

        @pl.when(jnp.logical_not(here))
        def _():
            send(src, slots.at[slot], ps.at[i], pr.at[slot], {"seq": row, "batch": owner}).start()

    d_normed = rows.finish()
    x = hid[...].astype(F32)
    r = lax.rsqrt(jnp.mean(x * x, axis=-1, keepdims=True) + EPS)
    y = x * r
    vec[0:1] = jnp.sum(d_normed * y, axis=0, keepdims=True)
    vec[1:2] = gfeed[...]
    pair = [send(vec, got_v.at[db], vs.at[db], vr.at[db], {"batch": at.batch_at(db)}) for db in range(1, nb)]
    for copy in pair:
        copy.start()
    dy = d_normed * gain[...]
    grad_in[...] = (d_stream[...] + r * (dy - y * jnp.mean(dy * y, axis=-1, keepdims=True))).astype(BF16)
    for copy in outs:
        copy.wait_recv()
    acc = gout[at.b].astype(F32)
    for db in range(1, nb):
        acc = acc + got_o[db].astype(F32)
    gout_sum[...] = acc
    for copy in pair:
        copy.wait_recv()
    row_sum = vec[...]
    for db in range(1, nb):
        row_sum = row_sum + got_v[db]
    got_w[0] = row_sum
    wide = [
        send(got_w.at[0], got_w.at[ds], xs.at[ds], xr.at[ds], {"seq": at.seq_at(ds)}) for ds in range(1, ns)
    ]
    for copy in wide:
        copy.start()
    for copy in wide + heads:
        copy.wait_recv()
    row_sum = got_w[0]
    for ds in range(1, ns):
        row_sum = row_sum + got_w[ds]
    vec_sum[...] = row_sum
    for src, row, owner, slot, i in placed:
        here = jnp.logical_and(row == at.s, owner == at.b)

        @pl.when(jnp.logical_not(here))
        def _():
            send(src, slots.at[slot], ps.at[i], pr.at[slot], {"seq": row, "batch": owner}).wait_send()

    for slot in range(slots.shape[0]):
        pltpu.make_async_copy(piece.at[0], slots.at[slot], pr.at[slot]).wait()
    for copy in small + over + outs + heads + pair + wide:
        copy.wait_send()
    own.wait()


def comm_call(kernel, outs, scratch, ident, name, args, specs, flops=0):
    sds = jax.ShapeDtypeStruct
    return pl.pallas_call(
        kernel,
        in_specs=specs,
        out_specs=[o[1] for o in outs],
        out_shape=[o[0] for o in outs],
        scratch_shapes=scratch,
        compiler_params=pltpu.CompilerParams(
            collective_id=ident, has_side_effects=True, vmem_limit_bytes=48 * 1024 * 1024
        ),
        name=name,
    )(*args)


def dma(n):
    return pltpu.SemaphoreType.DMA((n,))


def on_device(
    hidden_in, cotangent, lengths, mixer_gain, query_weight, key_weight, value_weight, beta_weight, alpha_weight,
    gate_weight, out_weight, feed_gain, feed_gate, feed_up, feed_down, conv_taps, decay_log, decay_bias, head_gain,
):
    ns, nb = lax.axis_size("seq"), lax.axis_size("batch")
    heads = decay_log.shape[0]
    rep = ns // heads
    assert hidden_in.shape[0] == 1 and ns == rep * heads and ns % nb == 0
    tok, width = hidden_in.shape[1:]
    rows = query_weight.shape[0]
    share = feed_gate.shape[1] // nb
    halves = ns // nb
    sds = jax.ShapeDtypeStruct
    vmem, hbm = pl.BlockSpec(memory_space=pltpu.VMEM), pl.BlockSpec(memory_space=pl.ANY)
    hidden, cot = hidden_in[0], cotangent[0]

    small = jnp.concatenate(
        [
            jnp.swapaxes(beta_weight.reshape(rows, 2, heads), 1, 2),
            alpha_weight[:, :, None],
            jnp.broadcast_to(mixer_gain[:, None, None], (rows, heads, 1)),
            jnp.broadcast_to(feed_gain[:, None, None], (rows, heads, 1)),
            jnp.zeros((rows, heads, DK - 5), BF16),
        ],
        axis=-1,
    )
    mix = jnp.concatenate(
        [
            query_weight.reshape(rows, heads, 1, DK),
            jnp.swapaxes(key_weight.reshape(rows, 2, heads, DK), 1, 2),
            jnp.swapaxes(value_weight.reshape(rows, 2, heads, DK), 1, 2),
            gate_weight.reshape(rows, heads, 1, DK),
            small[:, :, None],
            out_weight.T.reshape(rows, heads, 1, DK),
        ],
        axis=2,
    )
    mix = jnp.repeat(jnp.swapaxes(mix, 0, 1).reshape(heads, rows, 8 * DK), rep, axis=0)
    feed = jnp.stack(
        [jnp.swapaxes(w.reshape(rows, nb, share), 0, 1) for w in (feed_gate, feed_up, feed_down.T)], axis=1
    )
    nz = ns // 2
    hid_all, wm, ff = comm_call(
        functools.partial(gather_kernel, ns, nb),
        [
            (sds((ns, tok, width), BF16), hbm),
            (sds((ns, nb, rows, 8 * DK), BF16), hbm),
            (sds((3, nb, rows, share), BF16), hbm),
        ],
        [dma(3), dma(2 * nz - 1), dma(2 * nz - 1), dma(ns * nb), dma(ns * nb), dma(nb), dma(nb)],
        0, "gather", (hidden, mix, feed), [vmem] * 3,
    )
    wm = wm.reshape(width, 8 * DK)
    ff = lax.all_gather(ff.reshape(3, nb * rows, share), "seq", axis=1, tiled=True)
    gains = wm[:, 6 * DK + 3 : 6 * DK + 5].astype(F32).T
    gain_in, gain_mid = gains[0:1], gains[1:2]
    gain_head = head_gain.astype(F32)[None]

    part, normed, pre, gl, sm, gated, raw, *maps = mixer_fwd(
        lengths, decay_log, decay_bias, hid_all.reshape(ns * tok, width), gain_in, wm, conv_taps, gain_head, rep, heads
    )
    block = lambda n, kind=BF16: pltpu.VMEM((n, tok, width), kind)
    after, nm_all, cot_all = comm_call(
        functools.partial(mid_kernel, ns, nb),
        [
            (sds((tok, width), F32), vmem),
            (sds((nb, tok, width), BF16), hbm),
            (sds((nb, tok, width), BF16), hbm),
        ],
        [block(nz), block(nz), block(nz), pltpu.VMEM((tok, width), BF16), dma(2), dma(2 * nz), dma(2 * nz)]
        + [dma(nb)] * 4,
        1, "mid", (part.reshape(ns, tok, width), hidden, cot, gain_mid), [vmem] * 4,
    )
    nm_all, cot_all = nm_all.reshape(nb * tok, width), cot_all.reshape(nb * tok, width)
    w_gate, w_up, w_down = ff[0], ff[1], ff[2]
    dot = lambda a, b, dims: lax.dot_general(a, b, dims, preferred_element_type=F32)
    gate_act = dot(nm_all, w_gate, NN)
    up_act = dot(nm_all, w_up, NN)
    sig = jax.nn.sigmoid(gate_act)
    act = (gate_act * sig * up_act).astype(BF16)
    d_act = dot(cot_all, w_down, NN)
    d_gate = (d_act * up_act * sig * (1.0 + gate_act * (1.0 - sig))).astype(BF16)
    d_up = (d_act * gate_act * sig).astype(BF16)
    pout = dot(act, w_down, NT).astype(BF16).reshape(nb, tok, width)
    pmid = (dot(d_gate, w_gate, NT) + dot(d_up, w_up, NT)).astype(BF16).reshape(nb, tok, width)
    block_out, d_stream, dbr_all, gfeed = comm_call(
        functools.partial(turn_kernel, ns, nb),
        [
            (sds((tok, width), BF16), vmem),
            (sds((tok, width), F32), vmem),
            (sds((ns, tok, width), BF16), hbm),
            (sds((1, width), F32), vmem),
        ],
        [block(nb), block(nb), pltpu.VMEM((tok, width), BF16), dma(1)] + [dma(nb)] * 4 + [dma(2 * nz - 1)] * 2,
        2, "turn", (pmid, pout, after, cot, gain_mid), [vmem] * 5,
    )
    dbr_all = dbr_all.reshape(ns * tok, width)
    g_gate, g_up = dot(nm_all, d_gate, TN), dot(nm_all, d_up, TN)
    g_down = dot(act, cot_all, TN)
    g_down = jnp.swapaxes(g_down.astype(BF16).reshape(halves, share // halves, nb, width // nb), 1, 2)
    over_seq = lambda g: lax.psum_scatter(g, "seq", scatter_dimension=0, tiled=True)
    g_gate = over_seq(g_gate.astype(BF16)).astype(F32)
    g_up = over_seq(g_up.astype(BF16)).astype(F32)
    g_down = over_seq(g_down.reshape(ns, share // halves, width // nb))[0]
    moves = [
        (s * nb + b, (b * halves + s // nb) * nb + s % nb) for s in range(ns) for b in range(nb)
    ]
    g_down = lax.ppermute(g_down, ("seq", "batch"), moves).astype(F32)

    dall, dnp, tap_sums = mixer_bwd(
        lengths, decay_log, decay_bias, dbr_all, wm, conv_taps, gain_head, (pre, gl, sm, raw, *maps), rep, heads
    )
    g_mix = dot(normed, dall, TN)
    g_out = dot(gated, dbr_all, TN)
    s_at = lax.axis_index("seq")
    if rep > 1:
        g_out = lax.dynamic_slice_in_dim(g_out, (s_at % rep) * (DK // rep), DK // rep, 0)
    g_out = jnp.swapaxes(g_out.astype(BF16).reshape(DK // rep, nb, width // nb), 0, 1)
    grads = g_mix[:, : 6 * DK].astype(BF16).reshape(ns, width // ns, 6 * DK)
    smalls = jnp.concatenate([tap_sums[:4], g_mix[:, 6 * DK : 6 * DK + 3].T.reshape(4, 6 * DK)], axis=0)
    nq = heads * rep // nb
    nk = ns // nb
    cw = DK // rep
    wrows = width // ns
    grad_in, slots, gout_sum, small_all, vec_sum = comm_call(
        functools.partial(last_kernel, ns, nb, rep),
        [
            (sds((tok, width), BF16), vmem),
            (sds((6 * nq, wrows, cw), BF16), vmem),
            (sds((DK // rep, width // nb), F32), vmem),
            (sds((ns, 8, 6 * DK), F32), vmem),
            (sds((2, width), F32), vmem),
        ],
        [
            block(nz), block(nz), block(nz),
            pltpu.VMEM((nk * nb, wrows, 6 * DK), BF16),
            pltpu.VMEM((nk * 6, wrows, cw), BF16),
            pltpu.VMEM((nb, DK // rep, width // nb), BF16),
            pltpu.VMEM((nb, 8, 6 * DK), F32),
            pltpu.VMEM((8, 6 * DK), F32),
            pltpu.VMEM((nb, 2, width), F32),
            pltpu.VMEM((2, width), F32),
            pltpu.VMEM((ns, 2, width), F32),
            pltpu.SemaphoreType.REGULAR,
            dma(1), dma(2 * nz), dma(2 * nz), dma(nk * nb), dma(nk * nb), dma(nk * 6), dma(6 * nq),
            dma(nb), dma(nb), dma(nb), dma(nb), dma(ns), dma(ns), dma(nb), dma(nb), dma(ns), dma(ns),
        ],
        3, "last",
        (dnp.reshape(ns, tok, width), grads, g_out, smalls, hidden, gain_in, d_stream, gfeed), [vmem] * 8,
    )
    def owned(first, count):
        return jnp.swapaxes(slots[first : first + count], 0, 1).reshape(wrows, count * cw).astype(F32)

    small_all = small_all[::rep]
    head_weight = small_all[:, 4:8].reshape(heads, 3, width)
    return (
        block_out[None],
        grad_in[None],
        vec_sum[0],
        owned(0, nq),
        owned(nq, 2 * nq),
        owned(3 * nq, 2 * nq),
        jnp.transpose(head_weight[:, :2], (2, 1, 0)).reshape(width, 2 * heads),
        head_weight[:, 2].T,
        owned(5 * nq, nq),
        gout_sum,
        vec_sum[1],
        g_gate,
        g_up,
        g_down,
        jnp.transpose(small_all[:, :4, : 5 * DK].reshape(heads, 4, 5, DK), (1, 2, 0, 3)).reshape(4, -1),
        small_all[:, 1, 5 * DK],
        small_all[:, 2, 5 * DK],
        jnp.sum(small_all[:, 0, 5 * DK :], axis=0),
    )


def solution(mesh):
    both = ("seq", "batch")
    tokens, split_rows, grid = P("batch", "seq", None), P(both, None), P("seq", "batch")
    return jax.shard_map(
        on_device,
        mesh=mesh,
        in_specs=(
            tokens, tokens, P("batch"), P(both), split_rows, split_rows, split_rows, split_rows, split_rows,
            split_rows, P(None, both), P(both), split_rows, split_rows, P(None, both), P(), P(), P(), P(),
        ),
        out_specs=(
            tokens, tokens, P(), grid, grid, grid, P(), P(), grid, grid, P(), grid, grid, grid, P(), P(), P(), P(),
        ),
        check_vma=False,
    )
```

```python
import functools
import jax
import jax.numpy as jnp
from jax import lax
from jax.experimental import pallas as pl
from jax.experimental.pallas import tpu as pltpu
from jax.sharding import PartitionSpec as P

F32, BF16 = jnp.float32, jnp.bfloat16
EPS = 1e-05
DK = 128
HALF = 64
GS = 4
GB = GS * HALF
NN = (((1,), (0,)), ((), ()))
NT = (((1,), (1,)), ((), ()))
TN = (((0,), (0,)), ((), ()))


def mm(a, b, dims=NN):
    return lax.dot_general(a.astype(BF16), b.astype(BF16), dims, preferred_element_type=F32)


def split(a):
    hi = a.astype(BF16)
    return hi, (a - hi.astype(F32)).astype(BF16)


def mm3(a, b, dims=NN):
    (ah, al), (bh, bl) = (x if isinstance(x, tuple) else split(x) for x in (a, b))
    return (
        lax.dot_general(ah, bl, dims, preferred_element_type=F32)
        + lax.dot_general(al, bh, dims, preferred_element_type=F32)
    ) + lax.dot_general(ah, bh, dims, preferred_element_type=F32)


def iota(shape, axis):
    return lax.broadcasted_iota(jnp.int32, shape, axis)


def sub_masks():
    rows, cols = iota((128, 128), 0), iota((128, 128), 1)
    tr, tc = 2 * (rows & 63) + (rows >> 6), 2 * (cols & 63) + (cols >> 6)
    strict = tr > tc
    levels = []
    for bits in range(3, 7):
        same_up = (tr >> (bits + 1)) == (tc >> (bits + 1))
        levels.append(strict & same_up & ((tr >> bits) != (tc >> bits)))
    base = strict & ((tr >> 3) == (tc >> 3))
    return strict, base, levels


def unit(a):
    r = lax.rsqrt(jnp.sum(a * a, axis=-1, keepdims=True) + EPS)
    return a * r, r


def softplus(x):
    return jnp.maximum(x, 0.0) + jnp.log1p(jnp.exp(-jnp.abs(x)))


def lane(x, width=128):
    return jnp.broadcast_to(x, (x.shape[0], width))


def gates(sm, dec_bias):
    return jax.nn.sigmoid(sm[:, 0:1]), jax.nn.sigmoid(sm[:, 1:2]), sm[:, 2:3] + dec_bias


def span_decay(gb, tri):
    c = mm3(tri, gb)
    ct = jnp.transpose(jnp.concatenate([c, c], axis=0))[:64]
    e = jnp.exp(jnp.minimum(c - ct, 0.0))
    return c, e


def conv_mix(buf, taps):
    mix = taps[0:1] * buf[5 : 5 + GB]
    for j in range(1, 4):
        mix = mix + taps[j : j + 1] * buf[5 + j : 5 + j + GB]
    return mix


def head_taps(taps_ref, head, heads):
    parts = []
    for col in (head, heads + head, 2 * heads + head, 3 * heads + head, 4 * heads + head):
        parts.append(taps_ref[:, pl.ds(pl.multiple_of(col * 128, 128), 128)].astype(F32))
    return jnp.concatenate(parts, axis=1)


MESH = pl.DeviceIdType.MESH
SPAN_ROWS = 5 * 128 + HALF
SAVE_ROWS = GS * SPAN_ROWS + 3 * GB


class Place:
    def __init__(self, ns, nb):
        self.ns, self.nb, self.nz = ns, nb, ns // 2
        self.s, self.b = lax.axis_index("seq"), lax.axis_index("batch")
        self.z, self.c = self.s // 2, lax.rem(self.s, 2)
        self.sib = self.s + 1 - 2 * self.c

    def seq_at(self, ds):
        return lax.rem(self.s + ds, self.ns)

    def seq_before(self, ds):
        return lax.rem(self.s + self.ns - ds, self.ns)

    def peer(self, mask):
        out, bit = 0, 1
        while bit < self.nb:
            mine, other = lax.rem(self.b // bit, 2), lax.rem(mask // bit, 2) if not isinstance(mask, int) else mask // bit % 2
            out = out + bit * (mine + other - 2 * mine * other)
            bit *= 2
        return out

    def peers(self):
        return range(self.nb - 1, 0, -1)


def greet(at):
    barrier = pltpu.get_barrier_semaphore()
    for ds in range(1, at.ns):
        pl.semaphore_signal(barrier, inc=1, device_id={"seq": at.seq_at(ds)}, device_id_type=MESH)
    for m in at.peers():
        pl.semaphore_signal(barrier, inc=1, device_id={"batch": at.peer(m)}, device_id_type=MESH)


def enter(at):
    pl.semaphore_wait(pltpu.get_barrier_semaphore(), at.ns + at.nb - 2)


def send(src, dst, send_sem, recv_sem, where):
    return pltpu.make_async_remote_copy(
        src_ref=src, dst_ref=dst, send_sem=send_sem, recv_sem=recv_sem, device_id=where, device_id_type=MESH
    )


def fetch(pairs, sem):
    copies = [pltpu.make_async_copy(src, dst, sem.at[k]) for k, (src, dst) in enumerate(pairs)]
    for copy in copies:
        copy.start()
    return copies


class BatchGather:
    def __init__(self, at, src, out_at, ssem, rsem):
        self.copies = [
            send(src, out_at, ssem.at[m], rsem.at[m], {"batch": at.peer(m)}) for m in at.peers()
        ]

    def start(self):
        for copy in self.copies:
            copy.start()

    def finish(self):
        for copy in self.copies:
            copy.wait_recv()
        for copy in self.copies:
            copy.wait_send()


class SeqGather:
    def __init__(self, at, src, out, ssem, rsem):
        self.at, self.src, self.out, self.ssem, self.rsem = at, src, out, ssem, rsem

    def hop(self, t, up):
        at = self.at
        origin = at.z - (t - 1) if up else at.z + (t - 1)
        slot = 2 * origin + at.c
        src = self.src if t == 1 else self.out.at[slot]
        to = at.s + 2 if up else at.s - 2
        k = t if up else at.nz + t
        return send(src, self.out.at[slot], self.ssem.at[k], self.rsem.at[k], {"seq": to})

    def can_send(self, t, up):
        at = self.at
        if up:
            return jnp.logical_and(at.z - (t - 1) >= 0, at.z + 1 < at.nz)
        return jnp.logical_and(at.z + (t - 1) < at.nz, at.z >= 1)

    def can_recv(self, t, up):
        return self.at.z - t >= 0 if up else self.at.z + t < self.at.nz

    def across(self, t, up):
        at, nz = self.at, self.at.nz
        k = 2 * nz + (t if up else nz + t)
        origin = 0 if t == 0 else (-t if up else t)
        slot = 2 * (at.z + origin) + at.c
        src = self.src if t == 0 else self.out.at[slot]
        return send(src, self.out.at[slot], self.ssem.at[k], self.rsem.at[k], {"seq": at.sib})

    def start(self):
        for up in (True, False):
            pl.when(self.can_send(1, up))(lambda: self.hop(1, up).start())
        self.across(0, True).start()

    def forward(self, t):
        for up in (True, False):

            @pl.when(self.can_recv(t, up))
            def _():
                self.hop(t, up).wait_recv()
                if t + 1 < self.at.nz:
                    pl.when(self.can_send(t + 1, up))(lambda: self.hop(t + 1, up).start())
                self.across(t, up).start()

    def finish(self):
        self.across(0, True).wait()
        for t in range(1, self.at.nz):
            for up in (True, False):
                pl.when(self.can_recv(t, up))(lambda: self.across(t, up).wait())
                pl.when(self.can_send(t, up))(lambda: self.hop(t, up).wait_send())


class SeqSum:
    def __init__(self, at, part, got, out, far, sems):
        self.at, self.part, self.got, self.out, self.far = at, part, got, out, far
        self.pair_s, self.pair_r, self.hop_s, self.hop_r = sems

    def pair(self, i):
        at = self.at
        return send(self.part.at[i, 1 - at.c], self.got.at[i], self.pair_s.at[i], self.pair_r.at[i], {"seq": at.sib})

    def hop(self, i):
        at = self.at
        dz = lax.rem(i - at.z + at.nz, at.nz)
        return send(self.out.at[i], self.far.at[dz], self.hop_s.at[i], self.hop_r.at[dz], {"seq": 2 * i + at.c})

    def start(self, i):
        self.pair(i).start()

    def flush(self, i):
        self.pair(i).wait_recv()

        @pl.when(i != self.at.z)
        def _():
            mine = self.part[i, self.at.c].astype(F32)
            self.out[i] = (mine + self.got[i].astype(F32)).astype(BF16)
            self.hop(i).start()

    def finish(self):
        at = self.at
        total = self.part[at.z, at.c].astype(F32) + self.got[at.z].astype(F32)
        for dz in range(1, at.nz):
            send(self.out.at[0], self.far.at[dz], self.hop_s.at[0], self.hop_r.at[dz], {"seq": at.sib}).wait_recv()
            total = total + self.far[dz].astype(F32)
        return total

    def drain(self):
        for i in range(self.at.nz):
            self.pair(i).wait_send()
            pl.when(i != self.at.z)(lambda: self.hop(i).wait_send())


def norm_rows(x):
    return lax.rsqrt(jnp.mean(x * x, axis=-1, keepdims=True) + EPS)


def gather_kernel(
    ns, nb, rep, heads,
    hid, wq, wk, wv, wg, wo, beta, alpha, gain_in, gain_mid, fg, fu, fd,
    hid_out, wm_out, ff_out,
    hv, qv, kv, vv, gv, ov, fgv, fuv, fdv, wbuf, fbuf, isem, lsem, hs, hr, ws, wr, os_, or_, fs, fr,
):
    at = Place(ns, nb)
    greet(at)
    loads = fetch(
        [(hid, hv), (wq, qv), (wk, kv), (wv, vv), (wg, gv), (wo, ov), (fg, fgv), (fu, fuv), (fd, fdv)], isem
    )
    rows = beta.shape[0]
    lanes = iota((rows, 128), 1)
    eye = iota((rows, rows), 0) == iota((rows, rows), 1)
    column = lambda ref: jnp.sum(jnp.where(eye, ref[...].astype(F32), 0.0), axis=1, keepdims=True)
    be, al = beta[...].astype(F32), alpha[...].astype(F32)
    tail = jnp.where(lanes == 3, column(gain_in), jnp.where(lanes == 4, column(gain_mid), 0.0))
    share = fbuf.shape[3]
    for copy in loads[1:6]:
        copy.wait()
    for h in range(heads):
        col = lambda j: slice(128 * (j * heads + h), 128 * (j * heads + h) + 128)
        small = jnp.where(lanes == 0, be[:, h : h + 1], tail)
        small = jnp.where(lanes == 1, be[:, heads + h : heads + h + 1], small)
        small = jnp.where(lanes == 2, al[:, h : h + 1], small)
        parts = (
            qv[:, col(0)], kv[:, col(0)], kv[:, col(1)], vv[:, col(0)], vv[:, col(1)], gv[:, col(0)],
            small.astype(BF16), ov[:, col(0)],
        )
        for j, p in enumerate(parts):
            wbuf[h, :, 128 * j : 128 * j + 128] = p
    loads[0].wait()
    enter(at)

    def piece(to, where):
        return send(wbuf.at[to // rep], wm_out.at[at.s, at.b], ws.at[to], wr.at[at.s], where)

    def arrives(origin):
        send(wbuf.at[0], wm_out.at[origin, at.b], ws.at[0], wr.at[origin], {"seq": at.sib}).wait_recv()

    def pass_on(zo):
        for m in at.peers():
            both = wm_out.at[pl.ds(2 * zo, 2), at.b]
            send(both, both, os_.at[zo, m], or_.at[zo, m], {"batch": at.peer(m)}).start()

    def around(fn):
        for t in range(1, at.nz):
            pl.when(at.z + t < at.nz)(lambda: fn(at.z + t))
            pl.when(at.z - t >= 0)(lambda: fn(at.z - t))

    def scatter(zo):
        for core in range(2):
            piece(2 * zo + core, {"seq": 2 * zo + core}).start()

    own = pltpu.make_async_copy(wbuf.at[at.s // rep], wm_out.at[at.s, at.b], lsem.at[0])
    own.start()
    piece(at.sib, {"seq": at.sib}).start()
    around(scatter)
    line = SeqGather(at, hv, hid_out, hs, hr)
    line.start()
    place = pltpu.make_async_copy(hv, hid_out.at[at.s], lsem.at[1])
    place.start()
    arrives(at.sib)
    own.wait()
    pass_on(at.z)
    for copy in loads[6:]:
        copy.wait()
    for b in range(nb):
        for j, w in enumerate((fgv, fuv, fdv)):
            fbuf[b, j] = w[:, share * b : share * (b + 1)]
    kept = pltpu.make_async_copy(fbuf.at[at.b], ff_out.at[:, at.b], lsem.at[2])
    kept.start()
    cols = [
        send(fbuf.at[at.peer(m)], ff_out.at[:, at.b], fs.at[m], fr.at[m], {"batch": at.peer(m)}) for m in at.peers()
    ]

    def relay(zo):
        for core in range(2):
            arrives(2 * zo + core)
        pass_on(zo)

    for t in range(1, at.nz):
        pl.when(at.z + t < at.nz)(lambda: relay(at.z + t))
        pl.when(at.z - t >= 0)(lambda: relay(at.z - t))
        line.forward(t)
    for copy in cols:
        copy.start()
    line.finish()

    def settle(zo):
        for m in at.peers():
            both = wm_out.at[pl.ds(2 * zo, 2), at.b]
            send(both, both, os_.at[zo, m], or_.at[zo, m], {"batch": at.peer(m)}).wait()

    for zo in range(at.nz):
        settle(zo)
    piece(at.sib, {"seq": at.sib}).wait_send()

    def sent(zo):
        for core in range(2):
            piece(2 * zo + core, {"seq": 2 * zo + core}).wait_send()

    around(sent)
    for copy in cols:
        copy.wait()
    place.wait()
    kept.wait()


def front_kernel(
    ns, nb, rep, heads,
    len_ref, dlog_ref, dbias_ref, hid_hbm, w_hbm, taps_hbm, hg_ref, cot_hbm,
    normed_hbm, pre_hbm, gated_hbm, save_hbm, gains, after, nm_out, cot_out,
    hid_ref, w_ref, taps_ref, cot, nm, zero, save, preb, normedb, gatedb,
    buf, state, part, got, out, far, isem, bsem, lsem, osem, ps, pr, qs, qr, ms, mr, cs, cr,
):
    at = Place(ns, nb)
    greet(at)
    steps = at.nz
    loads = fetch([(w_hbm, w_ref), (taps_hbm, taps_ref), (cot_hbm, cot)], isem)

    def block_in(i):
        return pltpu.make_async_copy(hid_hbm.at[pl.ds(2 * i, 2)], hid_ref.at[pl.ds(2 * i, 2)], bsem.at[i])

    for i in range(steps):
        block_in(i).start()
    zero[...] = jnp.zeros_like(zero)
    for copy in loads:
        copy.wait()

    def saves(i):
        slot = lax.rem(i, 2)
        first = pl.multiple_of(i * GB, GB)
        here = pl.ds(first, GB)
        return [
            pltpu.make_async_copy(save.at[slot], save_hbm.at[i], osem.at[slot, 0]),
            pltpu.make_async_copy(preb.at[slot], pre_hbm.at[pl.ds(pl.multiple_of(first + 8, 8), GB)], osem.at[slot, 1]),
            pltpu.make_async_copy(normedb.at[slot], normed_hbm.at[here], osem.at[slot, 2]),
            pltpu.make_async_copy(gatedb.at[slot], gated_hbm.at[here], osem.at[slot, 3]),
        ]

    head = at.s // rep
    state[...] = jnp.zeros_like(state)
    buf[0:8] = jnp.zeros((8, 640), F32)
    gains[...] = jnp.transpose(w_ref[:, 768:896].astype(F32))[0:8]
    taps = head_taps(taps_ref, head, heads)
    hg = hg_ref[...].astype(F32)
    rows = SeqSum(at, part, got, out, far, (ps, pr, qs, qr))
    enter(at)
    mine = pltpu.make_async_copy(cot, cot_out.at[at.b], lsem.at[0])
    mine.start()
    edge = pltpu.make_async_copy(zero, pre_hbm.at[0:8], lsem.at[1])
    edge.start()
    cots = BatchGather(at, cot, cot_out.at[at.b], cs, cr)
    cots.start()

    def step(i, _):
        first = i * GB
        slot = lax.rem(i, 2)

        @pl.when(i >= 2)
        def _():
            for copy in saves(i - 2):
                copy.wait()

        def keep_map(kind, s, value):
            row = SPAN_ROWS * s + 128 * kind
            save[slot, row : row + value.shape[0]] = value

        def keep_rows(kind, value):
            row = SPAN_ROWS * GS + GB * kind
            save[slot, row : row + GB] = value

        block_in(i).wait()
        x = hid_ref[pl.ds(2 * i, 2)].reshape(GB, -1).astype(F32)
        normed = (x * norm_rows(x) * gains[3:4]).astype(BF16)
        normedb[slot] = normed
        proj = mm(normed, w_ref[:, 0:896])
        pre = proj[:, 0:640].astype(BF16).astype(F32)
        preb[slot] = pre
        gl, sm = proj[:, 640:768], proj[:, 768:896]
        keep_rows(0, gl)
        keep_rows(1, sm)
        buf[8 : 8 + GB] = pre
        mix = conv_mix(buf, taps)
        buf[0:8] = pre[GB - 8 : GB]
        act = mix * jax.nn.sigmoid(mix)
        q = unit(act[:, 0:128])[0] * DK ** (-0.5)
        k0, k1 = unit(act[:, 128:256])[0], unit(act[:, 256:384])[0]
        v0, v1 = act[:, 384:512], act[:, 512:640]
        keep = (first + iota((GB, 1), 0) < len_ref[0]).astype(F32)
        sig0, sig1, al = gates(sm, dbias_ref[head])
        b0, b1 = lane(sig0 * keep), lane(sig1 * keep)
        eg = jnp.exp(jnp.full((1, 1), dlog_ref[head], F32))
        g = lane(-eg * softplus(al) * keep)
        strict, base, levels = sub_masks()
        eye = (iota((128, 128), 0) == iota((128, 128), 1)).astype(F32)
        tri = (iota((64, 64), 0) >= iota((64, 64), 1)).astype(F32)
        causal = iota((64, 128), 0) >= (iota((64, 128), 1) & 63)
        K, Q, V, B, C, N, PM, Kc = [], [], [], [], [], [], [], []
        for s in range(GS):
            sl = slice(64 * s, 64 * s + 64)
            K.append(jnp.concatenate([k0[sl], k1[sl]], axis=0))
            V.append(jnp.concatenate([v0[sl], v1[sl]], axis=0))
            B.append(jnp.concatenate([b0[sl], b1[sl]], axis=0))
            Q.append(q[sl])
            c, e = span_decay(g[sl], tri)
            C.append(c)
            ee = jnp.concatenate([e, e], axis=0)
            gram = mm3(jnp.concatenate([K[s], Q[s]], axis=0), K[s], NT)
            N.append(jnp.where(strict, gram[:128] * ee, 0.0) * B[s])
            PM.append(jnp.where(causal, gram[128:] * e, 0.0))
            cc = jnp.concatenate([c, c], axis=0)
            Kc.append(jnp.exp(cc[63:64] - cc) * K[s])
            keep_map(3, s, N[s])
            keep_map(5, s, PM[s])
        n1 = [jnp.where(base, n, 0.0) for n in N]
        n1s = [split(n) for n in n1]
        n2 = [mm3(a, a) for a in n1s]
        n2s = [split(n) for n in n2]
        n3 = [mm3(a, b) for a, b in zip(n1s, n2s)]
        n4 = [mm3(a, a) for a in n2s]
        y = [eye - a + b - c for a, b, c in zip(n1, n2, n3)]
        X = [a + mm3(a, b) for a, b in zip(y, n4)]
        for lv in levels:
            xs = [split(x_) for x_ in X]
            bl = [jnp.where(lv, n, 0.0) for n in N]
            xb = [mm3(a, b) for a, b in zip(xs, bl)]
            X = [x_ - mm3(a, b) for x_, a, b in zip(X, xb, xs)]
        pl.when(i > 0)(lambda: rows.flush(i - 1))
        W, U = [], []
        for s in range(GS):
            cc = jnp.concatenate([C[s], C[s]], axis=0)
            rhs = jnp.concatenate([B[s] * jnp.exp(cc) * K[s], B[s] * V[s]], axis=1)
            wu = mm3(X[s], rhs)
            W.append(wu[:, :128])
            U.append(wu[:, 128:])
            keep_map(0, s, X[s])
            keep_map(1, s, W[s])
        S = state[...]
        raw = []
        Ws = [split(a) for a in W]
        Kcs = [split(a) for a in Kc]
        for s in range(GS):
            keep_map(4, s, S)
            ss = split(S)
            vn = U[s] - mm3(Ws[s], ss)
            keep_map(2, s, vn)
            vs = split(vn)
            raw.append(jnp.exp(C[s]) * mm3(Q[s], ss) + mm3(PM[s], vs))
            S = jnp.exp(C[s][63:64]) * S + mm3(Kcs[s], vs, TN)
        state[...] = S
        o = jnp.concatenate(raw, axis=0)
        keep_rows(2, o)
        gated = (o * norm_rows(o) * hg * (gl * jax.nn.sigmoid(gl))).astype(BF16)
        gatedb[slot] = gated
        for copy in saves(i):
            copy.start()
        if rep > 1:
            gated = jnp.where(lax.rem(at.s, rep) == 0, gated, jnp.zeros_like(gated))
        part[i] = mm(gated, w_ref[:, 896:1024], NT).astype(BF16).reshape(2, GB // 2, -1)
        rows.start(i)
        return 0

    lax.fori_loop(0, steps, step, 0)
    rows.flush(steps - 1)
    total = rows.finish() + hid_ref[at.s].astype(F32)
    after[...] = total
    nm[...] = (total * norm_rows(total) * gains[4:5]).astype(BF16)
    mids = BatchGather(at, nm, nm_out.at[at.b], ms, mr)
    mids.start()
    own = pltpu.make_async_copy(nm, nm_out.at[at.b], lsem.at[2])
    own.start()
    rows.drain()
    for i in (steps - 2, steps - 1):
        for copy in saves(i):
            copy.wait()
    cots.finish()
    mids.finish()
    mine.wait()
    edge.wait()
    own.wait()


def feed_kernel(
    ns, nb,
    nm_hbm, cot_hbm, ff_hbm, after, gains,
    block_out, d_stream, dbr_out, gfeed, sums,
    nm_all, cot_all, ff, acts, dgs, dus, pmid, pout, got_m, got_o, dbr, gbuf, gdown,
    isem, lsem, ms, mr, os_, or_, gs, gr, ds_s, dr_s,
):
    at = Place(ns, nb)
    greet(at)
    loads = fetch([(nm_hbm, nm_all), (cot_hbm, cot_all), (ff_hbm, ff)], isem)
    for copy in loads:
        copy.wait()
    tok = after.shape[0]
    share = ff.shape[2]
    enter(at)

    def mid_copy(m):
        to = at.peer(m)
        return send(pmid.at[to], got_m.at[m], ms.at[m], mr.at[m], {"batch": to})

    def out_copy(m):
        to = at.peer(m)
        return send(pout.at[to], got_o.at[m], os_.at[m], or_.at[m], {"batch": to})

    def both(ref, one, two):
        return jnp.concatenate([ref[one], ref[two]], axis=0)

    def pair(j, _):
        m = nb - 1 - 2 * j
        one, two = at.peer(m), at.peer(m - 1)
        x, d = both(nm_all, one, two), both(cot_all, one, two)
        ga, ua, da = mm(x, ff[0]), mm(x, ff[1]), mm(d, ff[2])
        sig = jax.nn.sigmoid(ga)
        act = (ga * sig * ua).astype(BF16)
        dg = (da * ua * sig * (1.0 + ga * (1.0 - sig))).astype(BF16)
        du = (da * ga * sig).astype(BF16)
        for ref, value in ((acts, act), (dgs, dg), (dus, du)):
            ref[one] = value[:tok]
            ref[two] = value[tok:]
        p = (mm(dg, ff[0], NT) + mm(du, ff[1], NT)).astype(BF16)
        pmid[one] = p[:tok]
        pmid[two] = p[tok:]
        mid_copy(m).start()
        pl.when(m > 1)(lambda: mid_copy(m - 1).start())
        return 0

    lax.fori_loop(0, nb // 2, pair, 0)

    def outs(j, _):
        m = nb - 1 - 2 * j
        one, two = at.peer(m), at.peer(m - 1)
        p = mm(both(acts, one, two), ff[2], NT).astype(BF16)
        pout[one] = p[:tok]
        pout[two] = p[tok:]
        out_copy(m).start()
        pl.when(m > 1)(lambda: out_copy(m - 1).start())
        return 0

    lax.fori_loop(0, nb // 2, outs, 0)
    x = after[...]
    d_mid = pmid[at.b].astype(F32)
    for m in at.peers():
        mid_copy(m).wait_recv()
        d_mid = d_mid + got_m[m].astype(F32)
    r = norm_rows(x)
    y = x * r
    gfeed[...] = jnp.sum(d_mid * y, axis=0, keepdims=True)
    dy = d_mid * gains[4:5]
    ds_ = cot_all[at.b].astype(F32) + r * (dy - y * jnp.mean(dy * y, axis=-1, keepdims=True))
    d_stream[...] = ds_
    dbr[...] = ds_.astype(BF16)
    line = SeqGather(at, dbr, dbr_out, gs, gr)
    line.start()
    own_rows = pltpu.make_async_copy(dbr, dbr_out.at[at.s], lsem.at[0])
    own_rows.start()
    halves = ns // nb
    deep, cols = share // halves, nm_all.shape[2] // ns
    flat = lambda ref: ref[...].reshape(nb * tok, -1)
    g = mm(flat(acts), flat(cot_all), TN).astype(BF16)
    for b in range(nb):
        for h in range(halves):
            for t in range(halves):
                gdown[b, h, deep * t : deep * (t + 1)] = g[
                    deep * h : deep * (h + 1), cols * (halves * b + t) : cols * (halves * b + t + 1)
                ]
    down = lambda b, h: sums.at[halves * b + h, pl.ds(2 * share, share)]
    moved = [
        send(gdown.at[at.peer(m), h], down(at.b, h), ds_s.at[m, h], dr_s.at[m, h], {"batch": at.peer(m)})
        for m in at.peers()
        for h in range(halves)
    ]
    for copy in moved:
        copy.start()
    kept = [
        pltpu.make_async_copy(gdown.at[at.b, h], down(at.b, h), lsem.at[1 + h]) for h in range(halves)
    ]
    line.forward(1)
    for k, left in enumerate((dgs, dus)):
        g = mm(flat(left), flat(nm_all), TN).astype(BF16)
        for i in range(ns):
            gbuf[k, i] = g[:, cols * i : cols * (i + 1)]
        kept.append(
            pltpu.make_async_copy(gbuf.at[k], sums.at[:, pl.ds(share * k, share)], lsem.at[1 + halves + k])
        )
        if k == 0:
            line.forward(2)
    for copy in kept:
        copy.start()
    for t in range(3, at.nz):
        line.forward(t)
    total = after[...] + pout[at.b].astype(F32)
    for m in at.peers():
        out_copy(m).wait_recv()
        total = total + got_o[m].astype(F32)
    block_out[...] = total.astype(BF16)
    line.finish()
    for copy in moved:
        copy.wait()
    for m in at.peers():
        mid_copy(m).wait_send()
        out_copy(m).wait_send()
    for copy in kept:
        copy.wait()
    own_rows.wait()


def back_kernel(
    ns, nb, rep, heads,
    len_ref, dlog_ref, dbias_ref, dbr_hbm, w_hbm, taps_hbm, hg_ref, normed_hbm, pre_hbm, gated_hbm, save_hbm,
    hid_hbm, gains, d_stream, gfeed,
    grad_in, slots, gout_sum, small_all, vec_sum,
    dbr_ref, w_ref, taps_ref, hid, save, buf, normedb, gatedb, isem, bsem,
    dbuf, dstate, small, gw, go, part, got, out, far, grads, gout, got_g, piece, got_o, got_s, got_v, vec, got_w,
    ready, ps, pr, qs, qr, gs, gr, bs, br, os_, or_, ss, sr, us, ur, vs_, vr, xs, xr,
):
    at = Place(ns, nb)
    greet(at)
    steps = at.nz
    loads = fetch([(w_hbm, w_ref), (taps_hbm, taps_ref), (hid_hbm, hid)], isem)

    def block_in(i):
        slot = lax.rem(i, 2)
        first = pl.multiple_of(i * GB, GB)
        here = pl.ds(first, GB)
        return [
            pltpu.make_async_copy(save_hbm.at[i], save.at[slot], bsem.at[slot, 0]),
            pltpu.make_async_copy(pre_hbm.at[pl.ds(first, 8 + GB)], buf.at[slot], bsem.at[slot, 1]),
            pltpu.make_async_copy(normed_hbm.at[here], normedb.at[slot], bsem.at[slot, 2]),
            pltpu.make_async_copy(gated_hbm.at[here], gatedb.at[slot], bsem.at[slot, 3]),
            pltpu.make_async_copy(dbr_hbm.at[pl.ds(2 * i, 2)], dbr_ref.at[slot], bsem.at[slot, 4]),
        ]

    for copy in block_in(steps - 1):
        copy.start()
    for copy in loads:
        copy.wait()
    head = at.s // rep
    dstate[...] = jnp.zeros_like(dstate)
    dbuf[GB : GB + 8] = jnp.zeros((8, 640), F32)
    small[...] = jnp.zeros_like(small)
    gw[...] = jnp.zeros_like(gw)
    go[...] = jnp.zeros_like(go)
    taps = head_taps(taps_ref, head, heads)
    hg = hg_ref[...].astype(F32)
    rows = SeqSum(at, part, got, out, far, (ps, pr, qs, qr))
    enter(at)
    for ds in range(1, ns):
        pl.semaphore_signal(ready, inc=1, device_id={"seq": at.seq_at(ds)}, device_id_type=MESH)

    def step(j, _):
        i = steps - 1 - j
        first = i * GB
        slot = lax.rem(i, 2)

        @pl.when(i > 0)
        def _():
            for copy in block_in(i - 1):
                copy.start()

        def kept_map(kind, s, high=128):
            row = SPAN_ROWS * s + 128 * kind
            return save[slot, row : row + high]

        def kept_rows(kind):
            row = SPAN_ROWS * GS + GB * kind
            return save[slot, row : row + GB]

        for copy in block_in(i):
            copy.wait()
        dbr = dbr_ref[slot].reshape(GB, -1)
        d_gated = mm(dbr, w_ref[:, 896:1024])
        gl, sm, o = kept_rows(0), kept_rows(1), kept_rows(2)
        sg = jax.nn.sigmoid(gl)
        rr = norm_rows(o)
        yn = o * rr
        dn = d_gated * (gl * sg)
        d_gl = d_gated * (yn * hg) * (sg * (1.0 + gl * (1.0 - sg)))
        dy = dn * hg
        d_raw = rr * (dy - yn * jnp.mean(yn * dy, axis=-1, keepdims=True))
        go[...] += mm(gatedb[slot], dbr, TN)

        mix = conv_mix(buf.at[slot], taps)
        sig = jax.nn.sigmoid(mix)
        act = mix * sig
        qn, rq = unit(act[:, 0:128])
        k0, r0 = unit(act[:, 128:256])
        k1, r1 = unit(act[:, 256:384])
        v0, v1 = act[:, 384:512], act[:, 512:640]
        q = qn * DK ** (-0.5)
        keep = (first + iota((GB, 1), 0) < len_ref[0]).astype(F32)
        sig0, sig1, al = gates(sm, dbias_ref[head])
        eg = jnp.exp(jnp.full((1, 1), dlog_ref[head], F32))
        g1 = -eg * softplus(al) * keep
        g = lane(g1)
        b0, b1 = lane(sig0 * keep), lane(sig1 * keep)
        strict, _, _ = sub_masks()
        tri = (iota((64, 64), 0) >= iota((64, 64), 1)).astype(F32)
        trit = (iota((64, 64), 0) <= iota((64, 64), 1)).astype(F32)
        causal = iota((64, 128), 0) >= (iota((64, 128), 1) & 63)
        K, Q, V, B, C, E, Kc, A1, A2, DO = [], [], [], [], [], [], [], [], [], []
        for s in range(GS):
            sl = slice(64 * s, 64 * s + 64)
            K.append(jnp.concatenate([k0[sl], k1[sl]], axis=0))
            V.append(jnp.concatenate([v0[sl], v1[sl]], axis=0))
            B.append(jnp.concatenate([b0[sl], b1[sl]], axis=0))
            Q.append(q[sl])
            c, e = span_decay(g[sl], tri)
            C.append(c)
            E.append(e)
            cc = jnp.concatenate([c, c], axis=0)
            Kc.append(jnp.exp(cc[63:64] - cc) * K[s])
            do = d_raw[sl]
            DO.append(do)
            A1.append(mm3(kept_map(5, s, HALF), do, TN))
            A2.append(mm3(jnp.exp(c) * Q[s], do, TN))
        dS = dstate[...]
        DV, DS = [None] * GS, [None] * GS
        for s in reversed(range(GS)):
            DS[s] = dS
            dvn = A1[s] + mm3(Kc[s], dS)
            DV[s] = dvn
            dS = jnp.exp(C[s][63:64]) * dS + A2[s] - mm3(kept_map(1, s), dvn, TN)
        dstate[...] = dS
        pl.when(j > 0)(lambda: rows.flush(i + 1))
        dq_l, dk0_l, dk1_l, dv0_l, dv1_l, db0_l, db1_l, dg_l = [], [], [], [], [], [], [], []
        for s in range(GS):
            vn, sst, n, p = kept_map(2, s), kept_map(4, s), kept_map(3, s), kept_map(5, s, HALF)
            vns = split(vn)
            ks = split(K[s])
            cc = jnp.concatenate([C[s], C[s]], axis=0)
            ec = jnp.exp(cc)
            ee = jnp.concatenate([E[s], E[s]], axis=0)
            dr = mm3(kept_map(0, s), DV[s], TN)
            both = split(jnp.concatenate([dr, DO[s]], axis=0))
            dd = mm3(both, vns, NT)
            dN = jnp.where(strict, -dd[:128], 0.0)
            dP = jnp.where(causal, dd[128:], 0.0)
            h = mm3(both, sst, NT)
            hk, hq = h[:128], h[128:]
            fh = dP * E[s]
            dq = ec[:64] * hq + mm3(fh, ks)
            dne = dN * ee
            dgm = dne * B[s]
            dkc = mm3(vns, DS[s], NT)
            ekc = jnp.exp(cc[63:64] - cc)
            dk = ekc * dkc - B[s] * ec * hk + mm3(fh, Q[s], TN) + mm3(dgm + jnp.transpose(dgm), ks)
            khk = jnp.sum(K[s] * hk, axis=-1, keepdims=True)
            ecl = ec[:, 0:1]
            db = (
                jnp.sum(dr * V[s], axis=-1, keepdims=True)
                - ecl * khk
                + jnp.sum(dne * mm3(ks, ks, NT), axis=-1, keepdims=True)
            )
            e1 = dN * n
            f1 = dP * p
            z = e1[:64, :64] + e1[:64, 64:] + e1[64:, :64] + e1[64:, 64:] + f1[:, :64] + f1[:, 64:]
            dc = jnp.sum(z - jnp.transpose(z), axis=-1, keepdims=True)
            dks = -B[s][:, 0:1] * ecl * khk
            hj = jnp.sum(Kc[s] * dkc, axis=-1, keepdims=True)
            dc = dc + dks[:64] + dks[64:] - hj[:64] - hj[64:]
            dc = dc + ec[:64, 0:1] * jnp.sum(Q[s] * hq, axis=-1, keepdims=True)
            dcl = jnp.sum(hj, axis=0, keepdims=True) + ec[63:64, 0:1] * jnp.sum(
                jnp.sum(sst * DS[s], axis=-1, keepdims=True), axis=0, keepdims=True
            )
            dg = mm3(trit, lane(dc)) + dcl
            dg_l.append(dg[:, 0:1])
            dq_l.append(dq)
            dk0_l.append(dk[:64])
            dk1_l.append(dk[64:])
            dv = B[s] * dr
            dv0_l.append(dv[:64])
            dv1_l.append(dv[64:])
            db0_l.append(db[:64])
            db1_l.append(db[64:])
        cat = lambda parts: jnp.concatenate(parts, axis=0)
        dq, dk0, dk1, dv0, dv1 = cat(dq_l), cat(dk0_l), cat(dk1_l), cat(dv0_l), cat(dv1_l)
        db0, db1, dg = cat(db0_l), cat(db1_l), cat(dg_l)

        def unit_back(d, n, rn):
            return rn * (d - n * jnp.sum(d * n, axis=-1, keepdims=True))

        d_act = jnp.concatenate(
            [unit_back(dq * DK ** (-0.5), qn, rq), unit_back(dk0, k0, r0), unit_back(dk1, k1, r1), dv0, dv1],
            axis=1,
        )
        d_mix = d_act * (sig * (1.0 + mix * (1.0 - sig)))
        for t in range(4):
            small[t : t + 1, 0:640] += jnp.sum(d_mix * buf[slot, 5 + t : 5 + t + GB], axis=0, keepdims=True)
        dbuf[0:GB] = d_mix
        d_pre = taps[3:4] * d_mix
        for t in range(3):
            d_pre = d_pre + taps[t : t + 1] * dbuf[3 - t : 3 - t + GB]
        dbuf[GB : GB + 8] = d_mix[0:8]
        d_al = -dg * eg * jax.nn.sigmoid(al) * keep
        d_b0 = db0 * keep * sig0 * (1.0 - sig0)
        d_b1 = db1 * keep * sig1 * (1.0 - sig1)
        lanes = iota((GB, 128), 1)
        d_sm = jnp.where(
            lanes == 0, d_b0, jnp.where(lanes == 1, d_b1, jnp.where(lanes == 2, d_al, 0.0))
        )
        small[0:1, 640:768] += jnp.sum(dn * yn, axis=0, keepdims=True)
        small[1:2, 640:768] += jnp.broadcast_to(jnp.sum(dg * g1, axis=0, keepdims=True), (1, 128))
        small[2:3, 640:768] += jnp.broadcast_to(jnp.sum(d_al, axis=0, keepdims=True), (1, 128))
        dall = jnp.concatenate([d_pre.astype(BF16), d_gl.astype(BF16), d_sm.astype(BF16)], axis=1)
        gw[...] += mm(normedb[slot], dall, TN)
        if rep > 1:
            dall = jnp.where(lax.rem(at.s, rep) == 0, dall, jnp.zeros_like(dall))
        part[i] = mm(dall, w_ref[:, 0:896], NT).astype(BF16).reshape(2, GB // 2, -1)
        rows.start(i)
        return 0

    lax.fori_loop(0, steps, step, 0)

    small[4:8] = jnp.transpose(gw[:, 768:896])[0:4]
    smalls = [send(small, got_s.at[m], ss.at[m], sr.at[m], {"batch": at.peer(m)}) for m in at.peers()]
    for copy in smalls:
        copy.start()
    nk, nq = ns // nb, slots.shape[0] // 6
    wrows = grads.shape[1]
    grads[...] = gw[:, 0:768].astype(BF16).reshape(ns, wrows, 768)
    over = []
    for k in range(nk):
        for m in at.peers():
            to = at.peer(m)
            n = k * nb + m
            over.append(send(grads.at[to + nb * k], got_g.at[n], gs.at[n], gr.at[n], {"batch": to}))
    for copy in over:
        copy.start()
    rows.flush(0)
    high, wide = gout.shape[1:]
    for b in range(nb):
        block = go[:, wide * b : wide * (b + 1)].astype(BF16)
        if rep > 1:
            block = jnp.where(lax.rem(at.s, rep) == 0, block[:high], block[high:])
        gout[b] = block
    outs = [send(gout.at[at.peer(m)], got_o.at[m], os_.at[m], or_.at[m], {"batch": at.peer(m)}) for m in at.peers()]
    for copy in outs:
        copy.start()
    total = small[...]
    for m, copy in zip(at.peers(), smalls):
        copy.wait_recv()
        total = total + got_s[m]
    small_all[at.s] = total
    heads_ = [
        send(small_all.at[at.s], small_all.at[at.s], us.at[ds], ur.at[ds], {"seq": at.seq_at(ds)})
        for ds in range(1, ns)
    ]
    for copy in heads_:
        copy.start()
    for copy in over:
        copy.wait_recv()
    pl.semaphore_wait(ready, ns - 1)
    width = slots.shape[2]
    placed = []
    for k in range(nk):
        row = at.b + nb * k
        acc = grads[row].astype(F32)
        for m in at.peers():
            acc = acc + got_g[k * nb + m].astype(F32)
        for m in range(6):
            block = acc[:, 128 * m : 128 * m + 128]
            if rep > 1:
                block = jnp.where(lax.rem(at.s, rep) == 0, block[:, :width], block[:, width:])
            piece[k * 6 + m] = block.astype(BF16)
            if m in (0, 5):
                owner, slot = at.s // nq, (0 if m == 0 else 5 * nq) + lax.rem(at.s, nq)
            else:
                unit_at = ((m - 1) % 2) * ns + at.s
                owner, slot = unit_at // (2 * nq), (nq if m < 3 else 3 * nq) + lax.rem(unit_at, 2 * nq)
            placed.append((row, owner, slot, k * 6 + m))

    def place(item):
        row, owner, slot, n = item
        src = piece.at[n]
        here = jnp.logical_and(row == at.s, owner == at.b)
        far_copy = lambda: send(src, slots.at[slot], bs.at[n], br.at[slot], {"seq": row, "batch": owner})
        near_copy = lambda: pltpu.make_async_copy(src, slots.at[slot], br.at[slot])
        return here, far_copy, near_copy

    for item in placed:
        here, far_copy, near_copy = place(item)
        pl.when(here)(lambda: near_copy().start())
        pl.when(jnp.logical_not(here))(lambda: far_copy().start())

    d_normed = rows.finish()
    x = hid[...].astype(F32)
    r = norm_rows(x)
    y = x * r
    vec[0:1] = jnp.sum(d_normed * y, axis=0, keepdims=True)
    vec[1:2] = gfeed[...]
    pairs = [send(vec, got_v.at[m], vs_.at[m], vr.at[m], {"batch": at.peer(m)}) for m in at.peers()]
    for copy in pairs:
        copy.start()
    dy = d_normed * gains[3:4]
    grad_in[...] = (d_stream[...] + r * (dy - y * jnp.mean(dy * y, axis=-1, keepdims=True))).astype(BF16)
    acc = gout[at.b].astype(F32)
    for m, copy in zip(at.peers(), outs):
        copy.wait_recv()
        acc = acc + got_o[m].astype(F32)
    gout_sum[...] = acc
    row_sum = vec[...]
    for m, copy in zip(at.peers(), pairs):
        copy.wait_recv()
        row_sum = row_sum + got_v[m]
    got_w[0] = row_sum
    spread = [send(got_w.at[0], got_w.at[ds], xs.at[ds], xr.at[ds], {"seq": at.seq_at(ds)}) for ds in range(1, ns)]
    for copy in spread:
        copy.start()
    for copy in spread + heads_:
        copy.wait_recv()
    row_sum = got_w[0]
    for ds in range(1, ns):
        row_sum = row_sum + got_w[ds]
    vec_sum[...] = row_sum
    for item in placed:
        here, far_copy, _ = place(item)
        pl.when(jnp.logical_not(here))(lambda: far_copy().wait_send())
    for slot in range(slots.shape[0]):
        pltpu.make_async_copy(piece.at[0], slots.at[slot], br.at[slot]).wait()
    for copy in smalls + over + outs + heads_ + pairs + spread:
        copy.wait_send()
    rows.drain()


def comm_call(kernel, outs, scratch, ident, name, args, specs, limit):
    return pl.pallas_call(
        kernel,
        in_specs=specs,
        out_specs=[o[1] for o in outs],
        out_shape=[o[0] for o in outs],
        scratch_shapes=scratch,
        compiler_params=pltpu.CompilerParams(
            collective_id=ident, has_side_effects=True, vmem_limit_bytes=limit * 1024 * 1024
        ),
        name=name,
    )(*args)


def dma(*shape):
    return pltpu.SemaphoreType.DMA(shape)


def on_device(
    hidden_in, cotangent, lengths, mixer_gain, query_weight, key_weight, value_weight, beta_weight, alpha_weight,
    gate_weight, out_weight, feed_gain, feed_gate, feed_up, feed_down, conv_taps, decay_log, decay_bias, head_gain,
):
    ns, nb = lax.axis_size("seq"), lax.axis_size("batch")
    heads = decay_log.shape[0]
    rep = ns // heads
    tok, width = hidden_in.shape[1:]
    assert hidden_in.shape[0] == 1 and ns == rep * heads and ns % nb == 0 and 2 * tok == GB
    rows = query_weight.shape[0]
    share = feed_gate.shape[1] // nb
    halves = ns // nb
    nz = ns // 2
    n = ns * tok
    sds = jax.ShapeDtypeStruct
    vmem, hbm = pl.BlockSpec(memory_space=pltpu.VMEM), pl.BlockSpec(memory_space=pltpu.HBM)
    smem = pl.BlockSpec(memory_space=pltpu.SMEM)
    hidden, cot = hidden_in[0], cotangent[0]
    buffer = lambda *shape: pltpu.VMEM(shape, BF16)
    block = lambda count: buffer(count, tok, width)
    wide = lambda *shape: pltpu.VMEM(shape, F32)
    vout = lambda kind, *shape: (sds(shape, kind), vmem)
    hout = lambda kind, *shape: (sds(shape, kind), hbm)
    key = heads * DK

    hid_all, wm, ff = comm_call(
        functools.partial(gather_kernel, ns, nb, rep, heads),
        [hout(BF16, ns, tok, width), hout(BF16, ns, nb, rows, 8 * DK), hout(BF16, 3, nb, rows, share)],
        [
            buffer(tok, width), buffer(rows, key), buffer(rows, 2 * key), buffer(rows, 2 * key), buffer(rows, key),
            buffer(rows, key), buffer(rows, nb * share), buffer(rows, nb * share), buffer(rows, nb * share),
            buffer(heads, rows, 8 * DK), buffer(nb, 3, rows, share), dma(9), dma(3), dma(4 * nz), dma(4 * nz), dma(ns),
            dma(ns), dma(nz, nb), dma(nz, nb), dma(nb), dma(nb),
        ],
        0, "gather",
        (
            hidden, query_weight, key_weight, value_weight, gate_weight, out_weight.T, beta_weight, alpha_weight,
            mixer_gain[None], feed_gain[None], feed_gate, feed_up, feed_down.T,
        ),
        [hbm] * 6 + [vmem] * 4 + [hbm] * 3, 62,
    )
    wm = wm.reshape(width, 8 * DK)
    ff = lax.all_gather(ff.reshape(3, nb * rows, share), "seq", axis=1, tiled=True)
    hg = head_gain[None]
    normed, pre, gated, save, gains, after, nm_all, cot_all = comm_call(
        functools.partial(front_kernel, ns, nb, rep, heads),
        [
            hout(BF16, n, width), hout(F32, n + 8, 5 * DK), hout(BF16, n, DK), hout(F32, nz, SAVE_ROWS, DK),
            vout(F32, 8, width), vout(F32, tok, width), hout(BF16, nb, tok, width), hout(BF16, nb, tok, width),
        ],
        [
            block(ns), buffer(width, 8 * DK), buffer(4, 5 * key), buffer(tok, width), buffer(tok, width),
            wide(8, 5 * DK), wide(2, SAVE_ROWS, DK), wide(2, GB, 5 * DK), buffer(2, GB, width), buffer(2, GB, DK),
            wide(8 + GB, 5 * DK), wide(DK, DK), buffer(nz, 2, tok, width), block(nz), block(nz), block(nz),
            dma(3), dma(nz), dma(3), dma(2, 4), dma(nz), dma(nz), dma(nz), dma(nz), dma(nb), dma(nb), dma(nb), dma(nb),
        ],
        1, "front",
        (lengths, decay_log, decay_bias, hid_all, wm, conv_taps, hg, cot),
        [smem] * 3 + [hbm] * 3 + [vmem, hbm], 61,
    )
    block_out, d_stream, dbr_all, gfeed, sums = comm_call(
        functools.partial(feed_kernel, ns, nb),
        [
            vout(BF16, tok, width), vout(F32, tok, width), hout(BF16, ns, tok, width), vout(F32, 1, width),
            hout(BF16, ns, 3 * share, width // ns),
        ],
        [
            block(nb), block(nb), buffer(3, width, share), buffer(nb, tok, share), buffer(nb, tok, share),
            buffer(nb, tok, share), block(nb), block(nb), block(nb), block(nb), buffer(tok, width),
            buffer(2, ns, share, width // ns), buffer(nb, halves, share, width // ns),
            dma(3), dma(3 + halves), dma(nb), dma(nb), dma(nb), dma(nb), dma(4 * nz), dma(4 * nz), dma(nb, halves),
            dma(nb, halves),
        ],
        2, "feed", (nm_all, cot_all, ff, after, gains), [hbm] * 3 + [vmem] * 2, 61,
    )
    sums = lax.psum_scatter(sums, "seq", scatter_dimension=0, tiled=False)
    g_down = jnp.swapaxes(sums[2 * share :].reshape(halves, share // halves, width // ns), 0, 1)
    g_down = g_down.reshape(share // halves, width // nb).astype(F32)

    nq = ns // nb
    nk = ns // nb
    cw = DK // rep
    wrows = width // ns
    grad_in, slots, gout_sum, small_all, vec_sum = comm_call(
        functools.partial(back_kernel, ns, nb, rep, heads),
        [
            vout(BF16, tok, width), vout(BF16, 6 * nq, wrows, cw), vout(F32, DK // rep, width // nb),
            vout(F32, ns, 8, width), vout(F32, 2, width),
        ],
        [
            buffer(2, 2, tok, width), buffer(width, 8 * DK), buffer(4, 5 * key), buffer(tok, width),
            wide(2, SAVE_ROWS, DK), wide(2, 8 + GB, 5 * DK), buffer(2, GB, width), buffer(2, GB, DK), dma(3), dma(2, 5),
            wide(GB + 8, 5 * DK), wide(DK, DK), wide(8, width), wide(width, 7 * DK),
            wide(DK, width), buffer(nz, 2, tok, width), block(nz), block(nz), block(nz),
            buffer(ns, wrows, 6 * DK), buffer(nb, DK // rep, width // nb), buffer(nk * nb, wrows, 6 * DK),
            buffer(nk * 6, wrows, cw), buffer(nb, DK // rep, width // nb), wide(nb, 8, width), wide(nb, 2, width),
            wide(2, width), wide(ns, 2, width), pltpu.SemaphoreType.REGULAR,
            dma(nz), dma(nz), dma(nz), dma(nz), dma(nk * nb), dma(nk * nb), dma(nk * 6), dma(6 * nq),
            dma(nb), dma(nb), dma(nb), dma(nb), dma(ns), dma(ns), dma(nb), dma(nb), dma(ns), dma(ns),
        ],
        3, "back",
        (
            lengths, decay_log, decay_bias, dbr_all, wm, conv_taps, hg, normed, pre, gated, save, hidden, gains,
            d_stream, gfeed,
        ),
        [smem] * 3 + [hbm] * 3 + [vmem] + [hbm] * 5 + [vmem] * 3, 61,
    )

    def owned(first, count):
        return jnp.swapaxes(slots[first : first + count], 0, 1).reshape(wrows, count * cw).astype(F32)

    small_all = small_all[::rep]
    return (
        block_out[None],
        grad_in[None],
        vec_sum[0],
        owned(0, nq),
        owned(nq, 2 * nq),
        owned(3 * nq, 2 * nq),
        jnp.transpose(small_all[:, 4:6], (2, 1, 0)).reshape(width, 2 * heads),
        small_all[:, 6].T,
        owned(5 * nq, nq),
        gout_sum,
        vec_sum[1],
        sums[:share].T.astype(F32),
        sums[share : 2 * share].T.astype(F32),
        g_down,
        jnp.transpose(small_all[:, :4, : 5 * DK].reshape(heads, 4, 5, DK), (1, 2, 0, 3)).reshape(4, -1),
        small_all[:, 1, 5 * DK],
        small_all[:, 2, 5 * DK],
        jnp.sum(small_all[:, 0, 5 * DK : 6 * DK], axis=0),
    )


def solution(mesh):
    both = ("seq", "batch")
    tokens, split_rows, grid = P("batch", "seq", None), P(both, None), P("seq", "batch")
    return jax.shard_map(
        on_device,
        mesh=mesh,
        in_specs=(
            tokens, tokens, P("batch"), P(both), split_rows, split_rows, split_rows, split_rows, split_rows,
            split_rows, P(None, both), P(both), split_rows, split_rows, P(None, both), P(), P(), P(), P(),
        ),
        out_specs=(
            tokens, tokens, P(), grid, grid, grid, P(), P(), grid, grid, P(), grid, grid, grid, P(), P(), P(), P(),
        ),
        check_vma=False,
    )
```

```python
import functools
import jax
import jax.numpy as jnp
from jax import lax
from jax.experimental import pallas as pl
from jax.experimental.pallas import tpu as pltpu
from jax.sharding import PartitionSpec as P

F32, BF16 = jnp.float32, jnp.bfloat16
EPS = 1e-05
DK = 128
HALF = 64
GS = 4
GB = GS * HALF
NN = (((1,), (0,)), ((), ()))
NT = (((1,), (1,)), ((), ()))
TN = (((0,), (0,)), ((), ()))


def mm(a, b, dims=NN):
    return lax.dot_general(a.astype(BF16), b.astype(BF16), dims, preferred_element_type=F32)


def split(a):
    hi = a.astype(BF16)
    return hi, (a - hi.astype(F32)).astype(BF16)


def mm3(a, b, dims=NN):
    (ah, al), (bh, bl) = (x if isinstance(x, tuple) else split(x) for x in (a, b))
    return (
        lax.dot_general(ah, bl, dims, preferred_element_type=F32)
        + lax.dot_general(al, bh, dims, preferred_element_type=F32)
    ) + lax.dot_general(ah, bh, dims, preferred_element_type=F32)


def iota(shape, axis):
    return lax.broadcasted_iota(jnp.int32, shape, axis)


def sub_masks():
    rows, cols = iota((128, 128), 0), iota((128, 128), 1)
    tr, tc = 2 * (rows & 63) + (rows >> 6), 2 * (cols & 63) + (cols >> 6)
    strict = tr > tc
    levels = []
    for bits in range(3, 7):
        same_up = (tr >> (bits + 1)) == (tc >> (bits + 1))
        levels.append(strict & same_up & ((tr >> bits) != (tc >> bits)))
    base = strict & ((tr >> 3) == (tc >> 3))
    return strict, base, levels


def unit(a):
    r = lax.rsqrt(jnp.sum(a * a, axis=-1, keepdims=True) + EPS)
    return a * r, r


def softplus(x):
    return jnp.maximum(x, 0.0) + jnp.log1p(jnp.exp(-jnp.abs(x)))


def lane(x, width=128):
    return jnp.broadcast_to(x, (x.shape[0], width))


def gates(sm, dec_bias):
    return jax.nn.sigmoid(sm[:, 0:1]), jax.nn.sigmoid(sm[:, 1:2]), sm[:, 2:3] + dec_bias


def span_decay(gb, tri):
    c = mm3(tri, gb)
    ct = jnp.transpose(jnp.concatenate([c, c], axis=0))[:64]
    e = jnp.exp(jnp.minimum(c - ct, 0.0))
    return c, e


def conv_mix(buf, taps):
    mix = taps[0:1] * buf[5 : 5 + GB]
    for j in range(1, 4):
        mix = mix + taps[j : j + 1] * buf[5 + j : 5 + j + GB]
    return mix


def head_taps(taps_ref, head, heads):
    parts = []
    for col in (head, heads + head, 2 * heads + head, 3 * heads + head, 4 * heads + head):
        parts.append(taps_ref[:, pl.ds(pl.multiple_of(col * 128, 128), 128)].astype(F32))
    return jnp.concatenate(parts, axis=1)


MESH = pl.DeviceIdType.MESH
SPAN_ROWS = 5 * 128 + HALF
SAVE_ROWS = GS * SPAN_ROWS + 3 * GB


class Place:
    def __init__(self, ns, nb):
        self.ns, self.nb, self.nz = ns, nb, ns // 2
        self.s, self.b = lax.axis_index("seq"), lax.axis_index("batch")
        self.z, self.c = self.s // 2, lax.rem(self.s, 2)
        self.sib = self.s + 1 - 2 * self.c

    def seq_at(self, ds):
        return lax.rem(self.s + ds, self.ns)

    def seq_before(self, ds):
        return lax.rem(self.s + self.ns - ds, self.ns)

    def peer(self, mask):
        out, bit = 0, 1
        while bit < self.nb:
            mine, other = lax.rem(self.b // bit, 2), lax.rem(mask // bit, 2) if not isinstance(mask, int) else mask // bit % 2
            out = out + bit * (mine + other - 2 * mine * other)
            bit *= 2
        return out

    def peers(self):
        return range(self.nb - 1, 0, -1)


def greet(at):
    barrier = pltpu.get_barrier_semaphore()
    for ds in range(1, at.ns):
        pl.semaphore_signal(barrier, inc=1, device_id={"seq": at.seq_at(ds)}, device_id_type=MESH)
    for m in at.peers():
        pl.semaphore_signal(barrier, inc=1, device_id={"batch": at.peer(m)}, device_id_type=MESH)


def enter(at):
    pl.semaphore_wait(pltpu.get_barrier_semaphore(), at.ns + at.nb - 2)


def send(src, dst, send_sem, recv_sem, where):
    return pltpu.make_async_remote_copy(
        src_ref=src, dst_ref=dst, send_sem=send_sem, recv_sem=recv_sem, device_id=where, device_id_type=MESH
    )


def fetch(pairs, sem):
    copies = [pltpu.make_async_copy(src, dst, sem.at[k]) for k, (src, dst) in enumerate(pairs)]
    for copy in copies:
        copy.start()
    return copies


class BatchGather:
    def __init__(self, at, src, out_at, ssem, rsem):
        self.copies = [
            send(src, out_at, ssem.at[m], rsem.at[m], {"batch": at.peer(m)}) for m in at.peers()
        ]

    def start(self):
        for copy in self.copies:
            copy.start()

    def finish(self):
        for copy in self.copies:
            copy.wait_recv()
        for copy in self.copies:
            copy.wait_send()


class SeqGather:
    def __init__(self, at, src, out, ssem, rsem):
        self.at, self.src, self.out, self.ssem, self.rsem = at, src, out, ssem, rsem

    def hop(self, t, up):
        at = self.at
        origin = at.z - (t - 1) if up else at.z + (t - 1)
        slot = 2 * origin + at.c
        src = self.src if t == 1 else self.out.at[slot]
        to = at.s + 2 if up else at.s - 2
        k = t if up else at.nz + t
        return send(src, self.out.at[slot], self.ssem.at[k], self.rsem.at[k], {"seq": to})

    def can_send(self, t, up):
        at = self.at
        if up:
            return jnp.logical_and(at.z - (t - 1) >= 0, at.z + 1 < at.nz)
        return jnp.logical_and(at.z + (t - 1) < at.nz, at.z >= 1)

    def can_recv(self, t, up):
        return self.at.z - t >= 0 if up else self.at.z + t < self.at.nz

    def across(self, t, up):
        at, nz = self.at, self.at.nz
        k = 2 * nz + (t if up else nz + t)
        origin = 0 if t == 0 else (-t if up else t)
        slot = 2 * (at.z + origin) + at.c
        src = self.src if t == 0 else self.out.at[slot]
        return send(src, self.out.at[slot], self.ssem.at[k], self.rsem.at[k], {"seq": at.sib})

    def start(self):
        for up in (True, False):
            pl.when(self.can_send(1, up))(lambda: self.hop(1, up).start())
        self.across(0, True).start()

    def forward(self, t):
        for up in (True, False):

            @pl.when(self.can_recv(t, up))
            def _():
                self.hop(t, up).wait_recv()
                if t + 1 < self.at.nz:
                    pl.when(self.can_send(t + 1, up))(lambda: self.hop(t + 1, up).start())
                self.across(t, up).start()

    def finish(self):
        self.across(0, True).wait()
        for t in range(1, self.at.nz):
            for up in (True, False):
                pl.when(self.can_recv(t, up))(lambda: self.across(t, up).wait())
                pl.when(self.can_send(t, up))(lambda: self.hop(t, up).wait_send())


class SeqSum:
    def __init__(self, at, part, got, out, far, sems):
        self.at, self.part, self.got, self.out, self.far = at, part, got, out, far
        self.pair_s, self.pair_r, self.hop_s, self.hop_r = sems

    def pair(self, i):
        at = self.at
        return send(self.part.at[i, 1 - at.c], self.got.at[i], self.pair_s.at[i], self.pair_r.at[i], {"seq": at.sib})

    def hop(self, i):
        at = self.at
        dz = lax.rem(i - at.z + at.nz, at.nz)
        return send(self.out.at[i], self.far.at[dz], self.hop_s.at[i], self.hop_r.at[dz], {"seq": 2 * i + at.c})

    def start(self, i):
        self.pair(i).start()

    def flush(self, i):
        self.pair(i).wait_recv()

        @pl.when(i != self.at.z)
        def _():
            mine = self.part[i, self.at.c].astype(F32)
            self.out[i] = (mine + self.got[i].astype(F32)).astype(BF16)
            self.hop(i).start()

    def finish(self):
        at = self.at
        total = self.part[at.z, at.c].astype(F32) + self.got[at.z].astype(F32)
        for dz in range(1, at.nz):
            send(self.out.at[0], self.far.at[dz], self.hop_s.at[0], self.hop_r.at[dz], {"seq": at.sib}).wait_recv()
            total = total + self.far[dz].astype(F32)
        return total

    def drain(self):
        for i in range(self.at.nz):
            self.pair(i).wait_send()
            pl.when(i != self.at.z)(lambda: self.hop(i).wait_send())


def norm_rows(x):
    return lax.rsqrt(jnp.mean(x * x, axis=-1, keepdims=True) + EPS)


def gather_kernel(
    ns, nb, rep, heads,
    hid, wq, wk, wv, wg, wo, beta, alpha, gain_in, gain_mid, fg, fu, fd,
    hid_out, wm_out, ff_out,
    hv, qv, kv, vv, gv, ov, fgv, fuv, fdv, wbuf, fbuf, isem, lsem, hs, hr, ws, wr, os_, or_, fs, fr,
):
    at = Place(ns, nb)
    greet(at)
    loads = fetch(
        [(hid, hv), (wq, qv), (wk, kv), (wv, vv), (wg, gv), (wo, ov), (fg, fgv), (fu, fuv), (fd, fdv)], isem
    )
    rows = beta.shape[1]
    lanes = iota((rows, 128), 1)
    eye = iota((rows, rows), 0) == iota((rows, rows), 1)
    column = lambda ref, k=0: jnp.sum(jnp.where(eye, ref[k : k + 1].astype(F32), 0.0), axis=1, keepdims=True)
    tail = jnp.where(lanes == 3, column(gain_in), jnp.where(lanes == 4, column(gain_mid), 0.0))
    share = fbuf.shape[3]
    for copy in loads[1:6]:
        copy.wait()
    for h in range(heads):
        col = lambda j: slice(128 * (j * heads + h), 128 * (j * heads + h) + 128)
        small = jnp.where(lanes == 0, column(beta, h), tail)
        small = jnp.where(lanes == 1, column(beta, heads + h), small)
        small = jnp.where(lanes == 2, column(alpha, h), small)
        parts = (
            qv[:, col(0)], kv[:, col(0)], kv[:, col(1)], vv[:, col(0)], vv[:, col(1)], gv[:, col(0)],
            small.astype(BF16), ov[:, col(0)],
        )
        for j, p in enumerate(parts):
            wbuf[h, :, 128 * j : 128 * j + 128] = p
    loads[0].wait()
    enter(at)

    def piece(to, where):
        return send(wbuf.at[to // rep], wm_out.at[at.s, at.b], ws.at[to], wr.at[at.s], where)

    def arrives(origin):
        send(wbuf.at[0], wm_out.at[origin, at.b], ws.at[0], wr.at[origin], {"seq": at.sib}).wait_recv()

    square = nb == 4

    def hop(block, sem, m):
        return lambda: send(block, block, os_.at[sem], or_.at[sem], {"batch": at.peer(m)})

    def plane(zo):
        block = wm_out.at[pl.ds(2 * zo, 2), at.b]
        half = lambda core, m: wm_out.at[2 * zo + core, at.peer(m)]
        if not square:
            return [hop(block, (zo, m), m) for m in at.peers()], []
        first = [hop(block, (zo, m), m) for m in (1, 2)]
        return first, [hop(half(0, 1), (zo, 3), 2), hop(half(1, 2), (zo, 0), 1)]

    def pass_on(zo):
        for copy in plane(zo)[0]:
            copy().start()

    def follow(zo):
        first, then = plane(zo)
        for copy, onward in zip(first, then):
            copy().wait_recv()
            onward().start()

    def around(fn):
        for t in range(1, at.nz):
            pl.when(at.z + t < at.nz)(lambda: fn(at.z + t))
            pl.when(at.z - t >= 0)(lambda: fn(at.z - t))

    def scatter(zo):
        for core in range(2):
            piece(2 * zo + core, {"seq": 2 * zo + core}).start()

    own = pltpu.make_async_copy(wbuf.at[at.s // rep], wm_out.at[at.s, at.b], lsem.at[0])
    own.start()
    piece(at.sib, {"seq": at.sib}).start()
    around(scatter)
    line = SeqGather(at, hv, hid_out, hs, hr)
    line.start()
    place = pltpu.make_async_copy(hv, hid_out.at[at.s], lsem.at[1])
    place.start()
    arrives(at.sib)
    own.wait()
    pass_on(at.z)
    for copy in loads[6:]:
        copy.wait()
    for b in range(nb):
        for j, w in enumerate((fgv, fuv, fdv)):
            fbuf[b, j] = w[:, share * b : share * (b + 1)]
    kept = pltpu.make_async_copy(fbuf.at[at.b], ff_out.at[:, at.b], lsem.at[2])
    kept.start()
    cols = [
        send(fbuf.at[at.peer(m)], ff_out.at[:, at.b], fs.at[m], fr.at[m], {"batch": at.peer(m)}) for m in at.peers()
    ]

    def relay(zo):
        for core in range(2):
            arrives(2 * zo + core)
        pass_on(zo)

    def at_distance(t, fn):
        if t == 0:
            fn(at.z)
        else:
            pl.when(at.z + t < at.nz)(lambda: fn(at.z + t))
            pl.when(at.z - t >= 0)(lambda: fn(at.z - t))

    for t in range(1, at.nz):
        at_distance(t, relay)
        line.forward(t)
        at_distance(t - 1, follow)
        if t == 1:
            for copy in cols:
                copy.start()
    at_distance(at.nz - 1, follow)
    line.finish()

    def settle(zo):
        first, then = plane(zo)
        for copy in then if square else first:
            copy().wait_recv()
        for copy in first + then:
            copy().wait_send()

    for zo in range(at.nz):
        settle(zo)
    piece(at.sib, {"seq": at.sib}).wait_send()

    def sent(zo):
        for core in range(2):
            piece(2 * zo + core, {"seq": 2 * zo + core}).wait_send()

    around(sent)
    for copy in cols:
        copy.wait()
    place.wait()
    kept.wait()


def front_kernel(
    ns, nb, rep, heads,
    len_ref, dlog_ref, dbias_ref, hid_hbm, w_hbm, taps_hbm, hg_ref, cot_hbm, feed_hbm,
    normed_hbm, pre_hbm, gated_hbm, save_hbm, gains, after, nm_out, cot_out, feed_out,
    hid_ref, w_ref, taps_ref, cot, nm, zero, save, preb, normedb, gatedb,
    buf, state, part, got, out, far, isem, bsem, lsem, osem, ps, pr, qs, qr, ms, mr, cs, cr, fs, fr,
):
    at = Place(ns, nb)
    greet(at)
    steps = at.nz
    loads = fetch([(w_hbm, w_ref), (taps_hbm, taps_ref), (cot_hbm, cot)], isem)

    def block_in(i):
        return pltpu.make_async_copy(hid_hbm.at[pl.ds(2 * i, 2)], hid_ref.at[pl.ds(2 * i, 2)], bsem.at[i])

    for i in range(steps):
        block_in(i).start()
    zero[...] = jnp.zeros_like(zero)
    for copy in loads:
        copy.wait()

    def saves(i):
        slot = lax.rem(i, 2)
        first = pl.multiple_of(i * GB, GB)
        here = pl.ds(first, GB)
        return [
            pltpu.make_async_copy(save.at[slot], save_hbm.at[i], osem.at[slot, 0]),
            pltpu.make_async_copy(preb.at[slot], pre_hbm.at[pl.ds(pl.multiple_of(first + 8, 8), GB)], osem.at[slot, 1]),
            pltpu.make_async_copy(normedb.at[slot], normed_hbm.at[here], osem.at[slot, 2]),
            pltpu.make_async_copy(gatedb.at[slot], gated_hbm.at[here], osem.at[slot, 3]),
        ]

    head = at.s // rep
    state[...] = jnp.zeros_like(state)
    buf[0:8] = jnp.zeros((8, 640), F32)
    gains[...] = jnp.transpose(w_ref[:, 768:896].astype(F32))[0:8]
    taps = head_taps(taps_ref, head, heads)
    hg = hg_ref[...].astype(F32)
    rows = SeqSum(at, part, got, out, far, (ps, pr, qs, qr))
    enter(at)
    line = SeqGather(at, feed_hbm, feed_out, fs, fr)
    line.start()
    mine = pltpu.make_async_copy(cot, cot_out.at[at.b], lsem.at[0])
    mine.start()
    edge = pltpu.make_async_copy(zero, pre_hbm.at[0:8], lsem.at[1])
    edge.start()
    cots = BatchGather(at, cot, cot_out.at[at.b], cs, cr)
    cots.start()

    def step(i, _):
        first = i * GB
        slot = lax.rem(i, 2)

        @pl.when(i >= 2)
        def _():
            for copy in saves(i - 2):
                copy.wait()

        def keep_map(kind, s, value):
            row = SPAN_ROWS * s + 128 * kind
            save[slot, row : row + value.shape[0]] = value

        def keep_rows(kind, value):
            row = SPAN_ROWS * GS + GB * kind
            save[slot, row : row + GB] = value

        block_in(i).wait()
        x = hid_ref[pl.ds(2 * i, 2)].reshape(GB, -1).astype(F32)
        normed = (x * norm_rows(x) * gains[3:4]).astype(BF16)
        normedb[slot] = normed
        proj = mm(normed, w_ref[:, 0:896])
        pre = proj[:, 0:640].astype(BF16).astype(F32)
        preb[slot] = pre
        gl, sm = proj[:, 640:768], proj[:, 768:896]
        keep_rows(0, gl)
        keep_rows(1, sm)
        buf[8 : 8 + GB] = pre
        mix = conv_mix(buf, taps)
        buf[0:8] = pre[GB - 8 : GB]
        act = mix * jax.nn.sigmoid(mix)
        q = unit(act[:, 0:128])[0] * DK ** (-0.5)
        k0, k1 = unit(act[:, 128:256])[0], unit(act[:, 256:384])[0]
        v0, v1 = act[:, 384:512], act[:, 512:640]
        keep = (first + iota((GB, 1), 0) < len_ref[0]).astype(F32)
        sig0, sig1, al = gates(sm, dbias_ref[head])
        b0, b1 = lane(sig0 * keep), lane(sig1 * keep)
        eg = jnp.exp(jnp.full((1, 1), dlog_ref[head], F32))
        g = lane(-eg * softplus(al) * keep)
        strict, base, levels = sub_masks()
        eye = (iota((128, 128), 0) == iota((128, 128), 1)).astype(F32)
        tri = (iota((64, 64), 0) >= iota((64, 64), 1)).astype(F32)
        causal = iota((64, 128), 0) >= (iota((64, 128), 1) & 63)
        K, Q, V, B, C, N, PM, Kc = [], [], [], [], [], [], [], []
        for s in range(GS):
            sl = slice(64 * s, 64 * s + 64)
            K.append(jnp.concatenate([k0[sl], k1[sl]], axis=0))
            V.append(jnp.concatenate([v0[sl], v1[sl]], axis=0))
            B.append(jnp.concatenate([b0[sl], b1[sl]], axis=0))
            Q.append(q[sl])
            c, e = span_decay(g[sl], tri)
            C.append(c)
            ee = jnp.concatenate([e, e], axis=0)
            gram = mm3(jnp.concatenate([K[s], Q[s]], axis=0), K[s], NT)
            N.append(jnp.where(strict, gram[:128] * ee, 0.0) * B[s])
            PM.append(jnp.where(causal, gram[128:] * e, 0.0))
            cc = jnp.concatenate([c, c], axis=0)
            Kc.append(jnp.exp(cc[63:64] - cc) * K[s])
            keep_map(3, s, N[s])
            keep_map(5, s, PM[s])
        n1 = [jnp.where(base, n, 0.0) for n in N]
        n1s = [split(n) for n in n1]
        n2 = [mm3(a, a) for a in n1s]
        n2s = [split(n) for n in n2]
        n3 = [mm3(a, b) for a, b in zip(n1s, n2s)]
        n4 = [mm3(a, a) for a in n2s]
        y = [eye - a + b - c for a, b, c in zip(n1, n2, n3)]
        X = [a + mm3(a, b) for a, b in zip(y, n4)]
        for lv in levels:
            xs = [split(x_) for x_ in X]
            bl = [jnp.where(lv, n, 0.0) for n in N]
            xb = [mm3(a, b) for a, b in zip(xs, bl)]
            X = [x_ - mm3(a, b) for x_, a, b in zip(X, xb, xs)]
        pl.when(i > 0)(lambda: rows.flush(i - 1))
        for t in range(1, steps // 2):
            pl.when(i == 2 * t)(lambda: line.forward(t))
        W, U = [], []
        for s in range(GS):
            cc = jnp.concatenate([C[s], C[s]], axis=0)
            rhs = jnp.concatenate([B[s] * jnp.exp(cc) * K[s], B[s] * V[s]], axis=1)
            wu = mm3(X[s], rhs)
            W.append(wu[:, :128])
            U.append(wu[:, 128:])
            keep_map(0, s, X[s])
            keep_map(1, s, W[s])
        S = state[...]
        raw = []
        Ws = [split(a) for a in W]
        Kcs = [split(a) for a in Kc]
        for s in range(GS):
            keep_map(4, s, S)
            ss = split(S)
            vn = U[s] - mm3(Ws[s], ss)
            keep_map(2, s, vn)
            vs = split(vn)
            raw.append(jnp.exp(C[s]) * mm3(Q[s], ss) + mm3(PM[s], vs))
            S = jnp.exp(C[s][63:64]) * S + mm3(Kcs[s], vs, TN)
        state[...] = S
        o = jnp.concatenate(raw, axis=0)
        keep_rows(2, o)
        gated = (o * norm_rows(o) * hg * (gl * jax.nn.sigmoid(gl))).astype(BF16)
        gatedb[slot] = gated
        for copy in saves(i):
            copy.start()
        if rep > 1:
            gated = jnp.where(lax.rem(at.s, rep) == 0, gated, jnp.zeros_like(gated))
        part[i] = mm(gated, w_ref[:, 896:1024], NT).astype(BF16).reshape(2, GB // 2, -1)
        rows.start(i)
        return 0

    lax.fori_loop(0, steps, step, 0)
    rows.flush(steps - 1)
    total = rows.finish() + hid_ref[at.s].astype(F32)
    after[...] = total
    nm[...] = (total * norm_rows(total) * gains[4:5]).astype(BF16)
    mids = BatchGather(at, nm, nm_out.at[at.b], ms, mr)
    mids.start()
    own = pltpu.make_async_copy(nm, nm_out.at[at.b], lsem.at[2])
    own.start()
    for t in range(steps // 2, steps):
        line.forward(t)
    rows.drain()
    line.finish()
    for i in (steps - 2, steps - 1):
        for copy in saves(i):
            copy.wait()
    cots.finish()
    mids.finish()
    mine.wait()
    edge.wait()
    own.wait()


def feed_kernel(
    ns, nb,
    nm_hbm, cot_hbm, ff_hbm, mine_hbm, after, gains,
    block_out, d_stream, dbr_out, gfeed, sums,
    nm_all, cot_all, ff, acts, dgs, dus, pmid, pout, got_m, got_o, dbr, gbuf, gdown,
    isem, lsem, ms, mr, os_, or_, gs, gr, ds_s, dr_s,
):
    at = Place(ns, nb)
    greet(at)
    loads = fetch([(nm_hbm, nm_all), (cot_hbm, cot_all)], isem)
    piece = mine_hbm.shape[1]

    def weights(i, src):
        return pltpu.make_async_copy(src, ff.at[:, piece * i : piece * (i + 1)], isem.at[2 + i])

    for i in range(ns):
        pl.when(i == at.s)(lambda: weights(i, mine_hbm).start())
        pl.when(i != at.s)(lambda: weights(i, ff_hbm.at[i]).start())
    for copy in loads:
        copy.wait()
    for i in range(ns):
        weights(i, mine_hbm).wait()
    tok = after.shape[0]
    share = ff.shape[2]
    enter(at)

    def mid_copy(m):
        to = at.peer(m)
        return send(pmid.at[to], got_m.at[m], ms.at[m], mr.at[m], {"batch": to})

    def out_copy(m):
        to = at.peer(m)
        return send(pout.at[to], got_o.at[m], os_.at[m], or_.at[m], {"batch": to})

    def both(ref, one, two):
        return jnp.concatenate([ref[one], ref[two]], axis=0)

    def pair(j, _):
        m = nb - 1 - 2 * j
        one, two = at.peer(m), at.peer(m - 1)
        x, d = both(nm_all, one, two), both(cot_all, one, two)
        ga, ua, da = mm(x, ff[0]), mm(x, ff[1]), mm(d, ff[2])
        sig = jax.nn.sigmoid(ga)
        act = (ga * sig * ua).astype(BF16)
        dg = (da * ua * sig * (1.0 + ga * (1.0 - sig))).astype(BF16)
        du = (da * ga * sig).astype(BF16)
        for ref, value in ((acts, act), (dgs, dg), (dus, du)):
            ref[one] = value[:tok]
            ref[two] = value[tok:]
        p = (mm(dg, ff[0], NT) + mm(du, ff[1], NT)).astype(BF16)
        pmid[one] = p[:tok]
        pmid[two] = p[tok:]
        mid_copy(m).start()
        pl.when(m > 1)(lambda: mid_copy(m - 1).start())
        return 0

    lax.fori_loop(0, nb // 2, pair, 0)

    def outs(j, _):
        m = nb - 1 - 2 * j
        one, two = at.peer(m), at.peer(m - 1)
        p = mm(both(acts, one, two), ff[2], NT).astype(BF16)
        pout[one] = p[:tok]
        pout[two] = p[tok:]
        out_copy(m).start()
        pl.when(m > 1)(lambda: out_copy(m - 1).start())
        return 0

    lax.fori_loop(0, nb // 2, outs, 0)
    x = after[...]
    d_mid = pmid[at.b].astype(F32)
    for m in at.peers():
        mid_copy(m).wait_recv()
        d_mid = d_mid + got_m[m].astype(F32)
    r = norm_rows(x)
    y = x * r
    gfeed[...] = jnp.sum(d_mid * y, axis=0, keepdims=True)
    dy = d_mid * gains[4:5]
    ds_ = cot_all[at.b].astype(F32) + r * (dy - y * jnp.mean(dy * y, axis=-1, keepdims=True))
    d_stream[...] = ds_
    dbr[...] = ds_.astype(BF16)
    line = SeqGather(at, dbr, dbr_out, gs, gr)
    line.start()
    own_rows = pltpu.make_async_copy(dbr, dbr_out.at[at.s], lsem.at[0])
    own_rows.start()
    halves = ns // nb
    deep, cols = share // halves, nm_all.shape[2] // ns
    flat = lambda ref: ref[...].reshape(nb * tok, -1)
    g = mm(flat(acts), flat(cot_all), TN).astype(BF16)
    for b in range(nb):
        for h in range(halves):
            for t in range(halves):
                gdown[b, h, deep * t : deep * (t + 1)] = g[
                    deep * h : deep * (h + 1), cols * (halves * b + t) : cols * (halves * b + t + 1)
                ]
    down = lambda b, h: sums.at[halves * b + h, pl.ds(2 * share, share)]
    moved = [
        send(gdown.at[at.peer(m), h], down(at.b, h), ds_s.at[m, h], dr_s.at[m, h], {"batch": at.peer(m)})
        for m in at.peers()
        for h in range(halves)
    ]
    for copy in moved:
        copy.start()
    kept = [
        pltpu.make_async_copy(gdown.at[at.b, h], down(at.b, h), lsem.at[1 + h]) for h in range(halves)
    ]
    line.forward(1)
    for k, left in enumerate((dgs, dus)):
        g = mm(flat(left), flat(nm_all), TN).astype(BF16)
        for i in range(ns):
            gbuf[k, i] = g[:, cols * i : cols * (i + 1)]
        kept.append(
            pltpu.make_async_copy(gbuf.at[k], sums.at[:, pl.ds(share * k, share)], lsem.at[1 + halves + k])
        )
        if k == 0:
            line.forward(2)
    for copy in kept:
        copy.start()
    for t in range(3, at.nz):
        line.forward(t)
    total = after[...] + pout[at.b].astype(F32)
    for m in at.peers():
        out_copy(m).wait_recv()
        total = total + got_o[m].astype(F32)
    block_out[...] = total.astype(BF16)
    line.finish()
    for copy in moved:
        copy.wait()
    for m in at.peers():
        mid_copy(m).wait_send()
        out_copy(m).wait_send()
    for copy in kept:
        copy.wait()
    own_rows.wait()


def back_kernel(
    ns, nb, rep, heads,
    len_ref, dlog_ref, dbias_ref, dbr_hbm, w_hbm, taps_hbm, hg_ref, normed_hbm, pre_hbm, gated_hbm, save_hbm,
    hid_hbm, sums, gains, d_stream, gfeed,
    grad_in, q_slots, k_slots, gout_sum, small_all, feed_sum,
    dbr_ref, w_ref, taps_ref, hid, save, buf, normedb, gatedb, isem, bsem,
    dbuf, dstate, small, gw, go, part, got, out, far, grads, gout, got_g, piece, got_o, got_s,
    f_own, f_got, f_up, f_down,
    ready, ps, pr, qs, qr, gs, gr, bs, br, kr, os_, or_, ss, sr, us, ur, fi, fps, fpr, fus, fur, fds, fdr,
):
    at = Place(ns, nb)
    greet(at)
    steps = at.nz
    loads = fetch([(w_hbm, w_ref), (taps_hbm, taps_ref), (hid_hbm, hid)], isem)

    def block_in(i):
        slot = lax.rem(i, 2)
        first = pl.multiple_of(i * GB, GB)
        here = pl.ds(first, GB)
        return [
            pltpu.make_async_copy(save_hbm.at[i], save.at[slot], bsem.at[slot, 0]),
            pltpu.make_async_copy(pre_hbm.at[pl.ds(first, 8 + GB)], buf.at[slot], bsem.at[slot, 1]),
            pltpu.make_async_copy(normed_hbm.at[here], normedb.at[slot], bsem.at[slot, 2]),
            pltpu.make_async_copy(gated_hbm.at[here], gatedb.at[slot], bsem.at[slot, 3]),
            pltpu.make_async_copy(dbr_hbm.at[pl.ds(2 * i, 2)], dbr_ref.at[slot], bsem.at[slot, 4]),
        ]

    for copy in block_in(steps - 1):
        copy.start()
    for copy in loads:
        copy.wait()
    head = at.s // rep
    dstate[...] = jnp.zeros_like(dstate)
    dbuf[GB : GB + 8] = jnp.zeros((8, 640), F32)
    small[...] = jnp.zeros_like(small)
    gw[...] = jnp.zeros_like(gw)
    go[...] = jnp.zeros_like(go)
    taps = head_taps(taps_ref, head, heads)
    hg = hg_ref[...].astype(F32)
    rows = SeqSum(at, part, got, out, far, (ps, pr, qs, qr))
    feed = LineSum(at, sums, f_own, f_got, f_up, f_down, (fi, fps, fpr, fus, fur, fds, fdr))
    feed.load()
    enter(at)
    feed.start()
    for ds in range(1, ns):
        pl.semaphore_signal(ready, inc=1, device_id={"seq": at.seq_at(ds)}, device_id_type=MESH)

    when = {f: f + (2 if f == 1 else 3) for f in range(1, feed.turns() + 1)}

    def turn(j, half):
        for f, h in when.items():
            if h < 2 * steps and h % 2 == half:
                pl.when(j == h // 2)(lambda: feed.relay(f))

    def step(j, _):
        i = steps - 1 - j
        first = i * GB
        slot = lax.rem(i, 2)

        @pl.when(i > 0)
        def _():
            for copy in block_in(i - 1):
                copy.start()

        def kept_map(kind, s, high=128):
            row = SPAN_ROWS * s + 128 * kind
            return save[slot, row : row + high]

        def kept_rows(kind):
            row = SPAN_ROWS * GS + GB * kind
            return save[slot, row : row + GB]

        for copy in block_in(i):
            copy.wait()
        dbr = dbr_ref[slot].reshape(GB, -1)
        d_gated = mm(dbr, w_ref[:, 896:1024])
        gl, sm, o = kept_rows(0), kept_rows(1), kept_rows(2)
        sg = jax.nn.sigmoid(gl)
        rr = norm_rows(o)
        yn = o * rr
        dn = d_gated * (gl * sg)
        d_gl = d_gated * (yn * hg) * (sg * (1.0 + gl * (1.0 - sg)))
        dy = dn * hg
        d_raw = rr * (dy - yn * jnp.mean(yn * dy, axis=-1, keepdims=True))
        go[...] += mm(gatedb[slot], dbr, TN)

        mix = conv_mix(buf.at[slot], taps)
        sig = jax.nn.sigmoid(mix)
        act = mix * sig
        qn, rq = unit(act[:, 0:128])
        k0, r0 = unit(act[:, 128:256])
        k1, r1 = unit(act[:, 256:384])
        v0, v1 = act[:, 384:512], act[:, 512:640]
        q = qn * DK ** (-0.5)
        keep = (first + iota((GB, 1), 0) < len_ref[0]).astype(F32)
        sig0, sig1, al = gates(sm, dbias_ref[head])
        eg = jnp.exp(jnp.full((1, 1), dlog_ref[head], F32))
        g1 = -eg * softplus(al) * keep
        g = lane(g1)
        b0, b1 = lane(sig0 * keep), lane(sig1 * keep)
        strict, _, _ = sub_masks()
        tri = (iota((64, 64), 0) >= iota((64, 64), 1)).astype(F32)
        trit = (iota((64, 64), 0) <= iota((64, 64), 1)).astype(F32)
        causal = iota((64, 128), 0) >= (iota((64, 128), 1) & 63)
        K, Q, V, B, C, E, Kc, A1, A2, DO = [], [], [], [], [], [], [], [], [], []
        for s in range(GS):
            sl = slice(64 * s, 64 * s + 64)
            K.append(jnp.concatenate([k0[sl], k1[sl]], axis=0))
            V.append(jnp.concatenate([v0[sl], v1[sl]], axis=0))
            B.append(jnp.concatenate([b0[sl], b1[sl]], axis=0))
            Q.append(q[sl])
            c, e = span_decay(g[sl], tri)
            C.append(c)
            E.append(e)
            cc = jnp.concatenate([c, c], axis=0)
            Kc.append(jnp.exp(cc[63:64] - cc) * K[s])
            do = d_raw[sl]
            DO.append(do)
            A1.append(mm3(kept_map(5, s, HALF), do, TN))
            A2.append(mm3(jnp.exp(c) * Q[s], do, TN))
        dS = dstate[...]
        DV, DS = [None] * GS, [None] * GS
        for s in reversed(range(GS)):
            DS[s] = dS
            dvn = A1[s] + mm3(Kc[s], dS)
            DV[s] = dvn
            dS = jnp.exp(C[s][63:64]) * dS + A2[s] - mm3(kept_map(1, s), dvn, TN)
        dstate[...] = dS
        pl.when(j > 0)(lambda: rows.flush(i + 1))

        pl.when(j == 0)(feed.begin)
        turn(j, 0)
        dq_l, dk0_l, dk1_l, dv0_l, dv1_l, db0_l, db1_l, dg_l = [], [], [], [], [], [], [], []
        for s in range(GS):
            vn, sst, n, p = kept_map(2, s), kept_map(4, s), kept_map(3, s), kept_map(5, s, HALF)
            vns = split(vn)
            ks = split(K[s])
            cc = jnp.concatenate([C[s], C[s]], axis=0)
            ec = jnp.exp(cc)
            ee = jnp.concatenate([E[s], E[s]], axis=0)
            dr = mm3(kept_map(0, s), DV[s], TN)
            both = split(jnp.concatenate([dr, DO[s]], axis=0))
            dd = mm3(both, vns, NT)
            dN = jnp.where(strict, -dd[:128], 0.0)
            dP = jnp.where(causal, dd[128:], 0.0)
            h = mm3(both, sst, NT)
            hk, hq = h[:128], h[128:]
            fh = dP * E[s]
            dq = ec[:64] * hq + mm3(fh, ks)
            dne = dN * ee
            dgm = dne * B[s]
            dkc = mm3(vns, DS[s], NT)
            ekc = jnp.exp(cc[63:64] - cc)
            dk = ekc * dkc - B[s] * ec * hk + mm3(fh, Q[s], TN) + mm3(dgm + jnp.transpose(dgm), ks)
            khk = jnp.sum(K[s] * hk, axis=-1, keepdims=True)
            ecl = ec[:, 0:1]
            db = (
                jnp.sum(dr * V[s], axis=-1, keepdims=True)
                - ecl * khk
                + jnp.sum(dne * mm3(ks, ks, NT), axis=-1, keepdims=True)
            )
            e1 = dN * n
            f1 = dP * p
            z = e1[:64, :64] + e1[:64, 64:] + e1[64:, :64] + e1[64:, 64:] + f1[:, :64] + f1[:, 64:]
            dc = jnp.sum(z - jnp.transpose(z), axis=-1, keepdims=True)
            dks = -B[s][:, 0:1] * ecl * khk
            hj = jnp.sum(Kc[s] * dkc, axis=-1, keepdims=True)
            dc = dc + dks[:64] + dks[64:] - hj[:64] - hj[64:]
            dc = dc + ec[:64, 0:1] * jnp.sum(Q[s] * hq, axis=-1, keepdims=True)
            dcl = jnp.sum(hj, axis=0, keepdims=True) + ec[63:64, 0:1] * jnp.sum(
                jnp.sum(sst * DS[s], axis=-1, keepdims=True), axis=0, keepdims=True
            )
            dg = mm3(trit, lane(dc)) + dcl
            dg_l.append(dg[:, 0:1])
            dq_l.append(dq)
            dk0_l.append(dk[:64])
            dk1_l.append(dk[64:])
            dv = B[s] * dr
            dv0_l.append(dv[:64])
            dv1_l.append(dv[64:])
            db0_l.append(db[:64])
            db1_l.append(db[64:])
        turn(j, 1)
        cat = lambda parts: jnp.concatenate(parts, axis=0)
        dq, dk0, dk1, dv0, dv1 = cat(dq_l), cat(dk0_l), cat(dk1_l), cat(dv0_l), cat(dv1_l)
        db0, db1, dg = cat(db0_l), cat(db1_l), cat(dg_l)

        def unit_back(d, n, rn):
            return rn * (d - n * jnp.sum(d * n, axis=-1, keepdims=True))

        d_act = jnp.concatenate(
            [unit_back(dq * DK ** (-0.5), qn, rq), unit_back(dk0, k0, r0), unit_back(dk1, k1, r1), dv0, dv1],
            axis=1,
        )
        d_mix = d_act * (sig * (1.0 + mix * (1.0 - sig)))
        for t in range(4):
            small[t : t + 1, 0:640] += jnp.sum(d_mix * buf[slot, 5 + t : 5 + t + GB], axis=0, keepdims=True)
        dbuf[0:GB] = d_mix
        d_pre = taps[3:4] * d_mix
        for t in range(3):
            d_pre = d_pre + taps[t : t + 1] * dbuf[3 - t : 3 - t + GB]
        dbuf[GB : GB + 8] = d_mix[0:8]
        d_al = -dg * eg * jax.nn.sigmoid(al) * keep
        d_b0 = db0 * keep * sig0 * (1.0 - sig0)
        d_b1 = db1 * keep * sig1 * (1.0 - sig1)
        lanes = iota((GB, 128), 1)
        d_sm = jnp.where(
            lanes == 0, d_b0, jnp.where(lanes == 1, d_b1, jnp.where(lanes == 2, d_al, 0.0))
        )
        small[0:1, 640:768] += jnp.sum(dn * yn, axis=0, keepdims=True)
        small[1:2, 640:768] += jnp.broadcast_to(jnp.sum(dg * g1, axis=0, keepdims=True), (1, 128))
        small[2:3, 640:768] += jnp.broadcast_to(jnp.sum(d_al, axis=0, keepdims=True), (1, 128))
        dall = jnp.concatenate([d_pre.astype(BF16), d_gl.astype(BF16), d_sm.astype(BF16)], axis=1)
        gw[...] += mm(normedb[slot], dall, TN)
        if rep > 1:
            dall = jnp.where(lax.rem(at.s, rep) == 0, dall, jnp.zeros_like(dall))
        d_normed = mm(dall, w_ref[:, 0:896], NT)
        part[i] = d_normed.astype(BF16).reshape(2, GB // 2, -1)
        rows.start(i)
        small[7:8] += jnp.sum(d_normed * normedb[slot].astype(F32), axis=0, keepdims=True)
        return 0

    lax.fori_loop(0, steps, step, 0)

    small[4:7] = jnp.transpose(gw[:, 768:896])[0:3]
    small[7:8] = small[7:8] / gains[3:4]
    fourth = small.shape[1] // 4
    for k in range(4):
        small[k : k + 1, 3 * fourth :] = gfeed[:, fourth * k : fourth * (k + 1)]
    smalls = [send(small, got_s.at[m], ss.at[m], sr.at[m], {"batch": at.peer(m)}) for m in at.peers()]
    for copy in smalls:
        copy.start()
    nq = q_slots.shape[0]
    part_rows, width = grads.shape[2], q_slots.shape[4]
    grads[...] = gw[:, 0:768].astype(BF16).reshape(ns, nb, part_rows, 768)
    over = [
        send(grads.at[:, at.peer(m)], got_g.at[m], gs.at[m], gr.at[m], {"batch": at.peer(m)}) for m in at.peers()
    ]
    for copy in over:
        copy.start()
    rows.flush(0)
    for f, h in when.items():
        if h >= 2 * steps:
            feed.relay(f)
    high, wide = gout.shape[1:]
    for b in range(nb):
        block = go[:, wide * b : wide * (b + 1)].astype(BF16)
        if rep > 1:
            block = jnp.where(lax.rem(at.s, rep) == 0, block[:high], block[high:])
        gout[b] = block
    outs = [send(gout.at[at.peer(m)], got_o.at[m], os_.at[m], or_.at[m], {"batch": at.peer(m)}) for m in at.peers()]
    for copy in outs:
        copy.start()
    total = small[...]
    for m, copy in zip(at.peers(), smalls):
        copy.wait_recv()
        total = total + got_s[m]
    small_all[at.s] = total
    heads_ = [
        send(small_all.at[at.s], small_all.at[at.s], us.at[ds], ur.at[ds], {"seq": at.seq_at(ds)})
        for ds in range(1, ns)
    ]
    for copy in heads_:
        copy.start()
    for copy in over:
        copy.wait_recv()
    pl.semaphore_wait(ready, ns - 1)
    acc = grads[:, at.b].astype(F32)
    for m in at.peers():
        acc = acc + got_g[m].astype(F32)
    for g, mats in enumerate(((0, 5), (1, 3), (2, 4))):
        for n, m in enumerate(mats):
            block = acc[:, :, 128 * m : 128 * m + 128]
            if rep > 1:
                block = jnp.where(lax.rem(at.s, rep) == 0, block[:, :, :width], block[:, :, width:])
            piece[g, :, n] = block.astype(BF16)
    placed = []
    for g in range(3):
        unit_at = at.s if g < 2 else ns + at.s
        dst, count, dst_sem = (q_slots, nq, br) if g == 0 else (k_slots, 2 * nq, kr)
        owner, slot = unit_at // count, lax.rem(unit_at, count)
        for row in range(ns):
            placed.append((g, row, owner, dst.at[slot, :, at.b], dst_sem.at[slot, at.b]))

    def place(item):
        g, row, owner, dst, sem = item
        src = piece.at[g, row]
        here = jnp.logical_and(row == at.s, owner == at.b)
        far_copy = lambda: send(src, dst, bs.at[g, row], sem, {"seq": row, "batch": owner})
        near_copy = lambda: pltpu.make_async_copy(src, dst, sem)
        return here, far_copy, near_copy

    for item in placed:
        here, far_copy, near_copy = place(item)
        pl.when(here)(lambda: near_copy().start())
        pl.when(jnp.logical_not(here))(lambda: far_copy().start())

    d_normed = rows.finish()
    x = hid[...].astype(F32)
    r = norm_rows(x)
    y = x * r
    dy = d_normed * gains[3:4]
    grad_in[...] = (d_stream[...] + r * (dy - y * jnp.mean(dy * y, axis=-1, keepdims=True))).astype(BF16)
    acc = gout[at.b].astype(F32)
    for m, copy in zip(at.peers(), outs):
        copy.wait_recv()
        acc = acc + got_o[m].astype(F32)
    gout_sum[...] = acc
    for copy in heads_:
        copy.wait_recv()
    for item in placed:
        here, far_copy, _ = place(item)
        pl.when(jnp.logical_not(here))(lambda: far_copy().wait_send())
    for dst, sem in ((q_slots, br), (k_slots, kr)):
        for slot in range(dst.shape[0]):
            for b in range(nb):
                pltpu.make_async_copy(piece.at[0, 0], dst.at[slot, :, b], sem.at[slot, b]).wait()
    for copy in smalls + over + outs + heads_:
        copy.wait_send()
    feed.finish(feed_sum)
    feed.drain()
    rows.drain()


class LineSum:
    def __init__(self, at, part, own, got, ups, downs, sems):
        self.at, self.part, self.own, self.got = at, part, own, got
        self.line = (ups, downs)
        self.isem, self.pair_s, self.pair_r, self.sems = sems[0], sems[1], sems[2], sems[3:]

    def mine(self, i):
        return pltpu.make_async_copy(self.part.at[i, self.at.c], self.own.at[i], self.isem.at[i])

    def pair(self, i):
        at = self.at
        return send(self.part.at[i, 1 - at.c], self.got.at[i], self.pair_s.at[i], self.pair_r.at[i], {"seq": at.sib})

    def hop(self, i, up, src=None):
        buf, k = self.line[0 if up else 1], 0 if up else 2
        return send(
            buf.at[i] if src is None else src, buf.at[i], self.sems[k].at[i], self.sems[k + 1].at[i],
            {"seq": self.at.s + 2 if up else self.at.s - 2},
        )

    def load(self):
        for i in range(self.at.nz):
            self.mine(i).start()

    def start(self):
        for i in range(self.at.nz):
            self.pair(i).start()

    def begin(self):
        at, nz = self.at, self.at.nz
        for i in range(nz):
            self.mine(i).wait()
            self.pair(i).wait_recv()
            self.own[i] = (self.own[i].astype(F32) + self.got[i].astype(F32)).astype(BF16)
        for k in range(nz - 1):
            pl.when(at.z == 0)(lambda: self.hop(nz - 1 - k, True, self.own.at[nz - 1 - k]).start())
            pl.when(at.z == nz - 1)(lambda: self.hop(k, False, self.own.at[k]).start())

    def relay(self, f):
        at, nz = self.at, self.at.nz
        for a in range(1, nz - 1):
            k = f - (2 * a - 1)
            if not 0 <= k < nz - 1 - a:
                continue

            @pl.when(at.z == a)
            def _():
                self.pass_on(nz - 1 - k, True)

            @pl.when(at.z == nz - 1 - a)
            def _():
                self.pass_on(k, False)

    def turns(self):
        nz = self.at.nz
        return max(2 * a - 1 + nz - 2 - a for a in range(1, nz - 1)) if nz > 2 else 0

    def pass_on(self, i, up):
        buf = self.line[0 if up else 1]
        self.hop(i, up).wait_recv()
        buf[i] = (buf[i].astype(F32) + self.own[i].astype(F32)).astype(BF16)
        self.hop(i, up).start()

    def finish(self, out):
        at = self.at
        out[...] = self.own[at.z].astype(F32)
        for up in (True, False):

            @pl.when(at.z > 0 if up else at.z < at.nz - 1)
            def _():
                self.hop(at.z, up).wait_recv()
                out[...] += self.line[0 if up else 1][at.z].astype(F32)

    def drain(self):
        at, nz = self.at, self.at.nz
        for i in range(nz):
            self.pair(i).wait_send()
            pl.when(i > at.z)(lambda: self.hop(i, True).wait_send())
            pl.when(i < at.z)(lambda: self.hop(i, False).wait_send())


def finish_kernel(
    rep, heads, share, halves,
    block_in, grad_in_, q_in, k_in, gout_in, small_in, feed_in,
    o_block, o_grad, o_gain, o_q, o_k, o_v, o_beta, o_alpha, o_gate, o_out, o_mid, o_fg, o_fu, o_fd, o_taps, o_log,
    o_bias, o_hg,
    block, grad, q_slots, k_slots, gout, small, feed, gq, gk, gv, gg, fd, taps, vec_a, vec_b, dlog, dbias,
    hgain, stack, isem, osem,
):
    loads = fetch(
        [
            (q_in, q_slots), (feed_in, feed), (small_in, small), (block_in, block), (grad_in_, grad),
            (gout_in, gout), (k_in, k_slots),
        ],
        isem,
    )
    outs = []

    def put(src, dst):
        copy = pltpu.make_async_copy(src, dst, osem.at[len(outs)])
        copy.start()
        outs.append(copy)

    loads[0].wait()
    loads[6].wait()
    cw = q_slots.shape[4]
    for ref, slots, n in ((gq, q_slots, 0), (gg, q_slots, 1), (gk, k_slots, 0), (gv, k_slots, 1)):
        for k in range(slots.shape[0]):
            ref[:, cw * k : cw * (k + 1)] = slots[k, n].astype(F32).reshape(ref.shape[0], cw)
    for src, dst in ((gq, o_q), (gk, o_k), (gv, o_v), (gg, o_gate)):
        put(src, dst)
    loads[1].wait()
    deep, cols = share // halves, feed.shape[1]
    for t in range(halves):
        fd[:, cols * t : cols * (t + 1)] = feed[2 * share + deep * t : 2 * share + deep * (t + 1)]
    for src, dst in ((feed.at[0:share], o_fg), (feed.at[share : 2 * share], o_fu), (fd, o_fd)):
        put(src, dst)
    loads[2].wait()
    lanes = iota((1, heads), 1)
    log_row, bias_row, gain_row = jnp.zeros((1, heads), F32), jnp.zeros((1, heads), F32), jnp.zeros((1, DK), F32)
    for h in range(heads):
        at = small.at[rep * h]
        for j in range(3):
            stack[j * heads + h : j * heads + h + 1] = at[4 + j : 5 + j]
        for g in range(5):
            col = DK * (heads * g + h)
            taps[:, col : col + DK] = at[0:4, DK * g : DK * (g + 1)]
        gain_row = gain_row + at[0:1, 5 * DK : 6 * DK]
        log_row = jnp.where(lanes == h, at[1:2, 5 * DK : 5 * DK + 1], log_row)
        bias_row = jnp.where(lanes == h, at[2:3, 5 * DK : 5 * DK + 1], bias_row)
    hgain[...] = gain_row
    dlog[...] = log_row
    dbias[...] = bias_row
    for src, dst in ((stack.at[: 2 * heads], o_beta), (stack.at[2 * heads :], o_alpha), (taps, o_taps), (hgain, o_hg), (dlog, o_log), (dbias, o_bias)):
        put(src, dst)
    every = small[0]
    for k in range(1, small.shape[0]):
        every = every + small[k]
    vec_a[...] = every[7:8]
    fourth = every.shape[1] // 4
    for k in range(4):
        vec_b[:, fourth * k : fourth * (k + 1)] = every[k : k + 1, 3 * fourth :]
    put(vec_a, o_gain)
    put(vec_b, o_mid)
    for copy, src, dst in ((loads[3], block, o_block), (loads[4], grad, o_grad), (loads[5], gout, o_out)):
        copy.wait()
        put(src, dst)
    for copy in outs:
        copy.wait()


def comm_call(kernel, outs, scratch, ident, name, args, specs, limit):
    return pl.pallas_call(
        kernel,
        in_specs=specs,
        out_specs=[o[1] for o in outs],
        out_shape=[o[0] for o in outs],
        scratch_shapes=scratch,
        compiler_params=pltpu.CompilerParams(
            collective_id=ident, has_side_effects=True, vmem_limit_bytes=limit * 1024 * 1024
        ),
        name=name,
    )(*args)


def dma(*shape):
    return pltpu.SemaphoreType.DMA(shape)


def on_device(
    hidden_in, cotangent, lengths, mixer_gain, query_weight, key_weight, value_weight, beta_weight, alpha_weight,
    gate_weight, out_weight, feed_gain, feed_gate, feed_up, feed_down, conv_taps, decay_log, decay_bias, head_gain,
):
    ns, nb = lax.axis_size("seq"), lax.axis_size("batch")
    heads = decay_log.shape[0]
    rep = ns // heads
    tok, width = hidden_in.shape[1:]
    assert hidden_in.shape[0] == 1 and ns == rep * heads and ns % nb == 0 and 2 * tok == GB
    rows = query_weight.shape[0]
    share = feed_gate.shape[1] // nb
    halves = ns // nb
    nz = ns // 2
    n = ns * tok
    sds = jax.ShapeDtypeStruct
    vmem, hbm = pl.BlockSpec(memory_space=pltpu.VMEM), pl.BlockSpec(memory_space=pltpu.HBM)
    smem = pl.BlockSpec(memory_space=pltpu.SMEM)
    hidden, cot = hidden_in[0], cotangent[0]
    buffer = lambda *shape: pltpu.VMEM(shape, BF16)
    block = lambda count: buffer(count, tok, width)
    wide = lambda *shape: pltpu.VMEM(shape, F32)
    vout = lambda kind, *shape: (sds(shape, kind), vmem)
    hout = lambda kind, *shape: (sds(shape, kind), hbm)
    key = heads * DK

    hid_all, wm, ff = comm_call(
        functools.partial(gather_kernel, ns, nb, rep, heads),
        [hout(BF16, ns, tok, width), hout(BF16, ns, nb, rows, 8 * DK), hout(BF16, 3, nb, rows, share)],
        [
            buffer(tok, width), buffer(rows, key), buffer(rows, 2 * key), buffer(rows, 2 * key), buffer(rows, key),
            buffer(rows, key), buffer(rows, nb * share), buffer(rows, nb * share), buffer(rows, nb * share),
            buffer(heads, rows, 8 * DK), buffer(nb, 3, rows, share), dma(9), dma(3), dma(4 * nz), dma(4 * nz), dma(ns),
            dma(ns), dma(nz, nb), dma(nz, nb), dma(nb), dma(nb),
        ],
        0, "gather",
        (
            hidden, query_weight, key_weight, value_weight, gate_weight, out_weight.T, beta_weight.T, alpha_weight.T,
            mixer_gain[None], feed_gain[None], feed_gate, feed_up, feed_down.T,
        ),
        [hbm] * 6 + [vmem] * 4 + [hbm] * 3, 62,
    )
    wm = wm.reshape(width, 8 * DK)
    ff = ff.reshape(3, nb * rows, share)
    hg = head_gain[None]
    normed, pre, gated, save, gains, after, nm_all, cot_all, ff_all = comm_call(
        functools.partial(front_kernel, ns, nb, rep, heads),
        [
            hout(BF16, n, width), hout(F32, n + 8, 5 * DK), hout(BF16, n, DK), hout(F32, nz, SAVE_ROWS, DK),
            vout(F32, 8, width), vout(F32, tok, width), hout(BF16, nb, tok, width), hout(BF16, nb, tok, width),
            hout(BF16, ns, 3, nb * rows, share),
        ],
        [
            block(ns), buffer(width, 8 * DK), buffer(4, 5 * key), buffer(tok, width), buffer(tok, width),
            wide(8, 5 * DK), wide(2, SAVE_ROWS, DK), wide(2, GB, 5 * DK), buffer(2, GB, width), buffer(2, GB, DK),
            wide(8 + GB, 5 * DK), wide(DK, DK), buffer(nz, 2, tok, width), block(nz), block(nz), block(nz),
            dma(3), dma(nz), dma(3), dma(2, 4), dma(nz), dma(nz), dma(nz), dma(nz), dma(nb), dma(nb), dma(nb), dma(nb),
            dma(4 * nz), dma(4 * nz),
        ],
        1, "front",
        (lengths, decay_log, decay_bias, hid_all, wm, conv_taps, hg, cot, ff),
        [smem] * 3 + [hbm] * 3 + [vmem, hbm, hbm], 61,
    )
    block_out, d_stream, dbr_all, gfeed, sums = comm_call(
        functools.partial(feed_kernel, ns, nb),
        [
            vout(BF16, tok, width), vout(F32, tok, width), hout(BF16, ns, tok, width), vout(F32, 1, width),
            hout(BF16, ns, 3 * share, width // ns),
        ],
        [
            block(nb), block(nb), buffer(3, width, share), buffer(nb, tok, share), buffer(nb, tok, share),
            buffer(nb, tok, share), block(nb), block(nb), block(nb), block(nb), buffer(tok, width),
            buffer(2, ns, share, width // ns), buffer(nb, halves, share, width // ns),
            dma(2 + ns), dma(3 + halves), dma(nb), dma(nb), dma(nb), dma(nb), dma(4 * nz), dma(4 * nz), dma(nb, halves),
            dma(nb, halves),
        ],
        2, "feed", (nm_all, cot_all, ff_all, ff, after, gains), [hbm] * 4 + [vmem] * 2, 61,
    )
    nq = ns // nb
    cw = DK // rep
    wrows = width // ns
    deep = 3 * share
    feed_buffers = [buffer(nz, deep, width // ns)] * 4
    quarter = wrows // nb
    grad_in, q_slots, k_slots, gout_sum, small_all, feed_sum = comm_call(
        functools.partial(back_kernel, ns, nb, rep, heads),
        [
            vout(BF16, tok, width), vout(BF16, nq, 2, nb, quarter, cw), vout(BF16, 2 * nq, 2, nb, quarter, cw),
            vout(F32, DK // rep, width // nb),
            vout(F32, ns, 8, width), vout(F32, deep, width // ns),
        ],
        [
            buffer(2, 2, tok, width), buffer(width, 8 * DK), buffer(4, 5 * key), buffer(tok, width),
            wide(2, SAVE_ROWS, DK), wide(2, 8 + GB, 5 * DK), buffer(2, GB, width), buffer(2, GB, DK), dma(3), dma(2, 5),
            wide(GB + 8, 5 * DK), wide(DK, DK), wide(8, width), wide(width, 7 * DK),
            wide(DK, width), buffer(nz, 2, tok, width), block(nz), block(nz), block(nz),
            buffer(ns, nb, quarter, 6 * DK), buffer(nb, DK // rep, width // nb), buffer(nb, ns, quarter, 6 * DK),
            buffer(3, ns, 2, quarter, cw), buffer(nb, DK // rep, width // nb), wide(nb, 8, width),
            *feed_buffers, pltpu.SemaphoreType.REGULAR,
            dma(nz), dma(nz), dma(nz), dma(nz), dma(nb), dma(nb), dma(3, ns), dma(nq, nb), dma(2 * nq, nb),
            dma(nb), dma(nb), dma(nb), dma(nb), dma(ns), dma(ns),
            *[dma(nz)] * 7,
        ],
        3, "back",
        (
            lengths, decay_log, decay_bias, dbr_all, wm, conv_taps, hg, normed, pre, gated, save, hidden,
            sums.reshape(nz, 2, deep, width // ns), gains, d_stream, gfeed,
        ),
        [smem] * 3 + [hbm] * 3 + [vmem] + [hbm] * 6 + [vmem] * 3, 61,
    )

    shapes = [
        sds((tok, width), BF16), sds((tok, width), BF16), sds((1, width), F32), sds((wrows, nq * cw), F32),
        sds((wrows, 2 * nq * cw), F32), sds((wrows, 2 * nq * cw), F32), sds((2 * heads, width), F32),
        sds((heads, width), F32), sds((wrows, nq * cw), F32), sds((DK // rep, width // nb), F32), sds((1, width), F32),
        sds((share, wrows), F32), sds((share, wrows), F32), sds((share // halves, width // nb), F32),
        sds((4, 5 * key), F32), sds((1, heads), F32), sds((1, heads), F32), sds((1, DK), F32),
    ]
    like = lambda *which: [pltpu.VMEM(shapes[k].shape, shapes[k].dtype) for k in which]
    outs = list(pl.pallas_call(
        functools.partial(finish_kernel, rep, heads, share, halves),
        in_specs=[hbm] * 7,
        out_specs=[hbm] * len(shapes),
        out_shape=shapes,
        scratch_shapes=like(0, 1) + [buffer(nq, 2, nb, quarter, cw), buffer(2 * nq, 2, nb, quarter, cw)] + like(9) + [wide(ns, 8, width)]
        + [wide(deep, width // ns)] + like(3, 4, 5, 8, 13, 14, 2, 10, 15, 16, 17)
        + [wide(3 * heads, width), dma(7), dma(len(shapes))],
        compiler_params=pltpu.CompilerParams(vmem_limit_bytes=61 * 1024 * 1024),
        name="finish",
    )(block_out, grad_in, q_slots, k_slots, gout_sum, small_all, feed_sum))
    for k in (0, 1):
        outs[k] = outs[k][None]
    for k in (6, 7, 11, 12):
        outs[k] = outs[k].T
    for k in (2, 10, 15, 16, 17):
        outs[k] = outs[k][0]
    return tuple(outs)


def solution(mesh):
    both = ("seq", "batch")
    tokens, split_rows, grid = P("batch", "seq", None), P(both, None), P("seq", "batch")
    return jax.shard_map(
        on_device,
        mesh=mesh,
        in_specs=(
            tokens, tokens, P("batch"), P(both), split_rows, split_rows, split_rows, split_rows, split_rows,
            split_rows, P(None, both), P(both), split_rows, split_rows, P(None, both), P(), P(), P(), P(),
        ),
        out_specs=(
            tokens, tokens, P(), grid, grid, grid, P(), P(), grid, grid, P(), grid, grid, grid, P(), P(), P(), P(),
        ),
        check_vma=False,
    )
```

```python
import functools
import jax
import jax.numpy as jnp
from jax import lax
from jax.experimental import pallas as pl
from jax.experimental.pallas import tpu as pltpu
from jax.sharding import PartitionSpec as P

F32, BF16 = jnp.float32, jnp.bfloat16
EPS = 1e-05
DK = 128
HALF = 64
GS = 4
GB = GS * HALF
NN = (((1,), (0,)), ((), ()))
NT = (((1,), (1,)), ((), ()))
TN = (((0,), (0,)), ((), ()))


def mm(a, b, dims=NN):
    return lax.dot_general(a.astype(BF16), b.astype(BF16), dims, preferred_element_type=F32)


def split(a):
    hi = a.astype(BF16)
    return hi, (a - hi.astype(F32)).astype(BF16)


def mm3(a, b, dims=NN):
    (ah, al), (bh, bl) = (x if isinstance(x, tuple) else split(x) for x in (a, b))
    return (
        lax.dot_general(ah, bl, dims, preferred_element_type=F32)
        + lax.dot_general(al, bh, dims, preferred_element_type=F32)
    ) + lax.dot_general(ah, bh, dims, preferred_element_type=F32)


def iota(shape, axis):
    return lax.broadcasted_iota(jnp.int32, shape, axis)


def sub_masks():
    rows, cols = iota((128, 128), 0), iota((128, 128), 1)
    tr, tc = 2 * (rows & 63) + (rows >> 6), 2 * (cols & 63) + (cols >> 6)
    strict = tr > tc
    levels = []
    for bits in range(3, 7):
        same_up = (tr >> (bits + 1)) == (tc >> (bits + 1))
        levels.append(strict & same_up & ((tr >> bits) != (tc >> bits)))
    base = strict & ((tr >> 3) == (tc >> 3))
    return strict, base, levels


def unit(a):
    r = lax.rsqrt(jnp.sum(a * a, axis=-1, keepdims=True) + EPS)
    return a * r, r


def softplus(x):
    return jnp.maximum(x, 0.0) + jnp.log1p(jnp.exp(-jnp.abs(x)))


def lane(x, width=128):
    return jnp.broadcast_to(x, (x.shape[0], width))


def gates(sm, dec_bias):
    return jax.nn.sigmoid(sm[:, 0:1]), jax.nn.sigmoid(sm[:, 1:2]), sm[:, 2:3] + dec_bias


def span_decay(gb, tri):
    c = mm3(tri, gb)
    ct = jnp.transpose(jnp.concatenate([c, c], axis=0))[:64]
    e = jnp.exp(jnp.minimum(c - ct, 0.0))
    return c, e


def conv_mix(buf, taps):
    mix = taps[0:1] * buf[5 : 5 + GB]
    for j in range(1, 4):
        mix = mix + taps[j : j + 1] * buf[5 + j : 5 + j + GB]
    return mix


def head_taps(taps_ref, head, heads):
    parts = []
    for col in (head, heads + head, 2 * heads + head, 3 * heads + head, 4 * heads + head):
        parts.append(taps_ref[:, pl.ds(pl.multiple_of(col * 128, 128), 128)].astype(F32))
    return jnp.concatenate(parts, axis=1)


MESH = pl.DeviceIdType.MESH
SPAN_ROWS = 5 * 128 + HALF
SAVE_ROWS = GS * SPAN_ROWS + 3 * GB


class Place:
    def __init__(self, ns, nb):
        self.ns, self.nb, self.nz = ns, nb, ns // 2
        self.s, self.b = lax.axis_index("seq"), lax.axis_index("batch")
        self.z, self.c = self.s // 2, lax.rem(self.s, 2)
        self.sib = self.s + 1 - 2 * self.c

    def seq_at(self, ds):
        return lax.rem(self.s + ds, self.ns)

    def seq_before(self, ds):
        return lax.rem(self.s + self.ns - ds, self.ns)

    def peer(self, mask):
        out, bit = 0, 1
        while bit < self.nb:
            mine, other = lax.rem(self.b // bit, 2), lax.rem(mask // bit, 2) if not isinstance(mask, int) else mask // bit % 2
            out = out + bit * (mine + other - 2 * mine * other)
            bit *= 2
        return out

    def peers(self):
        return range(self.nb - 1, 0, -1)


def greet(at):
    barrier = pltpu.get_barrier_semaphore()
    for ds in range(1, at.ns):
        pl.semaphore_signal(barrier, inc=1, device_id={"seq": at.seq_at(ds)}, device_id_type=MESH)
    for m in at.peers():
        pl.semaphore_signal(barrier, inc=1, device_id={"batch": at.peer(m)}, device_id_type=MESH)


def enter(at):
    pl.semaphore_wait(pltpu.get_barrier_semaphore(), at.ns + at.nb - 2)


def send(src, dst, send_sem, recv_sem, where):
    return pltpu.make_async_remote_copy(
        src_ref=src, dst_ref=dst, send_sem=send_sem, recv_sem=recv_sem, device_id=where, device_id_type=MESH
    )


def fetch(pairs, sem):
    copies = [pltpu.make_async_copy(src, dst, sem.at[k]) for k, (src, dst) in enumerate(pairs)]
    for copy in copies:
        copy.start()
    return copies


class BatchGather:
    def __init__(self, at, src, out_at, ssem, rsem):
        self.copies = [
            send(src, out_at, ssem.at[m], rsem.at[m], {"batch": at.peer(m)}) for m in at.peers()
        ]

    def start(self):
        for copy in self.copies:
            copy.start()

    def finish(self):
        for copy in self.copies:
            copy.wait_recv()
        for copy in self.copies:
            copy.wait_send()


class SeqGather:
    def __init__(self, at, src, out, ssem, rsem):
        self.at, self.src, self.out, self.ssem, self.rsem = at, src, out, ssem, rsem

    def hop(self, t, up):
        at = self.at
        origin = at.z - (t - 1) if up else at.z + (t - 1)
        slot = 2 * origin + at.c
        src = self.src if t == 1 else self.out.at[slot]
        to = at.s + 2 if up else at.s - 2
        k = t if up else at.nz + t
        return send(src, self.out.at[slot], self.ssem.at[k], self.rsem.at[k], {"seq": to})

    def can_send(self, t, up):
        at = self.at
        if up:
            return jnp.logical_and(at.z - (t - 1) >= 0, at.z + 1 < at.nz)
        return jnp.logical_and(at.z + (t - 1) < at.nz, at.z >= 1)

    def can_recv(self, t, up):
        return self.at.z - t >= 0 if up else self.at.z + t < self.at.nz

    def across(self, t, up):
        at, nz = self.at, self.at.nz
        k = 2 * nz + (t if up else nz + t)
        origin = 0 if t == 0 else (-t if up else t)
        slot = 2 * (at.z + origin) + at.c
        src = self.src if t == 0 else self.out.at[slot]
        return send(src, self.out.at[slot], self.ssem.at[k], self.rsem.at[k], {"seq": at.sib})

    def start(self):
        for up in (True, False):
            pl.when(self.can_send(1, up))(lambda: self.hop(1, up).start())
        self.across(0, True).start()

    def forward(self, t):
        for up in (True, False):

            @pl.when(self.can_recv(t, up))
            def _():
                self.hop(t, up).wait_recv()
                if t + 1 < self.at.nz:
                    pl.when(self.can_send(t + 1, up))(lambda: self.hop(t + 1, up).start())
                self.across(t, up).start()

    def finish(self):
        self.across(0, True).wait()
        for t in range(1, self.at.nz):
            for up in (True, False):
                pl.when(self.can_recv(t, up))(lambda: self.across(t, up).wait())
                pl.when(self.can_send(t, up))(lambda: self.hop(t, up).wait_send())


class SeqSum:
    def __init__(self, at, part, got, out, far, sems):
        self.at, self.part, self.got, self.out, self.far = at, part, got, out, far
        self.pair_s, self.pair_r, self.hop_s, self.hop_r = sems

    def pair(self, i):
        at = self.at
        return send(self.part.at[i, 1 - at.c], self.got.at[i], self.pair_s.at[i], self.pair_r.at[i], {"seq": at.sib})

    def hop(self, i):
        at = self.at
        dz = lax.rem(i - at.z + at.nz, at.nz)
        return send(self.out.at[i], self.far.at[dz], self.hop_s.at[i], self.hop_r.at[dz], {"seq": 2 * i + at.c})

    def start(self, i):
        self.pair(i).start()

    def flush(self, i):
        self.pair(i).wait_recv()

        @pl.when(i != self.at.z)
        def _():
            mine = self.part[i, self.at.c].astype(F32)
            self.out[i] = (mine + self.got[i].astype(F32)).astype(BF16)
            self.hop(i).start()

    def finish(self):
        at = self.at
        total = self.part[at.z, at.c].astype(F32) + self.got[at.z].astype(F32)
        for dz in range(1, at.nz):
            send(self.out.at[0], self.far.at[dz], self.hop_s.at[0], self.hop_r.at[dz], {"seq": at.sib}).wait_recv()
            total = total + self.far[dz].astype(F32)
        return total

    def drain(self):
        for i in range(self.at.nz):
            self.pair(i).wait_send()
            pl.when(i != self.at.z)(lambda: self.hop(i).wait_send())


def norm_rows(x):
    return lax.rsqrt(jnp.mean(x * x, axis=-1, keepdims=True) + EPS)


def collect(
    at, rep, heads,
    hid, wq, wk, wv, wg, wo, beta, alpha, gain_in, gain_mid, fg, fu, fd,
    hid_out, wm_out, ff_out,
    hv, qv, kv, vv, gv, ov, fgv, fuv, fdv, wbuf, fbuf, isem, lsem, hs, hr, ws, wr, os_, or_, fs, fr,
):
    ns, nb = at.ns, at.nb
    greet(at)
    loads = fetch(
        [(hid, hv), (wq, qv), (wk, kv), (wv, vv), (wg, gv), (wo, ov), (fg, fgv), (fu, fuv), (fd, fdv)], isem
    )
    rows = beta.shape[1]
    lanes = iota((rows, 128), 1)
    eye = iota((rows, rows), 0) == iota((rows, rows), 1)
    column = lambda ref, k=0: jnp.sum(jnp.where(eye, ref[k : k + 1].astype(F32), 0.0), axis=1, keepdims=True)
    tail = jnp.where(lanes == 3, column(gain_in), jnp.where(lanes == 4, column(gain_mid), 0.0))
    share = fbuf.shape[3]
    for copy in loads[1:6]:
        copy.wait()
    for h in range(heads):
        col = lambda j: slice(128 * (j * heads + h), 128 * (j * heads + h) + 128)
        small = jnp.where(lanes == 0, column(beta, h), tail)
        small = jnp.where(lanes == 1, column(beta, heads + h), small)
        small = jnp.where(lanes == 2, column(alpha, h), small)
        parts = (
            qv[:, col(0)], kv[:, col(0)], kv[:, col(1)], vv[:, col(0)], vv[:, col(1)], gv[:, col(0)],
            small.astype(BF16), ov[:, col(0)],
        )
        for j, p in enumerate(parts):
            wbuf[h, :, 128 * j : 128 * j + 128] = p
    loads[0].wait()
    enter(at)

    def piece(to, where):
        return send(wbuf.at[to // rep], wm_out.at[at.s, at.b], ws.at[to], wr.at[at.s], where)

    def arrives(origin):
        send(wbuf.at[0], wm_out.at[origin, at.b], ws.at[0], wr.at[origin], {"seq": at.sib}).wait_recv()

    square = nb == 4

    def hop(block, sem, m):
        return lambda: send(block, block, os_.at[sem], or_.at[sem], {"batch": at.peer(m)})

    def plane(zo):
        block = wm_out.at[pl.ds(2 * zo, 2), at.b]
        half = lambda core, m: wm_out.at[2 * zo + core, at.peer(m)]
        if not square:
            return [hop(block, (zo, m), m) for m in at.peers()], []
        first = [hop(block, (zo, m), m) for m in (1, 2)]
        return first, [hop(half(0, 1), (zo, 3), 2), hop(half(1, 2), (zo, 0), 1)]

    def pass_on(zo):
        for copy in plane(zo)[0]:
            copy().start()

    def follow(zo):
        first, then = plane(zo)
        for copy, onward in zip(first, then):
            copy().wait_recv()
            onward().start()

    def around(fn):
        for t in range(1, at.nz):
            pl.when(at.z + t < at.nz)(lambda: fn(at.z + t))
            pl.when(at.z - t >= 0)(lambda: fn(at.z - t))

    def scatter(zo):
        for core in range(2):
            piece(2 * zo + core, {"seq": 2 * zo + core}).start()

    own = pltpu.make_async_copy(wbuf.at[at.s // rep], wm_out.at[at.s, at.b], lsem.at[0])
    own.start()
    piece(at.sib, {"seq": at.sib}).start()
    around(scatter)
    line = SeqGather(at, hv, hid_out, hs, hr)
    line.start()
    place = pltpu.make_async_copy(hv, hid_out.at[at.s], lsem.at[1])
    place.start()
    arrives(at.sib)
    own.wait()
    pass_on(at.z)
    for copy in loads[6:]:
        copy.wait()
    for b in range(nb):
        for j, w in enumerate((fgv, fuv, fdv)):
            fbuf[b, j] = w[:, share * b : share * (b + 1)]
    kept = pltpu.make_async_copy(fbuf.at[at.b], ff_out.at[:, at.b], lsem.at[2])
    kept.start()
    cols = [
        send(fbuf.at[at.peer(m)], ff_out.at[:, at.b], fs.at[m], fr.at[m], {"batch": at.peer(m)}) for m in at.peers()
    ]

    def relay(zo):
        for core in range(2):
            arrives(2 * zo + core)
        pass_on(zo)

    def at_distance(t, fn):
        if t == 0:
            fn(at.z)
        else:
            pl.when(at.z + t < at.nz)(lambda: fn(at.z + t))
            pl.when(at.z - t >= 0)(lambda: fn(at.z - t))

    for t in range(1, at.nz):
        at_distance(t, relay)
        line.forward(t)
        at_distance(t - 1, follow)
        if t == 1:
            for copy in cols:
                copy.start()
    at_distance(at.nz - 1, follow)
    line.finish()

    def settle(zo):
        first, then = plane(zo)
        for copy in then if square else first:
            copy().wait_recv()
        for copy in first + then:
            copy().wait_send()

    for zo in range(at.nz):
        settle(zo)
    piece(at.sib, {"seq": at.sib}).wait_send()

    def sent(zo):
        for core in range(2):
            piece(2 * zo + core, {"seq": 2 * zo + core}).wait_send()

    around(sent)
    for copy in cols:
        copy.wait()
    place.wait()
    kept.wait()


def front_kernel(
    ns, nb, rep, heads,
    len_ref, dlog_ref, dbias_ref, taps_hbm, hg_ref, cot_hbm,
    hid, wq, wk, wv, wg, wo, beta, alpha, gain_in, gain_mid, fg, fu, fd,
    w_hbm, feed_hbm, normed_hbm, pre_hbm, gated_hbm, save_hbm, gains, after, nm_out, cot_out, feed_out,
    hv, qv, kv, vv, gv, ov, fgv, fuv, fdv, wbuf, fbuf, gisem, glsem, hs, hr, ws, wr, gs, gr, gfs, gfr,
    hid_ref, w4, taps_ref, cot, nm, zero, save, preb, normedb, gatedb,
    buf, state, part, got, out, far, isem, bsem, lsem, osem, ps, pr, qs, qr, ms, mr, cs, cr, fs, fr,
):
    at = Place(ns, nb)
    steps = at.nz
    loads = fetch([(taps_hbm, taps_ref), (cot_hbm, cot)], isem)
    collect(
        at, rep, heads, hid, wq, wk, wv, wg, wo, beta, alpha, gain_in, gain_mid, fg, fu, fd, hid_ref, w4, feed_hbm,
        hv, qv, kv, vv, gv, ov, fgv, fuv, fdv, wbuf, fbuf, gisem, glsem, hs, hr, ws, wr, gs, gr, gfs, gfr,
    )
    weights_out = pltpu.make_async_copy(w4, w_hbm, bsem.at[0])
    weights_out.start()
    columns = lambda a, b: w4[:, :, :, a:b].reshape(-1, b - a)
    zero[...] = jnp.zeros_like(zero)
    for copy in loads:
        copy.wait()

    def saves(i):
        slot = lax.rem(i, 2)
        first = pl.multiple_of(i * GB, GB)
        here = pl.ds(first, GB)
        return [
            pltpu.make_async_copy(save.at[slot], save_hbm.at[i], osem.at[slot, 0]),
            pltpu.make_async_copy(preb.at[slot], pre_hbm.at[pl.ds(pl.multiple_of(first + 8, 8), GB)], osem.at[slot, 1]),
            pltpu.make_async_copy(normedb.at[slot], normed_hbm.at[here], osem.at[slot, 2]),
            pltpu.make_async_copy(gatedb.at[slot], gated_hbm.at[here], osem.at[slot, 3]),
        ]

    head = at.s // rep
    state[...] = jnp.zeros_like(state)
    buf[0:8] = jnp.zeros((8, 640), F32)
    gains[...] = jnp.transpose(columns(768, 896).astype(F32))[0:8]
    taps = head_taps(taps_ref, head, heads)
    hg = hg_ref[...].astype(F32)
    rows = SeqSum(at, part, got, out, far, (ps, pr, qs, qr))
    line = SeqGather(at, feed_hbm, feed_out, fs, fr)
    line.start()
    mine = pltpu.make_async_copy(cot, cot_out.at[at.b], lsem.at[0])
    mine.start()
    edge = pltpu.make_async_copy(zero, pre_hbm.at[0:8], lsem.at[1])
    edge.start()
    cots = BatchGather(at, cot, cot_out.at[at.b], cs, cr)
    cots.start()

    def step(i, _):
        first = i * GB
        slot = lax.rem(i, 2)

        @pl.when(i >= 2)
        def _():
            for copy in saves(i - 2):
                copy.wait()

        def keep_map(kind, s, value):
            row = SPAN_ROWS * s + 128 * kind
            save[slot, row : row + value.shape[0]] = value

        def keep_rows(kind, value):
            row = SPAN_ROWS * GS + GB * kind
            save[slot, row : row + GB] = value

        x = hid_ref[pl.ds(2 * i, 2)].reshape(GB, -1).astype(F32)
        normed = (x * norm_rows(x) * gains[3:4]).astype(BF16)
        normedb[slot] = normed
        proj = mm(normed, columns(0, 896))
        pre = proj[:, 0:640].astype(BF16).astype(F32)
        preb[slot] = pre
        gl, sm = proj[:, 640:768], proj[:, 768:896]
        keep_rows(0, gl)
        keep_rows(1, sm)
        buf[8 : 8 + GB] = pre
        mix = conv_mix(buf, taps)
        buf[0:8] = pre[GB - 8 : GB]
        act = mix * jax.nn.sigmoid(mix)
        q = unit(act[:, 0:128])[0] * DK ** (-0.5)
        k0, k1 = unit(act[:, 128:256])[0], unit(act[:, 256:384])[0]
        v0, v1 = act[:, 384:512], act[:, 512:640]
        keep = (first + iota((GB, 1), 0) < len_ref[0]).astype(F32)
        sig0, sig1, al = gates(sm, dbias_ref[head])
        b0, b1 = lane(sig0 * keep), lane(sig1 * keep)
        eg = jnp.exp(jnp.full((1, 1), dlog_ref[head], F32))
        g = lane(-eg * softplus(al) * keep)
        strict, base, levels = sub_masks()
        eye = (iota((128, 128), 0) == iota((128, 128), 1)).astype(F32)
        tri = (iota((64, 64), 0) >= iota((64, 64), 1)).astype(F32)
        causal = iota((64, 128), 0) >= (iota((64, 128), 1) & 63)
        K, Q, V, B, C, N, PM, Kc = [], [], [], [], [], [], [], []
        for s in range(GS):
            sl = slice(64 * s, 64 * s + 64)
            K.append(jnp.concatenate([k0[sl], k1[sl]], axis=0))
            V.append(jnp.concatenate([v0[sl], v1[sl]], axis=0))
            B.append(jnp.concatenate([b0[sl], b1[sl]], axis=0))
            Q.append(q[sl])
            c, e = span_decay(g[sl], tri)
            C.append(c)
            ee = jnp.concatenate([e, e], axis=0)
            gram = mm3(jnp.concatenate([K[s], Q[s]], axis=0), K[s], NT)
            N.append(jnp.where(strict, gram[:128] * ee, 0.0) * B[s])
            PM.append(jnp.where(causal, gram[128:] * e, 0.0))
            cc = jnp.concatenate([c, c], axis=0)
            Kc.append(jnp.exp(cc[63:64] - cc) * K[s])
            keep_map(3, s, N[s])
            keep_map(5, s, PM[s])
        n1 = [jnp.where(base, n, 0.0) for n in N]
        n1s = [split(n) for n in n1]
        n2 = [mm3(a, a) for a in n1s]
        n2s = [split(n) for n in n2]
        n3 = [mm3(a, b) for a, b in zip(n1s, n2s)]
        n4 = [mm3(a, a) for a in n2s]
        y = [eye - a + b - c for a, b, c in zip(n1, n2, n3)]
        X = [a + mm3(a, b) for a, b in zip(y, n4)]
        for lv in levels:
            xs = [split(x_) for x_ in X]
            bl = [jnp.where(lv, n, 0.0) for n in N]
            xb = [mm3(a, b) for a, b in zip(xs, bl)]
            X = [x_ - mm3(a, b) for x_, a, b in zip(X, xb, xs)]
        pl.when(i > 0)(lambda: rows.flush(i - 1))
        for t in range(1, steps // 2):
            pl.when(i == 2 * t)(lambda: line.forward(t))
        W, U = [], []
        for s in range(GS):
            cc = jnp.concatenate([C[s], C[s]], axis=0)
            rhs = jnp.concatenate([B[s] * jnp.exp(cc) * K[s], B[s] * V[s]], axis=1)
            wu = mm3(X[s], rhs)
            W.append(wu[:, :128])
            U.append(wu[:, 128:])
            keep_map(0, s, X[s])
            keep_map(1, s, W[s])
        S = state[...]
        raw = []
        Ws = [split(a) for a in W]
        Kcs = [split(a) for a in Kc]
        for s in range(GS):
            keep_map(4, s, S)
            ss = split(S)
            vn = U[s] - mm3(Ws[s], ss)
            keep_map(2, s, vn)
            vs = split(vn)
            raw.append(jnp.exp(C[s]) * mm3(Q[s], ss) + mm3(PM[s], vs))
            S = jnp.exp(C[s][63:64]) * S + mm3(Kcs[s], vs, TN)
        state[...] = S
        o = jnp.concatenate(raw, axis=0)
        keep_rows(2, o)
        gated = (o * norm_rows(o) * hg * (gl * jax.nn.sigmoid(gl))).astype(BF16)
        gatedb[slot] = gated
        for copy in saves(i):
            copy.start()
        if rep > 1:
            gated = jnp.where(lax.rem(at.s, rep) == 0, gated, jnp.zeros_like(gated))
        part[i] = mm(gated, columns(896, 1024), NT).astype(BF16).reshape(2, GB // 2, -1)
        rows.start(i)
        return 0

    lax.fori_loop(0, steps, step, 0)
    rows.flush(steps - 1)
    total = rows.finish() + hid_ref[at.s].astype(F32)
    after[...] = total
    nm[...] = (total * norm_rows(total) * gains[4:5]).astype(BF16)
    mids = BatchGather(at, nm, nm_out.at[at.b], ms, mr)
    mids.start()
    own = pltpu.make_async_copy(nm, nm_out.at[at.b], lsem.at[2])
    own.start()
    for t in range(steps // 2, steps):
        line.forward(t)
    rows.drain()
    line.finish()
    for i in (steps - 2, steps - 1):
        for copy in saves(i):
            copy.wait()
    cots.finish()
    mids.finish()
    mine.wait()
    edge.wait()
    weights_out.wait()
    own.wait()


def feed_part(
    at,
    nm_hbm, cot_hbm, ff_hbm, mine_hbm, after, gains,
    block_out, d_stream, dbr_out, gfeed, sums,
    nm_all, cot_all, ff, acts, dgs, dus, pmid, pout, got_m, got_o, gbuf, gdown,
    isem, lsem, ms, mr, os_, or_, gs, gr, ds_s, dr_s, then=lambda: None,
):
    ns, nb = at.ns, at.nb
    loads = fetch([(nm_hbm, nm_all), (cot_hbm, cot_all)], isem)
    piece = mine_hbm.shape[1]

    def weights(i, src):
        return pltpu.make_async_copy(src, ff.at[:, piece * i : piece * (i + 1)], isem.at[2 + i])

    for i in range(ns):
        pl.when(i == at.s)(lambda: weights(i, mine_hbm).start())
        pl.when(i != at.s)(lambda: weights(i, ff_hbm.at[i]).start())
    for copy in loads:
        copy.wait()
    for i in range(ns):
        weights(i, mine_hbm).wait()
    tok = after.shape[0]
    share = ff.shape[2]
    enter(at)

    def mid_copy(m):
        to = at.peer(m)
        return send(pmid.at[to], got_m.at[m], ms.at[m], mr.at[m], {"batch": to})

    def out_copy(m):
        to = at.peer(m)
        return send(pout.at[to], got_o.at[m], os_.at[m], or_.at[m], {"batch": to})

    def both(ref, one, two):
        return jnp.concatenate([ref[one], ref[two]], axis=0)

    def pair(j, _):
        m = nb - 1 - 2 * j
        one, two = at.peer(m), at.peer(m - 1)
        x, d = both(nm_all, one, two), both(cot_all, one, two)
        ga, ua, da = mm(x, ff[0]), mm(x, ff[1]), mm(d, ff[2])
        sig = jax.nn.sigmoid(ga)
        act = (ga * sig * ua).astype(BF16)
        dg = (da * ua * sig * (1.0 + ga * (1.0 - sig))).astype(BF16)
        du = (da * ga * sig).astype(BF16)
        for ref, value in ((acts, act), (dgs, dg), (dus, du)):
            ref[one] = value[:tok]
            ref[two] = value[tok:]
        p = (mm(dg, ff[0], NT) + mm(du, ff[1], NT)).astype(BF16)
        pmid[one] = p[:tok]
        pmid[two] = p[tok:]
        mid_copy(m).start()
        pl.when(m > 1)(lambda: mid_copy(m - 1).start())
        return 0

    lax.fori_loop(0, nb // 2, pair, 0)

    def outs(j, _):
        m = nb - 1 - 2 * j
        one, two = at.peer(m), at.peer(m - 1)
        p = mm(both(acts, one, two), ff[2], NT).astype(BF16)
        pout[one] = p[:tok]
        pout[two] = p[tok:]
        out_copy(m).start()
        pl.when(m > 1)(lambda: out_copy(m - 1).start())
        return 0

    lax.fori_loop(0, nb // 2, outs, 0)
    x = after[...]
    d_mid = pmid[at.b].astype(F32)
    for m in at.peers():
        mid_copy(m).wait_recv()
        d_mid = d_mid + got_m[m].astype(F32)
    r = norm_rows(x)
    y = x * r
    gfeed[...] = jnp.sum(d_mid * y, axis=0, keepdims=True)
    dy = d_mid * gains[4:5]
    ds_ = cot_all[at.b].astype(F32) + r * (dy - y * jnp.mean(dy * y, axis=-1, keepdims=True))
    d_stream[...] = ds_
    dbr_out[at.s] = ds_.astype(BF16)
    line = SeqGather(at, dbr_out.at[at.s], dbr_out, gs, gr)
    line.start()
    halves = ns // nb
    deep, cols = share // halves, nm_all.shape[2] // ns
    flat = lambda ref: ref[...].reshape(nb * tok, -1)
    g = mm(flat(acts), flat(cot_all), TN).astype(BF16)
    for b in range(nb):
        for h in range(halves):
            for t in range(halves):
                gdown[b, h, deep * t : deep * (t + 1)] = g[
                    deep * h : deep * (h + 1), cols * (halves * b + t) : cols * (halves * b + t + 1)
                ]
    down = lambda b, h: sums.at[halves * b + h, pl.ds(2 * share, share)]
    moved = [
        send(gdown.at[at.peer(m), h], down(at.b, h), ds_s.at[m, h], dr_s.at[m, h], {"batch": at.peer(m)})
        for m in at.peers()
        for h in range(halves)
    ]
    for copy in moved:
        copy.start()
    kept = [
        pltpu.make_async_copy(gdown.at[at.b, h], down(at.b, h), lsem.at[1 + h]) for h in range(halves)
    ]
    line.forward(1)
    for k, left in enumerate((dgs, dus)):
        g = mm(flat(left), flat(nm_all), TN).astype(BF16)
        for i in range(ns):
            gbuf[k, i] = g[:, cols * i : cols * (i + 1)]
        kept.append(
            pltpu.make_async_copy(gbuf.at[k], sums.at[:, pl.ds(share * k, share)], lsem.at[1 + halves + k])
        )
        if k == 0:
            line.forward(2)
    for copy in kept:
        copy.start()
    for copy in moved + kept:
        copy.wait()
    then()
    for t in range(3, at.nz):
        line.forward(t)
    total = after[...] + pout[at.b].astype(F32)
    for m in at.peers():
        out_copy(m).wait_recv()
        total = total + got_o[m].astype(F32)
    block_out[...] = total.astype(BF16)
    line.finish()
    for m in at.peers():
        mid_copy(m).wait_send()
        out_copy(m).wait_send()


def feed_kernel(ns, nb, *refs):
    at = Place(ns, nb)
    greet(at)
    feed_part(at, *refs)


FEED_SCRATCH = 24


def back_kernel(
    ns, nb, rep, heads, merged,
    len_ref, dlog_ref, dbias_ref, w_hbm, taps_hbm, hg_ref, normed_hbm, pre_hbm, gated_hbm, save_hbm,
    hid_hbm, gains, *refs,
):
    at = Place(ns, nb)
    greet(at)
    if merged:
        nm_hbm, cot_hbm, ff_hbm, mine_hbm, after, block_out, sums, *refs = refs
        outs, refs = refs[:6], refs[6:]
        *feed_refs, d_stream, gfeed = refs[:FEED_SCRATCH]
        refs = refs[FEED_SCRATCH:]
    else:
        dbr_hbm, sums, d_stream, gfeed, *refs = refs
        outs, refs = refs[:6], refs[6:]
    grad_in, q_slots, k_slots, gout_sum, small_all, feed_sum = outs
    (
        dbr_ref, w_ref, taps_ref, hid, save, buf, normedb, gatedb, isem, bsem,
        dbuf, dstate, small, gw, go, part, got, out, far, grads, gout, got_g, piece, got_o, got_s,
        f_own, f_got, f_up, f_down,
        ready, ps, pr, qs, qr, gs, gr, bs, br, kr, os_, or_, ss, sr, us, ur, fi, fps, fpr, fus, fur, fds, fdr,
    ) = refs
    steps = at.nz
    loads = fetch([(w_hbm, w_ref), (taps_hbm, taps_ref), (hid_hbm, hid)], isem)

    def block_in(i):
        slot = lax.rem(i, 2)
        first = pl.multiple_of(i * GB, GB)
        here = pl.ds(first, GB)
        return [
            pltpu.make_async_copy(save_hbm.at[i], save.at[slot], bsem.at[slot, 0]),
            pltpu.make_async_copy(pre_hbm.at[pl.ds(first, 8 + GB)], buf.at[slot], bsem.at[slot, 1]),
            pltpu.make_async_copy(normed_hbm.at[here], normedb.at[slot], bsem.at[slot, 2]),
            pltpu.make_async_copy(gated_hbm.at[here], gatedb.at[slot], bsem.at[slot, 3]),
        ]

    for copy in block_in(steps - 1):
        copy.start()
    for copy in loads:
        copy.wait()
    head = at.s // rep
    dstate[...] = jnp.zeros_like(dstate)
    dbuf[GB : GB + 8] = jnp.zeros((8, 640), F32)
    small[...] = jnp.zeros_like(small)
    gw[...] = jnp.zeros_like(gw)
    go[...] = jnp.zeros_like(go)
    taps = head_taps(taps_ref, head, heads)
    hg = hg_ref[...].astype(F32)
    rows = SeqSum(at, part, got, out, far, (ps, pr, qs, qr))
    feed = LineSum(at, sums, f_own, f_got, f_up, f_down, (fi, fps, fpr, fus, fur, fds, fdr))

    def begin_sums():
        feed.load()
        feed.start()

    if merged:
        feed_part(
            at, nm_hbm, cot_hbm, ff_hbm, mine_hbm, after, gains, block_out, d_stream, dbr_ref, gfeed, sums,
            *feed_refs, begin_sums,
        )
    else:
        rows_in = pltpu.make_async_copy(dbr_hbm, dbr_ref, isem.at[3])
        rows_in.start()
        enter(at)
        begin_sums()
        rows_in.wait()
    feed.begin()
    for ds in range(1, ns):
        pl.semaphore_signal(ready, inc=1, device_id={"seq": at.seq_at(ds)}, device_id_type=MESH)

    when = {f: f + (2 if f == 1 else 3) for f in range(1, feed.turns() + 1)}

    def turn(j, half):
        for f, h in when.items():
            if h < 2 * steps and h % 2 == half:
                pl.when(j == h // 2)(lambda: feed.relay(f))

    def step(j, _):
        i = steps - 1 - j
        first = i * GB
        slot = lax.rem(i, 2)

        @pl.when(i > 0)
        def _():
            for copy in block_in(i - 1):
                copy.start()

        def kept_map(kind, s, high=128):
            row = SPAN_ROWS * s + 128 * kind
            return save[slot, row : row + high]

        def kept_rows(kind):
            row = SPAN_ROWS * GS + GB * kind
            return save[slot, row : row + GB]

        for copy in block_in(i):
            copy.wait()
        dbr = dbr_ref[pl.ds(2 * i, 2)].reshape(GB, -1)
        d_gated = mm(dbr, w_ref[:, 896:1024])
        gl, sm, o = kept_rows(0), kept_rows(1), kept_rows(2)
        sg = jax.nn.sigmoid(gl)
        rr = norm_rows(o)
        yn = o * rr
        dn = d_gated * (gl * sg)
        d_gl = d_gated * (yn * hg) * (sg * (1.0 + gl * (1.0 - sg)))
        dy = dn * hg
        d_raw = rr * (dy - yn * jnp.mean(yn * dy, axis=-1, keepdims=True))
        go[...] += mm(gatedb[slot], dbr, TN)

        mix = conv_mix(buf.at[slot], taps)
        sig = jax.nn.sigmoid(mix)
        act = mix * sig
        qn, rq = unit(act[:, 0:128])
        k0, r0 = unit(act[:, 128:256])
        k1, r1 = unit(act[:, 256:384])
        v0, v1 = act[:, 384:512], act[:, 512:640]
        q = qn * DK ** (-0.5)
        keep = (first + iota((GB, 1), 0) < len_ref[0]).astype(F32)
        sig0, sig1, al = gates(sm, dbias_ref[head])
        eg = jnp.exp(jnp.full((1, 1), dlog_ref[head], F32))
        g1 = -eg * softplus(al) * keep
        g = lane(g1)
        b0, b1 = lane(sig0 * keep), lane(sig1 * keep)
        strict, _, _ = sub_masks()
        tri = (iota((64, 64), 0) >= iota((64, 64), 1)).astype(F32)
        trit = (iota((64, 64), 0) <= iota((64, 64), 1)).astype(F32)
        causal = iota((64, 128), 0) >= (iota((64, 128), 1) & 63)
        K, Q, V, B, C, E, Kc, A1, A2, DO = [], [], [], [], [], [], [], [], [], []
        for s in range(GS):
            sl = slice(64 * s, 64 * s + 64)
            K.append(jnp.concatenate([k0[sl], k1[sl]], axis=0))
            V.append(jnp.concatenate([v0[sl], v1[sl]], axis=0))
            B.append(jnp.concatenate([b0[sl], b1[sl]], axis=0))
            Q.append(q[sl])
            c, e = span_decay(g[sl], tri)
            C.append(c)
            E.append(e)
            cc = jnp.concatenate([c, c], axis=0)
            Kc.append(jnp.exp(cc[63:64] - cc) * K[s])
            do = d_raw[sl]
            DO.append(do)
            A1.append(mm3(kept_map(5, s, HALF), do, TN))
            A2.append(mm3(jnp.exp(c) * Q[s], do, TN))
        dS = dstate[...]
        DV, DS = [None] * GS, [None] * GS
        for s in reversed(range(GS)):
            DS[s] = dS
            dvn = A1[s] + mm3(Kc[s], dS)
            DV[s] = dvn
            dS = jnp.exp(C[s][63:64]) * dS + A2[s] - mm3(kept_map(1, s), dvn, TN)
        dstate[...] = dS
        pl.when(j > 0)(lambda: rows.flush(i + 1))

        turn(j, 0)
        dq_l, dk0_l, dk1_l, dv0_l, dv1_l, db0_l, db1_l, dg_l = [], [], [], [], [], [], [], []
        for s in range(GS):
            vn, sst, n, p = kept_map(2, s), kept_map(4, s), kept_map(3, s), kept_map(5, s, HALF)
            vns = split(vn)
            ks = split(K[s])
            cc = jnp.concatenate([C[s], C[s]], axis=0)
            ec = jnp.exp(cc)
            ee = jnp.concatenate([E[s], E[s]], axis=0)
            dr = mm3(kept_map(0, s), DV[s], TN)
            both = split(jnp.concatenate([dr, DO[s]], axis=0))
            dd = mm3(both, vns, NT)
            dN = jnp.where(strict, -dd[:128], 0.0)
            dP = jnp.where(causal, dd[128:], 0.0)
            h = mm3(both, sst, NT)
            hk, hq = h[:128], h[128:]
            fh = dP * E[s]
            dq = ec[:64] * hq + mm3(fh, ks)
            dne = dN * ee
            dgm = dne * B[s]
            dkc = mm3(vns, DS[s], NT)
            ekc = jnp.exp(cc[63:64] - cc)
            dk = ekc * dkc - B[s] * ec * hk + mm3(fh, Q[s], TN) + mm3(dgm + jnp.transpose(dgm), ks)
            khk = jnp.sum(K[s] * hk, axis=-1, keepdims=True)
            ecl = ec[:, 0:1]
            db = (
                jnp.sum(dr * V[s], axis=-1, keepdims=True)
                - ecl * khk
                + jnp.sum(dne * mm3(ks, ks, NT), axis=-1, keepdims=True)
            )
            e1 = dN * n
            f1 = dP * p
            z = e1[:64, :64] + e1[:64, 64:] + e1[64:, :64] + e1[64:, 64:] + f1[:, :64] + f1[:, 64:]
            dc = jnp.sum(z - jnp.transpose(z), axis=-1, keepdims=True)
            dks = -B[s][:, 0:1] * ecl * khk
            hj = jnp.sum(Kc[s] * dkc, axis=-1, keepdims=True)
            dc = dc + dks[:64] + dks[64:] - hj[:64] - hj[64:]
            dc = dc + ec[:64, 0:1] * jnp.sum(Q[s] * hq, axis=-1, keepdims=True)
            dcl = jnp.sum(hj, axis=0, keepdims=True) + ec[63:64, 0:1] * jnp.sum(
                jnp.sum(sst * DS[s], axis=-1, keepdims=True), axis=0, keepdims=True
            )
            dg = mm3(trit, lane(dc)) + dcl
            dg_l.append(dg[:, 0:1])
            dq_l.append(dq)
            dk0_l.append(dk[:64])
            dk1_l.append(dk[64:])
            dv = B[s] * dr
            dv0_l.append(dv[:64])
            dv1_l.append(dv[64:])
            db0_l.append(db[:64])
            db1_l.append(db[64:])
        turn(j, 1)
        cat = lambda parts: jnp.concatenate(parts, axis=0)
        dq, dk0, dk1, dv0, dv1 = cat(dq_l), cat(dk0_l), cat(dk1_l), cat(dv0_l), cat(dv1_l)
        db0, db1, dg = cat(db0_l), cat(db1_l), cat(dg_l)

        def unit_back(d, n, rn):
            return rn * (d - n * jnp.sum(d * n, axis=-1, keepdims=True))

        d_act = jnp.concatenate(
            [unit_back(dq * DK ** (-0.5), qn, rq), unit_back(dk0, k0, r0), unit_back(dk1, k1, r1), dv0, dv1],
            axis=1,
        )
        d_mix = d_act * (sig * (1.0 + mix * (1.0 - sig)))
        for t in range(4):
            small[t : t + 1, 0:640] += jnp.sum(d_mix * buf[slot, 5 + t : 5 + t + GB], axis=0, keepdims=True)
        dbuf[0:GB] = d_mix
        d_pre = taps[3:4] * d_mix
        for t in range(3):
            d_pre = d_pre + taps[t : t + 1] * dbuf[3 - t : 3 - t + GB]
        dbuf[GB : GB + 8] = d_mix[0:8]
        d_al = -dg * eg * jax.nn.sigmoid(al) * keep
        d_b0 = db0 * keep * sig0 * (1.0 - sig0)
        d_b1 = db1 * keep * sig1 * (1.0 - sig1)
        lanes = iota((GB, 128), 1)
        d_sm = jnp.where(
            lanes == 0, d_b0, jnp.where(lanes == 1, d_b1, jnp.where(lanes == 2, d_al, 0.0))
        )
        small[0:1, 640:768] += jnp.sum(dn * yn, axis=0, keepdims=True)
        small[1:2, 640:768] += jnp.broadcast_to(jnp.sum(dg * g1, axis=0, keepdims=True), (1, 128))
        small[2:3, 640:768] += jnp.broadcast_to(jnp.sum(d_al, axis=0, keepdims=True), (1, 128))
        dall = jnp.concatenate([d_pre.astype(BF16), d_gl.astype(BF16), d_sm.astype(BF16)], axis=1)
        gw[...] += mm(normedb[slot], dall, TN)
        if rep > 1:
            dall = jnp.where(lax.rem(at.s, rep) == 0, dall, jnp.zeros_like(dall))
        d_normed = mm(dall, w_ref[:, 0:896], NT)
        part[i] = d_normed.astype(BF16).reshape(2, GB // 2, -1)
        rows.start(i)
        small[7:8] += jnp.sum(d_normed * normedb[slot].astype(F32), axis=0, keepdims=True)
        return 0

    lax.fori_loop(0, steps, step, 0)

    small[4:7] = jnp.transpose(gw[:, 768:896])[0:3]
    small[7:8] = small[7:8] / gains[3:4]
    fourth = small.shape[1] // 4
    for k in range(4):
        small[k : k + 1, 3 * fourth :] = gfeed[:, fourth * k : fourth * (k + 1)]
    smalls = [send(small, got_s.at[m], ss.at[m], sr.at[m], {"batch": at.peer(m)}) for m in at.peers()]
    for copy in smalls:
        copy.start()
    nq = q_slots.shape[0]
    part_rows, width = grads.shape[2], q_slots.shape[4]
    grads[...] = gw[:, 0:768].astype(BF16).reshape(ns, nb, part_rows, 768)
    over = [
        send(grads.at[:, at.peer(m)], got_g.at[m], gs.at[m], gr.at[m], {"batch": at.peer(m)}) for m in at.peers()
    ]
    for copy in over:
        copy.start()
    rows.flush(0)
    for f, h in when.items():
        if h >= 2 * steps:
            feed.relay(f)
    high, wide = gout.shape[1:]
    for b in range(nb):
        block = go[:, wide * b : wide * (b + 1)].astype(BF16)
        if rep > 1:
            block = jnp.where(lax.rem(at.s, rep) == 0, block[:high], block[high:])
        gout[b] = block
    outs = [send(gout.at[at.peer(m)], got_o.at[m], os_.at[m], or_.at[m], {"batch": at.peer(m)}) for m in at.peers()]
    for copy in outs:
        copy.start()
    total = small[...]
    for m, copy in zip(at.peers(), smalls):
        copy.wait_recv()
        total = total + got_s[m]
    small_all[at.s] = total
    heads_ = [
        send(small_all.at[at.s], small_all.at[at.s], us.at[ds], ur.at[ds], {"seq": at.seq_at(ds)})
        for ds in range(1, ns)
    ]
    for copy in heads_:
        copy.start()
    for copy in over:
        copy.wait_recv()
    pl.semaphore_wait(ready, ns - 1)
    acc = grads[:, at.b].astype(F32)
    for m in at.peers():
        acc = acc + got_g[m].astype(F32)
    for g, mats in enumerate(((0, 5), (1, 3), (2, 4))):
        for n, m in enumerate(mats):
            block = acc[:, :, 128 * m : 128 * m + 128]
            if rep > 1:
                block = jnp.where(lax.rem(at.s, rep) == 0, block[:, :, :width], block[:, :, width:])
            piece[g, :, n] = block.astype(BF16)
    placed = []
    for g in range(3):
        unit_at = at.s if g < 2 else ns + at.s
        dst, count, dst_sem = (q_slots, nq, br) if g == 0 else (k_slots, 2 * nq, kr)
        owner, slot = unit_at // count, lax.rem(unit_at, count)
        for row in range(ns):
            placed.append((g, row, owner, dst.at[slot, :, at.b], dst_sem.at[slot, at.b]))

    def place(item):
        g, row, owner, dst, sem = item
        src = piece.at[g, row]
        here = jnp.logical_and(row == at.s, owner == at.b)
        far_copy = lambda: send(src, dst, bs.at[g, row], sem, {"seq": row, "batch": owner})
        near_copy = lambda: pltpu.make_async_copy(src, dst, sem)
        return here, far_copy, near_copy

    for item in placed:
        here, far_copy, near_copy = place(item)
        pl.when(here)(lambda: near_copy().start())
        pl.when(jnp.logical_not(here))(lambda: far_copy().start())

    d_normed = rows.finish()
    x = hid[...].astype(F32)
    r = norm_rows(x)
    y = x * r
    dy = d_normed * gains[3:4]
    grad_in[...] = (d_stream[...] + r * (dy - y * jnp.mean(dy * y, axis=-1, keepdims=True))).astype(BF16)
    acc = gout[at.b].astype(F32)
    for m, copy in zip(at.peers(), outs):
        copy.wait_recv()
        acc = acc + got_o[m].astype(F32)
    gout_sum[...] = acc
    for copy in heads_:
        copy.wait_recv()
    for item in placed:
        here, far_copy, _ = place(item)
        pl.when(jnp.logical_not(here))(lambda: far_copy().wait_send())
    for dst, sem in ((q_slots, br), (k_slots, kr)):
        for slot in range(dst.shape[0]):
            for b in range(nb):
                pltpu.make_async_copy(piece.at[0, 0], dst.at[slot, :, b], sem.at[slot, b]).wait()
    for copy in smalls + over + outs + heads_:
        copy.wait_send()
    feed.finish(feed_sum)
    feed.drain()
    rows.drain()


class LineSum:
    def __init__(self, at, part, own, got, ups, downs, sems):
        self.at, self.part, self.own, self.got = at, part, own, got
        self.line = (ups, downs)
        self.isem, self.pair_s, self.pair_r, self.sems = sems[0], sems[1], sems[2], sems[3:]

    def mine(self, i):
        return pltpu.make_async_copy(self.part.at[2 * i + self.at.c], self.own.at[i], self.isem.at[i])

    def pair(self, i):
        at = self.at
        return send(self.part.at[2 * i + 1 - at.c], self.got.at[i], self.pair_s.at[i], self.pair_r.at[i], {"seq": at.sib})

    def hop(self, i, up, src=None):
        buf, k = self.line[0 if up else 1], 0 if up else 2
        return send(
            buf.at[i] if src is None else src, buf.at[i], self.sems[k].at[i], self.sems[k + 1].at[i],
            {"seq": self.at.s + 2 if up else self.at.s - 2},
        )

    def load(self):
        for i in range(self.at.nz):
            self.mine(i).start()

    def start(self):
        for i in range(self.at.nz):
            self.pair(i).start()

    def begin(self):
        at, nz = self.at, self.at.nz
        for i in range(nz):
            self.mine(i).wait()
            self.pair(i).wait_recv()
            self.own[i] = (self.own[i].astype(F32) + self.got[i].astype(F32)).astype(BF16)
        for k in range(nz - 1):
            pl.when(at.z == 0)(lambda: self.hop(nz - 1 - k, True, self.own.at[nz - 1 - k]).start())
            pl.when(at.z == nz - 1)(lambda: self.hop(k, False, self.own.at[k]).start())

    def relay(self, f):
        at, nz = self.at, self.at.nz
        for a in range(1, nz - 1):
            k = f - (2 * a - 1)
            if not 0 <= k < nz - 1 - a:
                continue

            @pl.when(at.z == a)
            def _():
                self.pass_on(nz - 1 - k, True)

            @pl.when(at.z == nz - 1 - a)
            def _():
                self.pass_on(k, False)

    def turns(self):
        nz = self.at.nz
        return max(2 * a - 1 + nz - 2 - a for a in range(1, nz - 1)) if nz > 2 else 0

    def pass_on(self, i, up):
        buf = self.line[0 if up else 1]
        self.hop(i, up).wait_recv()
        buf[i] = (buf[i].astype(F32) + self.own[i].astype(F32)).astype(BF16)
        self.hop(i, up).start()

    def finish(self, out):
        at = self.at
        out[...] = self.own[at.z].astype(F32)
        for up in (True, False):

            @pl.when(at.z > 0 if up else at.z < at.nz - 1)
            def _():
                self.hop(at.z, up).wait_recv()
                out[...] += self.line[0 if up else 1][at.z].astype(F32)

    def drain(self):
        at, nz = self.at, self.at.nz
        for i in range(nz):
            self.pair(i).wait_send()
            pl.when(i > at.z)(lambda: self.hop(i, True).wait_send())
            pl.when(i < at.z)(lambda: self.hop(i, False).wait_send())


def finish_kernel(
    rep, heads, share, halves,
    block_in, grad_in_, q_in, k_in, gout_in, small_in, feed_in,
    o_block, o_grad, o_gain, o_q, o_k, o_v, o_beta, o_alpha, o_gate, o_out, o_mid, o_fg, o_fu, o_fd, o_taps, o_log,
    o_bias, o_hg,
    block, grad, q_slots, k_slots, gout, small, feed, gq, gk, gv, gg, fd, taps, vec_a, vec_b, dlog, dbias,
    hgain, stack, isem, osem,
):
    loads = fetch(
        [
            (q_in, q_slots), (feed_in, feed), (small_in, small), (block_in, block), (grad_in_, grad),
            (gout_in, gout), (k_in, k_slots),
        ],
        isem,
    )
    outs = []

    def put(src, dst):
        copy = pltpu.make_async_copy(src, dst, osem.at[len(outs)])
        copy.start()
        outs.append(copy)

    loads[0].wait()
    loads[6].wait()
    cw = q_slots.shape[4]
    for ref, slots, n in ((gq, q_slots, 0), (gg, q_slots, 1), (gk, k_slots, 0), (gv, k_slots, 1)):
        for k in range(slots.shape[0]):
            ref[:, cw * k : cw * (k + 1)] = slots[k, n].astype(F32).reshape(ref.shape[0], cw)
    for src, dst in ((gq, o_q), (gk, o_k), (gv, o_v), (gg, o_gate)):
        put(src, dst)
    loads[1].wait()
    deep, cols = share // halves, feed.shape[1]
    for t in range(halves):
        fd[:, cols * t : cols * (t + 1)] = feed[2 * share + deep * t : 2 * share + deep * (t + 1)]
    for src, dst in ((feed.at[0:share], o_fg), (feed.at[share : 2 * share], o_fu), (fd, o_fd)):
        put(src, dst)
    loads[2].wait()
    lanes = iota((1, heads), 1)
    log_row, bias_row, gain_row = jnp.zeros((1, heads), F32), jnp.zeros((1, heads), F32), jnp.zeros((1, DK), F32)
    for h in range(heads):
        at = small.at[rep * h]
        for j in range(3):
            stack[j * heads + h : j * heads + h + 1] = at[4 + j : 5 + j]
        for g in range(5):
            col = DK * (heads * g + h)
            taps[:, col : col + DK] = at[0:4, DK * g : DK * (g + 1)]
        gain_row = gain_row + at[0:1, 5 * DK : 6 * DK]
        log_row = jnp.where(lanes == h, at[1:2, 5 * DK : 5 * DK + 1], log_row)
        bias_row = jnp.where(lanes == h, at[2:3, 5 * DK : 5 * DK + 1], bias_row)
    hgain[...] = gain_row
    dlog[...] = log_row
    dbias[...] = bias_row
    for src, dst in ((stack.at[: 2 * heads], o_beta), (stack.at[2 * heads :], o_alpha), (taps, o_taps), (hgain, o_hg), (dlog, o_log), (dbias, o_bias)):
        put(src, dst)
    every = small[0]
    for k in range(1, small.shape[0]):
        every = every + small[k]
    vec_a[...] = every[7:8]
    fourth = every.shape[1] // 4
    for k in range(4):
        vec_b[:, fourth * k : fourth * (k + 1)] = every[k : k + 1, 3 * fourth :]
    put(vec_a, o_gain)
    put(vec_b, o_mid)
    for copy, src, dst in ((loads[3], block, o_block), (loads[4], grad, o_grad), (loads[5], gout, o_out)):
        copy.wait()
        put(src, dst)
    for copy in outs:
        copy.wait()


def comm_call(kernel, outs, scratch, ident, name, args, specs, limit):
    return pl.pallas_call(
        kernel,
        in_specs=specs,
        out_specs=[o[1] for o in outs],
        out_shape=[o[0] for o in outs],
        scratch_shapes=scratch,
        compiler_params=pltpu.CompilerParams(
            collective_id=ident, has_side_effects=True, vmem_limit_bytes=limit * 1024 * 1024
        ),
        name=name,
    )(*args)


def dma(*shape):
    return pltpu.SemaphoreType.DMA(shape)


def on_device(
    hidden_in, cotangent, lengths, mixer_gain, query_weight, key_weight, value_weight, beta_weight, alpha_weight,
    gate_weight, out_weight, feed_gain, feed_gate, feed_up, feed_down, conv_taps, decay_log, decay_bias, head_gain,
):
    ns, nb = lax.axis_size("seq"), lax.axis_size("batch")
    heads = decay_log.shape[0]
    rep = ns // heads
    tok, width = hidden_in.shape[1:]
    assert hidden_in.shape[0] == 1 and ns == rep * heads and ns % nb == 0 and 2 * tok == GB
    rows = query_weight.shape[0]
    share = feed_gate.shape[1] // nb
    halves = ns // nb
    nz = ns // 2
    n = ns * tok
    sds = jax.ShapeDtypeStruct
    vmem, hbm = pl.BlockSpec(memory_space=pltpu.VMEM), pl.BlockSpec(memory_space=pltpu.HBM)
    smem = pl.BlockSpec(memory_space=pltpu.SMEM)
    hidden, cot = hidden_in[0], cotangent[0]
    buffer = lambda *shape: pltpu.VMEM(shape, BF16)
    block = lambda count: buffer(count, tok, width)
    wide = lambda *shape: pltpu.VMEM(shape, F32)
    vout = lambda kind, *shape: (sds(shape, kind), vmem)
    hout = lambda kind, *shape: (sds(shape, kind), hbm)
    key = heads * DK

    hg = head_gain[None]
    wm, ff, normed, pre, gated, save, gains, after, nm_all, cot_all, ff_all = comm_call(
        functools.partial(front_kernel, ns, nb, rep, heads),
        [
            hout(BF16, ns, nb, rows, 8 * DK), hout(BF16, 3, nb, rows, share),
            hout(BF16, n, width), hout(F32, n + 8, 5 * DK), hout(BF16, n, DK), hout(F32, nz, SAVE_ROWS, DK),
            vout(F32, 8, width), vout(F32, tok, width), hout(BF16, nb, tok, width), hout(BF16, nb, tok, width),
            hout(BF16, ns, 3, nb, rows, share),
        ],
        [
            buffer(tok, width), buffer(rows, key), buffer(rows, 2 * key), buffer(rows, 2 * key), buffer(rows, key),
            buffer(rows, key), buffer(rows, nb * share), buffer(rows, nb * share), buffer(rows, nb * share),
            buffer(heads, rows, 8 * DK), buffer(nb, 3, rows, share), dma(9), dma(3), dma(4 * nz), dma(4 * nz), dma(ns),
            dma(ns), dma(nz, nb), dma(nz, nb), dma(nb), dma(nb),
            block(ns), buffer(ns, nb, rows, 8 * DK), buffer(4, 5 * key), buffer(tok, width), buffer(tok, width),
            wide(8, 5 * DK), wide(2, SAVE_ROWS, DK), wide(2, GB, 5 * DK), buffer(2, GB, width), buffer(2, GB, DK),
            wide(8 + GB, 5 * DK), wide(DK, DK), buffer(nz, 2, tok, width), block(nz), block(nz), block(nz),
            dma(2), dma(1), dma(3), dma(2, 4), dma(nz), dma(nz), dma(nz), dma(nz), dma(nb), dma(nb), dma(nb), dma(nb),
            dma(4 * nz), dma(4 * nz),
        ],
        1, "front",
        (
            lengths, decay_log, decay_bias, conv_taps, hg, cot,
            hidden, query_weight, key_weight, value_weight, gate_weight, out_weight.T, beta_weight.T, alpha_weight.T,
            mixer_gain[None], feed_gain[None], feed_gate, feed_up, feed_down.T,
        ),
        [smem] * 3 + [hbm, vmem, hbm] + [hbm] * 6 + [vmem] * 4 + [hbm] * 3, 61,
    )
    wm = wm.reshape(width, 8 * DK)
    ff = ff.reshape(3, nb * rows, share)
    ff_all = ff_all.reshape(ns, 3, nb * rows, share)
    nq = ns // nb
    cw = DK // rep
    wrows = width // ns
    deep = 3 * share
    quarter = wrows // nb
    merged = nb <= 4
    feed_scratch = [
        block(nb), block(nb), buffer(3, width, share), buffer(nb, tok, share), buffer(nb, tok, share),
        buffer(nb, tok, share), block(nb), block(nb), block(nb), block(nb),
        buffer(2, ns, share, width // ns), buffer(nb, halves, share, width // ns),
        dma(2 + ns), dma(3 + halves), dma(nb), dma(nb), dma(nb), dma(nb), dma(4 * nz), dma(4 * nz), dma(nb, halves),
        dma(nb, halves),
    ]
    sums_out = hout(BF16, ns, deep, width // ns)
    back_in = [lengths, decay_log, decay_bias, wm, conv_taps, hg, normed, pre, gated, save, hidden, gains]
    back_specs = [smem] * 3 + [hbm] * 2 + [vmem] + [hbm] * 5 + [vmem]
    back_outs = [
        vout(BF16, tok, width), vout(BF16, nq, 2, nb, quarter, cw), vout(BF16, 2 * nq, 2, nb, quarter, cw),
        vout(F32, DK // rep, width // nb), vout(F32, ns, 8, width), vout(F32, deep, width // ns),
    ]
    if merged:
        back_in += [nm_all, cot_all, ff_all, ff, after]
        back_specs += [hbm] * 4 + [vmem]
        back_outs = [vout(BF16, tok, width), sums_out] + back_outs
        extra = feed_scratch + [wide(tok, width), wide(1, width)]
        assert len(extra) == FEED_SCRATCH
    else:
        block_out, d_stream, dbr_all, gfeed, sums = comm_call(
            functools.partial(feed_kernel, ns, nb),
            [
                vout(BF16, tok, width), vout(F32, tok, width), vout(BF16, ns, tok, width), vout(F32, 1, width),
                sums_out,
            ],
            feed_scratch, 2, "feed", (nm_all, cot_all, ff_all, ff, after, gains), [hbm] * 4 + [vmem] * 2, 55,
        )
        back_in += [dbr_all, sums, d_stream, gfeed]
        back_specs += [hbm] * 2 + [vmem] * 2
        extra = []
    outs = comm_call(
        functools.partial(back_kernel, ns, nb, rep, heads, merged),
        back_outs,
        extra + [
            block(ns), buffer(width, 8 * DK), buffer(4, 5 * key), buffer(tok, width),
            wide(2, SAVE_ROWS, DK), wide(2, 8 + GB, 5 * DK), buffer(2, GB, width), buffer(2, GB, DK), dma(4), dma(2, 4),
            wide(GB + 8, 5 * DK), wide(DK, DK), wide(8, width), wide(width, 7 * DK),
            wide(DK, width), buffer(nz, 2, tok, width), block(nz), block(nz), block(nz),
            buffer(ns, nb, quarter, 6 * DK), buffer(nb, DK // rep, width // nb), buffer(nb, ns, quarter, 6 * DK),
            buffer(3, ns, 2, quarter, cw), buffer(nb, DK // rep, width // nb), wide(nb, 8, width),
            *[buffer(nz, deep, width // ns)] * 4, pltpu.SemaphoreType.REGULAR,
            dma(nz), dma(nz), dma(nz), dma(nz), dma(nb), dma(nb), dma(3, ns), dma(nq, nb), dma(2 * nq, nb),
            dma(nb), dma(nb), dma(nb), dma(nb), dma(ns), dma(ns),
            *[dma(nz)] * 7,
        ],
        3, "back", back_in, back_specs, 61,
    )
    if merged:
        block_out, _, *outs = outs
    grad_in, q_slots, k_slots, gout_sum, small_all, feed_sum = outs
    shapes = [
        sds((tok, width), BF16), sds((tok, width), BF16), sds((1, width), F32), sds((wrows, nq * cw), F32),
        sds((wrows, 2 * nq * cw), F32), sds((wrows, 2 * nq * cw), F32), sds((2 * heads, width), F32),
        sds((heads, width), F32), sds((wrows, nq * cw), F32), sds((DK // rep, width // nb), F32), sds((1, width), F32),
        sds((share, wrows), F32), sds((share, wrows), F32), sds((share // halves, width // nb), F32),
        sds((4, 5 * key), F32), sds((1, heads), F32), sds((1, heads), F32), sds((1, DK), F32),
    ]
    like = lambda *which: [pltpu.VMEM(shapes[k].shape, shapes[k].dtype) for k in which]
    outs = list(pl.pallas_call(
        functools.partial(finish_kernel, rep, heads, share, halves),
        in_specs=[hbm] * 7,
        out_specs=[hbm] * len(shapes),
        out_shape=shapes,
        scratch_shapes=like(0, 1) + [buffer(nq, 2, nb, quarter, cw), buffer(2 * nq, 2, nb, quarter, cw)] + like(9) + [wide(ns, 8, width)]
        + [wide(deep, width // ns)] + like(3, 4, 5, 8, 13, 14, 2, 10, 15, 16, 17)
        + [wide(3 * heads, width), dma(7), dma(len(shapes))],
        compiler_params=pltpu.CompilerParams(vmem_limit_bytes=61 * 1024 * 1024),
        name="finish",
    )(block_out, grad_in, q_slots, k_slots, gout_sum, small_all, feed_sum))
    for k in (0, 1):
        outs[k] = outs[k][None]
    for k in (6, 7, 11, 12):
        outs[k] = outs[k].T
    for k in (2, 10, 15, 16, 17):
        outs[k] = outs[k][0]
    return tuple(outs)


def solution(mesh):
    both = ("seq", "batch")
    tokens, split_rows, grid = P("batch", "seq", None), P(both, None), P("seq", "batch")
    return jax.shard_map(
        on_device,
        mesh=mesh,
        in_specs=(
            tokens, tokens, P("batch"), P(both), split_rows, split_rows, split_rows, split_rows, split_rows,
            split_rows, P(None, both), P(both), split_rows, split_rows, P(None, both), P(), P(), P(), P(),
        ),
        out_specs=(
            tokens, tokens, P(), grid, grid, grid, P(), P(), grid, grid, P(), grid, grid, grid, P(), P(), P(), P(),
        ),
        check_vma=False,
    )
```
